128 devices in a mesh: rows: 64 (over z, y, x), terms: 2 (over core).
Axes of the slice: x: 4, y: 4, z: 4, core: 2. Of those that a mesh axis runs over, the one named last changes fastest.
Arguments:
- wavefunc: float32 [512, 4, 4, 512], replicated
- left_env: bfloat16 [128, 512, 512], P('terms')
- two_site: bfloat16 [128, 16, 16], P('terms')
- right_env: bfloat16 [128, 512, 512], P('terms', 'rows')
Outputs:
- output 1: float32 [7, 512, 4, 4, 512], P(None, 'terms', None, None, 'rows')
- output 2: float32 [6], replicated
- output 3: float32 [6], replicated
All inputs are finite; a program needn't handle non-finite values.
Results may differ from the reference program's by a relative error of at most 0.0125741.
Values are sent between devices in bfloat16 or wider.
A program may use at most 1 GiB of HBM per device.

```python
import jax
import jax.numpy as jnp
from jax import lax

BOND_DIM = 512
PHYS_DIM = 4
NUM_TERMS = 128
LANCZOS_STEPS = 6


def symmetric_draw(draw_key, term_count, mat_size):
    raw_draw = jax.random.normal(draw_key, (term_count, mat_size, mat_size), jnp.float32)
    return (raw_draw + jnp.swapaxes(raw_draw, 1, 2)) * (2.0 * mat_size) ** -0.5


def setup_inputs(seed: int = 0) -> dict:
    base_key = jax.random.key(seed)
    key_psi, key_left, key_two, key_right, key_shift = jax.random.split(base_key, 5)
    pair_dim = PHYS_DIM * PHYS_DIM
    eye_bond = jnp.eye(BOND_DIM, dtype=jnp.float32)
    eye_pair = jnp.eye(pair_dim, dtype=jnp.float32)
    wavefunc = jax.random.normal(key_psi, (BOND_DIM, PHYS_DIM, PHYS_DIM, BOND_DIM), jnp.float32)
    left_env = (symmetric_draw(key_left, NUM_TERMS, BOND_DIM) + eye_bond).astype(jnp.bfloat16)
    right_env = (symmetric_draw(key_right, NUM_TERMS, BOND_DIM) + eye_bond).astype(jnp.bfloat16)
    shifts = NUM_TERMS ** -0.5 + 0.5 * jax.random.normal(key_shift, (NUM_TERMS,), jnp.float32)
    two_site = ((symmetric_draw(key_two, NUM_TERMS, pair_dim) + shifts[:, None, None] * eye_pair) * NUM_TERMS ** -0.5).astype(jnp.bfloat16)
    return {'wavefunc': wavefunc, 'left_env': left_env, 'two_site': two_site, 'right_env': right_env}


def reference(wavefunc, left_env, two_site, right_env):
    pair_dim = PHYS_DIM * PHYS_DIM
    vec_shape = (BOND_DIM, pair_dim, BOND_DIM)

    def apply_ham(in_vec):
        u_mat = in_vec.astype(jnp.bfloat16).reshape(BOND_DIM * pair_dim, BOND_DIM)

        def add_term(running, term_ops):
            left_mat, two_mat, right_mat = term_ops
            right_part = jnp.dot(u_mat, right_mat.T, preferred_element_type=jnp.float32).astype(jnp.bfloat16)
            mid_part = jnp.einsum('qp,cpb->cqb', two_mat.astype(jnp.float32), right_part.reshape(vec_shape).astype(jnp.float32)).astype(jnp.bfloat16)
            left_part = jnp.dot(left_mat, mid_part.reshape(BOND_DIM, pair_dim * BOND_DIM), preferred_element_type=jnp.float32)
            return running + left_part.reshape(vec_shape), None

        sigma_vec, _ = lax.scan(add_term, jnp.zeros(vec_shape, jnp.float32), (left_env, two_site, right_env))
        return sigma_vec

    init_scale = jnp.sqrt(jnp.mean(wavefunc * wavefunc))
    first_vec = (wavefunc / init_scale).reshape(vec_shape)

    def lanczos_step(state_in, unused):
        prev_vec, cur_vec, prev_beta = state_in
        w_vec = apply_ham(cur_vec)
        alpha_val = jnp.mean(w_vec * cur_vec)
        w_vec = w_vec - alpha_val * cur_vec - prev_beta * prev_vec
        beta_val = jnp.sqrt(jnp.mean(w_vec * w_vec))
        next_vec = w_vec / beta_val
        return (cur_vec, next_vec, beta_val), (next_vec, alpha_val, beta_val)

    start_state = (jnp.zeros(vec_shape, jnp.float32), first_vec, jnp.zeros((), jnp.float32))
    _, (later_vecs, alpha_diag, beta_offdiag) = lax.scan(lanczos_step, start_state, None, length=LANCZOS_STEPS)
    krylov = jnp.concatenate([first_vec[None], later_vecs], axis=0).reshape(LANCZOS_STEPS + 1, BOND_DIM, PHYS_DIM, PHYS_DIM, BOND_DIM)
    return krylov, alpha_diag, beta_offdiag
```

```python
import jax
import jax.numpy as jnp
from jax import lax
from jax.experimental import pallas as pl
from jax.experimental.pallas import tpu as pltpu
from jax.sharding import PartitionSpec as P

STEPS = 6
F32 = jnp.float32
BF16 = jnp.bfloat16
MESH = pl.DeviceIdType.MESH
NT = 64


def total(x):
    return jnp.sum(jnp.sum(x, axis=1, keepdims=True), axis=0, keepdims=True)


def col_sum(x):
    return jnp.sum(x, axis=0, keepdims=True)


def kernel(elem_count, u0_ref, v0_ref, kr0_ref, left_ref, right_ref, two_ref, kr_ref, ab_ref,
           u_ref, rin, rb, lb, wt, y_ref, z_ref, acc_o, acc_m, recv_s, recv_x, vecs, kbuf, red_a, red_b,
           ld_sem, r_send, r_recv, s_send, s_recv, x_send, x_recv, a_send, a_recv, b_send, b_recv,
           g1_send, g1_recv, g2_send, g2_recv, g3_send, g3_recv, k_send, k_recv):
    r = lax.axis_index('rows')
    c = lax.axis_index('terms')
    x = lax.rem(r, 4)
    y = lax.rem(r // 4, 4)
    z = r // 16
    row_base = r - x

    def rcopy(src, dst, ssem, rsem, row, core):
        return pltpu.make_async_remote_copy(src_ref=src, dst_ref=dst, send_sem=ssem, recv_sem=rsem,
                                            device_id=(row, core), device_id_type=MESH)

    cp_l = pltpu.make_async_copy(left_ref.at[:, pl.ds(pl.multiple_of(x * 128, 128), 128), :], lb, ld_sem.at[0])
    cp_u = pltpu.make_async_copy(u0_ref, u_ref, ld_sem.at[1])
    cp_r = pltpu.make_async_copy(right_ref, rin.at[x], ld_sem.at[2])
    cp_r.start()
    cp_u.start()
    cp_l.start()
    cp_r.wait()
    r_copies = []
    for d in range(1, 4):
        px = lax.rem(x + d, 4)
        cp = rcopy(rin.at[x], rin.at[x], r_send.at[d - 1], r_recv.at[d - 1], row_base + px, c)
        cp.start()
        r_copies.append(cp)

    lane16 = lax.broadcasted_iota(jnp.int32, (16, 256), 1)
    row16 = lax.broadcasted_iota(jnp.int32, (16, 256), 0)
    e_col = (lane16 // 16 == row16).astype(BF16)
    row_e = lax.broadcasted_iota(jnp.int32, (256, 16), 0)
    lane_e = lax.broadcasted_iota(jnp.int32, (256, 16), 1)
    e_row = (row_e // 16 == lane_e).astype(BF16)
    row_m = lax.broadcasted_iota(jnp.int32, (256, 256), 0)
    lane_m = lax.broadcasted_iota(jnp.int32, (256, 256), 1)
    diag = lax.rem(row_m, 16) == lax.rem(lane_m, 16)

    def build_w(k, carry):
        wk = two_ref[pl.ds(pl.multiple_of(k * 16, 16), 16), :]
        wide = jnp.dot(wk, e_col, preferred_element_type=F32).astype(BF16)
        full = jnp.dot(e_row, wide, preferred_element_type=F32)
        wt[k] = jnp.where(diag, full, 0.0).astype(BF16)
        return carry

    lax.fori_loop(0, NT, build_w, 0)

    vecs[0] = v0_ref[...]
    kbuf[0] = kr0_ref[...]
    for cp in r_copies:
        cp.wait()

    def build_r(i, carry):
        rows = pl.ds(pl.multiple_of(i * 64, 64), 64)
        for bhi in range(2):
            lo = rin[2 * bhi, rows, :].astype(F32).reshape(8, 8, 512)
            hi = rin[2 * bhi + 1, rows, :].astype(F32).reshape(8, 8, 512)
            both = jnp.concatenate([lo, hi], axis=1).reshape(128, 512)
            rb[bhi, pl.ds(pl.multiple_of(i * 128, 128), 128), :] = both.astype(BF16)
        return carry

    lax.fori_loop(0, 8, build_r, 0)
    cp_u.wait()
    cp_l.wait()

    row_id = lax.broadcasted_iota(jnp.int32, (8, 128), 0)
    ab_ref[...] = jnp.zeros_like(ab_ref)

    def pack(p, n, am, rr, ss):
        out = jnp.where(row_id == 0, p, 0.0)
        out = jnp.where(row_id == 1, n, out)
        out = jnp.where(row_id == 2, am, out)
        out = jnp.where(row_id == 3, rr, out)
        return jnp.where(row_id == 4, ss, out)

    def safe_div(num, den):
        ok = den > 0.0
        return jnp.where(ok, num / jnp.where(ok, den, 1.0), 0.0)

    def merge(p, n, am, rr, ss):
        n_all = col_sum(n)
        mean = safe_div(col_sum(am * n), n_all)
        gap = mean - am
        r_all = col_sum(rr + gap * (gap * n - 2.0 * ss))
        return col_sum(p), n_all, mean, r_all, col_sum(ss)

    def step(j, prev_beta):
        def s1(pp, carry):
            w = jnp.concatenate([u_ref[2 * pp].reshape(512, 128), u_ref[2 * pp + 1].reshape(512, 128)], axis=1)
            for bhi in range(2):
                for mc in range(2):
                    o = jnp.dot(rb[bhi, mc * 512:(mc + 1) * 512, :], w, preferred_element_type=F32)
                    o = o.astype(BF16).reshape(32, 16, 256)
                    y_ref[mc * 32:(mc + 1) * 32, bhi, 2 * pp] = o[:, :, :128]
                    y_ref[mc * 32:(mc + 1) * 32, bhi, 2 * pp + 1] = o[:, :, 128:]
            return carry

        lax.fori_loop(0, 8, s1, 0)

        def s2(kk, carry):
            for i in range(4):
                k = kk * 4 + i
                rhs = jnp.concatenate([y_ref[k, 0].reshape(256, 128), y_ref[k, 1].reshape(256, 128)], axis=1)
                o = jnp.dot(wt[k], rhs, preferred_element_type=F32).astype(BF16)
                z_ref[0, k] = o[:, :128]
                z_ref[1, k] = o[:, 128:]
            return carry

        lax.fori_loop(0, NT // 4, s2, 0)

        def s3(bhi, acc):
            def part(kc):
                lhs = jnp.concatenate([z_ref[bhi, kc * 8 + i] for i in range(8)], axis=1)
                rhs = lb[pl.ds(kc * 8, 8)].reshape(1024, 512)
                return jnp.dot(lhs, rhs, preferred_element_type=F32)

            o = part(0)
            for i in range(4):
                acc[i] = o[:, i * 128:(i + 1) * 128]

            def more(kc, carry):
                o = part(kc)
                for i in range(4):
                    acc[i] += o[:, i * 128:(i + 1) * 128]
                return carry

            lax.fori_loop(1, 8, more, 0)

        s3(1 - c, acc_o)
        cp_s = rcopy(acc_o, recv_s, s_send.at[0], s_recv.at[0], r, 1 - c)
        cp_s.start()
        s3(c, acc_m)
        cp_s.wait()
        for i in range(4):
            acc_m[i] += recv_s[i]
        x_copies = []
        for d in range(1, 4):
            px = lax.rem(x + d, 4)
            cp = rcopy(acc_m.at[px], recv_x.at[d - 1], x_send.at[d - 1], x_recv.at[d - 1], row_base + px, c)
            cp.start()
            x_copies.append(cp)
        for cp in x_copies:
            cp.wait()
        w_vec = (acc_m[x] + recv_x[0]) + (recv_x[1] + recv_x[2])
        v_cur = vecs[j]
        v_old = vecs[lax.max(j - 1, 0)]

        w_res = w_vec - prev_beta * v_old
        n_loc = total(v_cur * v_cur)
        a_loc = safe_div(total(w_res * v_cur), n_loc)
        e_loc = w_res - a_loc * v_cur
        red_a[0] = pack(total(w_vec * v_cur), n_loc, a_loc, total(e_loc * e_loc), total(e_loc * v_cur))

        a_copies = []
        for d in range(1, 8):
            slot = lax.rem(x * 2 + c + d, 8)
            cp = rcopy(red_a.at[0], red_a.at[d], a_send.at[d - 1], a_recv.at[d - 1], row_base + slot // 2, lax.rem(slot, 2))
            cp.start()
            a_copies.append(cp)
        for cp in a_copies:
            cp.wait()
        me = x * 2 + c
        blocks = [red_a[lax.rem(me - s + 8, 8)] for s in range(8)]

        def gather_rows(blks, i):
            return jnp.concatenate([bk[i:i + 1, :] for bk in blks], axis=0)

        red_b[0] = pack(*merge(*[gather_rows(blocks, i) for i in range(5)]))
        b_copies = []
        g = z * 4 + y
        for d in range(1, 16):
            pg = lax.rem(g + d, 16)
            cp = rcopy(red_b.at[0], red_b.at[d], b_send.at[d - 1], b_recv.at[d - 1], pg * 4 + x, c)
            cp.start()
            b_copies.append(cp)
        for cp in b_copies:
            cp.wait()
        blocks = [red_b[lax.rem(g - s + 16, 16)] for s in range(16)]
        p_all, n_all, a_all, r_all, s_all = [gather_rows(blocks, i) for i in range(5)]
        alpha = col_sum(p_all) / elem_count
        gap = alpha - a_all
        beta = jnp.sqrt(col_sum(r_all + gap * (gap * n_all - 2.0 * s_all)) / elem_count)
        alpha_s = alpha[:, :1]
        beta_s = beta[:, :1]

        v_new = (w_vec - alpha_s * v_cur - prev_beta * v_old) / beta_s
        vecs[j + 1] = v_new
        ab_ref[pl.ds(j, 1), :] = alpha
        ab_ref[pl.ds(8 + j, 1), :] = beta

        for h in range(2):
            dst_x = 2 * c + h
            dst_c = x // 2
            is_me = jnp.logical_and(dst_x == x, dst_c == c)
            lanes = pl.ds(pl.multiple_of(lax.rem(x, 2) * 128, 128), 128)
            src = vecs.at[j + 1].reshape(16, 16, 128).at[:, h * 8:(h + 1) * 8, :]

            @pl.when(jnp.logical_not(is_me))
            def _():
                rcopy(src, kbuf.at[j + 1, :, :, lanes], k_send.at[j, h], k_recv.at[j, lax.rem(x, 2)],
                      row_base + dst_x, dst_c).start()

            @pl.when(is_me)
            def _():
                kbuf[j + 1, :, :, lanes] = v_new.reshape(16, 16, 128)[:, h * 8:(h + 1) * 8, :]

        @pl.when(j < STEPS - 1)
        def _():
            u_ref[:, z, y, c] = v_new.astype(BF16).reshape(16, 16, 128)
            lo, hi = pl.ds(0, 8), pl.ds(8, 8)
            cps = []
            for d in range(1, 4):
                zrow = lax.rem(z + d, 4) * 16 + y * 4 + x
                yrow = z * 16 + lax.rem(y + d, 4) * 4 + x
                s1_ = u_ref.at[lo, z, y, c]
                s2_ = u_ref.at[hi, z, y, c]
                cps.append(rcopy(s1_, s1_, g1_send.at[0, d - 1], g1_recv.at[0, d - 1], zrow, c))
                cps.append(rcopy(s2_, s2_, g1_send.at[1, d - 1], g1_recv.at[1, d - 1], yrow, c))
            for cp in cps:
                cp.start()
            for cp in cps:
                cp.wait()
            cps = []
            for d in range(1, 4):
                zrow = lax.rem(z + d, 4) * 16 + y * 4 + x
                yrow = z * 16 + lax.rem(y + d, 4) * 4 + x
                s1_ = u_ref.at[lo, :, y, c]
                s2_ = u_ref.at[hi, z, :, c]
                cps.append(rcopy(s1_, s1_, g2_send.at[0, d - 1], g2_recv.at[0, d - 1], yrow, c))
                cps.append(rcopy(s2_, s2_, g2_send.at[1, d - 1], g2_recv.at[1, d - 1], zrow, c))
            for cp in cps:
                cp.start()
            for cp in cps:
                cp.wait()
            s3_ = u_ref.at[:, :, :, c]
            cp3 = rcopy(s3_, s3_, g3_send.at[0], g3_recv.at[0], r, 1 - c)
            cp3.start()
            cp3.wait()

        return beta_s

    lax.fori_loop(0, STEPS, step, jnp.zeros((1, 1), F32))

    def drain(j, carry):
        for h in range(2):
            dst_x = 2 * c + h
            dst_c = x // 2
            src = vecs.at[j + 1].reshape(16, 16, 128).at[:, h * 8:(h + 1) * 8, :]

            @pl.when(jnp.logical_not(jnp.logical_and(dst_x == x, dst_c == c)))
            def _():
                rcopy(src, kbuf.at[j + 1, :, :, 0:128], k_send.at[j, h], k_recv.at[j, 0],
                      row_base + dst_x, dst_c).wait_send()

        for m in range(2):
            src_x = 2 * c + m
            src_c = x // 2

            @pl.when(jnp.logical_not(jnp.logical_and(src_x == x, src_c == c)))
            def _():
                rcopy(vecs.at[j + 1].reshape(16, 16, 128).at[:, 0:8, :], kbuf.at[j + 1, :, :, m * 128:(m + 1) * 128],
                      k_send.at[j, 0], k_recv.at[j, m], row_base + src_x, src_c).wait_recv()

        return carry

    lax.fori_loop(0, STEPS, drain, 0)
    cp_k = pltpu.make_async_copy(kbuf, kr_ref, ld_sem.at[0])
    cp_k.start()
    cp_k.wait()


def solution(mesh):
    assert mesh.shape['terms'] == 2 and mesh.shape['rows'] == 64

    def body_fn(wavefunc, left_loc, two_loc, right_loc):
        elem_count = float(wavefunc.size)
        row = lax.axis_index('rows')
        core = lax.axis_index('terms')
        xi = lax.rem(row, 4)
        gi = row // 4
        wave = wavefunc.reshape(512, 16, 512)
        scale = jnp.sqrt(jnp.mean(wave * wave))
        slab = lax.dynamic_slice(wave, (xi * 128, 0, 0), (128, 16, 512)) / scale
        u0 = jnp.transpose(slab.astype(BF16), (1, 2, 0)).reshape(16, 4, 4, 2, 16, 128)
        mine = lax.dynamic_slice(slab, (0, 0, gi * 32 + core * 16), (128, 16, 16))
        v0 = jnp.transpose(mine, (1, 2, 0)).reshape(256, 128)
        out0 = lax.dynamic_slice(wave, (core * 256, 0, row * 8), (256, 16, 8)) / scale
        kr0 = jnp.transpose(out0, (1, 2, 0))
        vm = pl.BlockSpec(memory_space=pltpu.VMEM)
        hbm = pl.BlockSpec(memory_space=pl.ANY)
        dma = pltpu.SemaphoreType.DMA
        kr, ab = pl.pallas_call(
            lambda *refs: kernel(elem_count, *refs),
            out_shape=(jax.ShapeDtypeStruct((STEPS + 1, 16, 8, 256), F32), jax.ShapeDtypeStruct((16, 128), F32)),
            in_specs=[hbm, vm, vm, hbm, hbm, vm],
            out_specs=(hbm, vm),
            scratch_shapes=[
                pltpu.VMEM((16, 4, 4, 2, 16, 128), BF16),
                pltpu.VMEM((4, 512, 512), BF16),
                pltpu.VMEM((2, 1024, 512), BF16),
                pltpu.VMEM((NT, 128, 512), BF16),
                pltpu.VMEM((NT, 256, 256), BF16),
                pltpu.VMEM((NT, 2, 16, 16, 128), BF16),
                pltpu.VMEM((2, NT, 256, 128), BF16),
                pltpu.VMEM((4, 256, 128), F32),
                pltpu.VMEM((4, 256, 128), F32),
                pltpu.VMEM((4, 256, 128), F32),
                pltpu.VMEM((3, 256, 128), F32),
                pltpu.VMEM((STEPS + 1, 256, 128), F32),
                pltpu.VMEM((STEPS + 1, 16, 8, 256), F32),
                pltpu.VMEM((8, 8, 128), F32),
                pltpu.VMEM((16, 8, 128), F32),
                dma((3,)), dma((3,)), dma((3,)), dma((1,)), dma((1,)), dma((3,)), dma((3,)),
                dma((7,)), dma((7,)), dma((15,)), dma((15,)),
                dma((2, 3)), dma((2, 3)), dma((2, 3)), dma((2, 3)), dma((1,)), dma((1,)),
                dma((STEPS, 2)), dma((STEPS, 2)),
            ],
            compiler_params=pltpu.CompilerParams(has_side_effects=True, vmem_limit_bytes=60 * 1024 * 1024),
        )(u0, v0, kr0, left_loc, right_loc.reshape(512, 512), two_loc.reshape(1024, 16))
        krylov = jnp.transpose(kr.reshape(STEPS + 1, 4, 4, 8, 256), (0, 4, 1, 2, 3))
        return krylov, ab[:STEPS, 0], ab[8:8 + STEPS, 0]

    return jax.shard_map(body_fn, mesh=mesh, in_specs=(P(), P('terms'), P('terms'), P('terms', 'rows')),
                         out_specs=(P(None, 'terms', None, None, 'rows'), P(), P()), check_vma=False)
```

```python
import jax
import jax.numpy as jnp
from jax import lax
from jax.experimental import pallas as pl
from jax.experimental.pallas import tpu as pltpu
from jax.sharding import PartitionSpec as P

STEPS = 6
F32 = jnp.float32
BF16 = jnp.bfloat16
MESH = pl.DeviceIdType.MESH
NT = 64


def total(x):
    return jnp.sum(jnp.sum(x, axis=1, keepdims=True), axis=0, keepdims=True)


def col_sum(x):
    return jnp.sum(x, axis=0, keepdims=True)


def sq_block(blk):
    out = jnp.zeros((8, 128), F32)
    sq = (blk * blk).reshape(16, 8, 512).sum(axis=0)
    for i in range(4):
        out = out + sq[:, i * 128:(i + 1) * 128]
    return out


def kernel(elem_count, wave_ref, left_ref, right_ref, two_ref, kr_ref, ab_ref,
           slab, nslab, tmp, ut, u_ref, rin, rb, lb, wt, y_ref, z_ref, acc_o, acc_m, recv_s, recv_x, vecs, kbuf,
           red_n, red_a, red_b,
           ld_sem, sl_sem, r_send, r_recv, n_send, n_recv, s_send, s_recv, x_send, x_recv, a_send, a_recv,
           b_send, b_recv, g1_send, g1_recv, g2_send, g2_recv, g3_send, g3_recv, k_send, k_recv):
    r = lax.axis_index('rows')
    c = lax.axis_index('terms')
    x = lax.rem(r, 4)
    y = lax.rem(r // 4, 4)
    z = r // 16
    g = r // 4
    row_base = r - x

    def rcopy(src, dst, ssem, rsem, row, core):
        return pltpu.make_async_remote_copy(src_ref=src, dst_ref=dst, send_sem=ssem, recv_sem=rsem,
                                            device_id=(row, core), device_id_type=MESH)

    cp_r = pltpu.make_async_copy(right_ref, rin.at[x], ld_sem.at[0])
    cp_r.start()
    n_loads, s_loads = [], []
    for p in range(16):
        rows_n = pl.ds(pl.multiple_of(z * 128, 128), 128)
        n_loads.append(pltpu.make_async_copy(wave_ref.at[rows_n, p // 4, p % 4, :], nslab.at[p], sl_sem.at[0, p]))
    for p in range(16):
        rows_s = pl.ds(pl.multiple_of(x * 128, 128), 128)
        s_loads.append(pltpu.make_async_copy(wave_ref.at[rows_s, p // 4, p % 4, :], slab.at[p], sl_sem.at[1, p]))
    cp_l = pltpu.make_async_copy(left_ref.at[:, pl.ds(pl.multiple_of(x * 128, 128), 128), :], lb, ld_sem.at[1])
    for cp in n_loads + s_loads:
        cp.start()
    cp_l.start()
    cp_r.wait()

    right = row_base + lax.rem(x + 1, 4)
    left = row_base + lax.rem(x + 3, 4)
    xl = lax.rem(x + 3, 4)
    xr = lax.rem(x + 1, 4)
    halves = [pl.ds(0, 256), pl.ds(256, 256)]

    def r_move(i, block, half, row):
        ref = rin.at[block, halves[half], :]
        return rcopy(ref, ref, r_send.at[i], r_recv.at[i], row, c)

    r0 = r_move(0, x, 0, right)
    r1 = r_move(1, x, 1, left)
    r2 = r_move(2, x, 1, right)
    r3 = r_move(3, x, 0, left)
    r4 = r_move(4, xl, 0, right)
    r5 = r_move(5, xr, 1, left)
    for cp in (r0, r1, r2, r3):
        cp.start()

    for cp in n_loads:
        cp.wait()

    ssq = jnp.zeros((8, 128), F32)
    ssq = lax.fori_loop(0, 16, lambda p, acc: acc + sq_block(nslab[p]), ssq)
    red_n[0] = jnp.zeros((8, 128), F32) + total(ssq)
    n_copies = []
    for d in range(1, 4):
        row = lax.rem(z + d, 4) * 16 + y * 4 + x
        cp = rcopy(red_n.at[0], red_n.at[d], n_send.at[d - 1], n_recv.at[d - 1], row, c)
        cp.start()
        n_copies.append(cp)

    lane16 = lax.broadcasted_iota(jnp.int32, (16, 256), 1)
    row16 = lax.broadcasted_iota(jnp.int32, (16, 256), 0)
    e_col = (lane16 // 16 == row16).astype(BF16)
    row_e = lax.broadcasted_iota(jnp.int32, (256, 16), 0)
    lane_e = lax.broadcasted_iota(jnp.int32, (256, 16), 1)
    e_row = (row_e // 16 == lane_e).astype(BF16)
    row_m = lax.broadcasted_iota(jnp.int32, (256, 256), 0)
    lane_m = lax.broadcasted_iota(jnp.int32, (256, 256), 1)
    diag = lax.rem(row_m, 16) == lax.rem(lane_m, 16)

    def build_w(k, carry):
        wk = two_ref[pl.ds(pl.multiple_of(k * 16, 16), 16), :]
        wide = jnp.dot(wk, e_col, preferred_element_type=F32).astype(BF16)
        full = jnp.dot(e_row, wide, preferred_element_type=F32)
        wt[k] = jnp.where(diag, full, 0.0).astype(BF16)
        return carry

    lax.fori_loop(0, NT, build_w, 0)
    r0.wait_recv()
    r4.start()
    r1.wait_recv()
    r5.start()

    for cp in n_copies:
        cp.wait()
    norm = [red_n[lax.rem(z - s + 4, 4)] for s in range(4)]
    scale = jnp.sqrt(((norm[0] + norm[1]) + (norm[2] + norm[3]))[:1, :1] / elem_count)
    for cp in s_loads:
        cp.wait()
    b_lanes = pl.ds(pl.multiple_of((g // 4) * 128, 128), 128)
    b_rows = pl.ds(pl.multiple_of(lax.rem(g, 4) * 32 + c * 16, 16), 16)

    def first(p, carry):
        ut[p] = (slab[p] / scale).astype(BF16)
        tmp[...] = jnp.transpose(slab[p, :, b_lanes])
        vecs[0, pl.ds(pl.multiple_of(p * 16, 16), 16), :] = tmp[b_rows, :] / scale
        return carry

    lax.fori_loop(0, 16, first, 0)

    out_lanes = pl.ds(pl.multiple_of(lax.rem(x, 2) * 128, 128), 128)

    def piece(jv, h):
        return vecs.at[jv].reshape(16, 16, 128).at[:, h * 8:(h + 1) * 8, :]

    def emit(jv):
        for h in range(2):
            dst_x = 2 * c + h
            dst_c = x // 2
            is_me = jnp.logical_and(dst_x == x, dst_c == c)

            @pl.when(jnp.logical_not(is_me))
            def _():
                rcopy(piece(jv, h), kbuf.at[jv, :, :, out_lanes], k_send.at[jv, h], k_recv.at[jv, lax.rem(x, 2)],
                      row_base + dst_x, dst_c).start()

            @pl.when(is_me)
            def _():
                kbuf[jv, :, :, out_lanes] = vecs[jv].reshape(16, 16, 128)[:, h * 8:(h + 1) * 8, :]

    for cp in (r2, r3, r4, r5):
        cp.wait_recv()
    emit(0)

    def build_r(i, carry):
        rows = pl.ds(pl.multiple_of(i * 64, 64), 64)
        for bhi in range(2):
            lo = rin[2 * bhi, rows, :].astype(F32).reshape(8, 8, 512)
            hi = rin[2 * bhi + 1, rows, :].astype(F32).reshape(8, 8, 512)
            both = jnp.concatenate([lo, hi], axis=1).reshape(128, 512)
            rb[bhi, pl.ds(pl.multiple_of(i * 128, 128), 128), :] = both.astype(BF16)
        return carry

    lax.fori_loop(0, 8, build_r, 0)
    for cp in (r0, r1, r2, r3, r4, r5):
        cp.wait_send()

    def put_y(o, bhi, mc, pp):
        o = o.astype(BF16).reshape(32, 16, 256)
        y_ref[mc * 32:(mc + 1) * 32, bhi, 2 * pp] = o[:, :, :128]
        y_ref[mc * 32:(mc + 1) * 32, bhi, 2 * pp + 1] = o[:, :, 128:]

    def s1_first(pp, carry):
        w = ut[pl.ds(2 * pp, 2)].reshape(256, 512)
        for bhi in range(2):
            for mc in range(2):
                o = lax.dot_general(rb[bhi, mc * 512:(mc + 1) * 512, :], w, (((1,), (1,)), ((), ())),
                                    preferred_element_type=F32)
                put_y(o, bhi, mc, pp)
        return carry

    def s1(pp, carry):
        w = jnp.concatenate([u_ref[2 * pp].reshape(512, 128), u_ref[2 * pp + 1].reshape(512, 128)], axis=1)
        for bhi in range(2):
            for mc in range(2):
                o = jnp.dot(rb[bhi, mc * 512:(mc + 1) * 512, :], w, preferred_element_type=F32)
                put_y(o, bhi, mc, pp)
        return carry

    lax.fori_loop(0, 8, s1_first, 0)
    cp_l.wait()

    row_id = lax.broadcasted_iota(jnp.int32, (8, 128), 0)
    ab_ref[...] = jnp.zeros_like(ab_ref)

    def pack(p, n, am, rr, ss):
        out = jnp.where(row_id == 0, p, 0.0)
        out = jnp.where(row_id == 1, n, out)
        out = jnp.where(row_id == 2, am, out)
        out = jnp.where(row_id == 3, rr, out)
        return jnp.where(row_id == 4, ss, out)

    def safe_div(num, den):
        ok = den > 0.0
        return jnp.where(ok, num / jnp.where(ok, den, 1.0), 0.0)

    def merge(p, n, am, rr, ss):
        n_all = col_sum(n)
        mean = safe_div(col_sum(am * n), n_all)
        gap = mean - am
        r_all = col_sum(rr + gap * (gap * n - 2.0 * ss))
        return col_sum(p), n_all, mean, r_all, col_sum(ss)

    def step(j, prev_beta):
        def s2(kk, carry):
            for i in range(4):
                k = kk * 4 + i
                rhs = jnp.concatenate([y_ref[k, 0].reshape(256, 128), y_ref[k, 1].reshape(256, 128)], axis=1)
                o = jnp.dot(wt[k], rhs, preferred_element_type=F32).astype(BF16)
                z_ref[0, k] = o[:, :128]
                z_ref[1, k] = o[:, 128:]
            return carry

        lax.fori_loop(0, NT // 4, s2, 0)

        def s3(bhi, acc):
            def part(kc):
                lhs = jnp.concatenate([z_ref[bhi, kc * 8 + i] for i in range(8)], axis=1)
                rhs = lb[pl.ds(kc * 8, 8)].reshape(1024, 512)
                return jnp.dot(lhs, rhs, preferred_element_type=F32)

            o = part(0)
            for i in range(4):
                acc[i] = o[:, i * 128:(i + 1) * 128]

            def more(kc, carry):
                o = part(kc)
                for i in range(4):
                    acc[i] += o[:, i * 128:(i + 1) * 128]
                return carry

            lax.fori_loop(1, 8, more, 0)

        s3(1 - c, acc_o)
        cp_s = rcopy(acc_o, recv_s, s_send.at[0], s_recv.at[0], r, 1 - c)
        cp_s.start()
        s3(c, acc_m)
        cp_s.wait()
        for i in range(4):
            acc_m[i] += recv_s[i]
        x_copies = []
        for d in range(1, 4):
            px = lax.rem(x + d, 4)
            cp = rcopy(acc_m.at[px], recv_x.at[d - 1], x_send.at[d - 1], x_recv.at[d - 1], row_base + px, c)
            cp.start()
            x_copies.append(cp)
        for cp in x_copies:
            cp.wait()
        w_vec = (acc_m[x] + recv_x[0]) + (recv_x[1] + recv_x[2])
        v_cur = vecs[j]
        v_old = vecs[lax.max(j - 1, 0)]

        w_res = w_vec - prev_beta * v_old
        n_loc = total(v_cur * v_cur)
        a_loc = safe_div(total(w_res * v_cur), n_loc)
        e_loc = w_res - a_loc * v_cur
        red_a[0] = pack(total(w_vec * v_cur), n_loc, a_loc, total(e_loc * e_loc), total(e_loc * v_cur))

        a_copies = []
        for d in range(1, 8):
            slot = lax.rem(x * 2 + c + d, 8)
            cp = rcopy(red_a.at[0], red_a.at[d], a_send.at[d - 1], a_recv.at[d - 1], row_base + slot // 2, lax.rem(slot, 2))
            cp.start()
            a_copies.append(cp)
        for cp in a_copies:
            cp.wait()
        me = x * 2 + c
        blocks = [red_a[lax.rem(me - s + 8, 8)] for s in range(8)]

        def gather_rows(blks, i):
            return jnp.concatenate([bk[i:i + 1, :] for bk in blks], axis=0)

        red_b[0] = pack(*merge(*[gather_rows(blocks, i) for i in range(5)]))
        b_copies = []
        for d in range(1, 16):
            pg = lax.rem(g + d, 16)
            cp = rcopy(red_b.at[0], red_b.at[d], b_send.at[d - 1], b_recv.at[d - 1], pg * 4 + x, c)
            cp.start()
            b_copies.append(cp)
        for cp in b_copies:
            cp.wait()
        blocks = [red_b[lax.rem(g - s + 16, 16)] for s in range(16)]
        p_all, n_all, a_all, r_all, s_all = [gather_rows(blocks, i) for i in range(5)]
        alpha = col_sum(p_all) / elem_count
        gap = alpha - a_all
        beta = jnp.sqrt(col_sum(r_all + gap * (gap * n_all - 2.0 * s_all)) / elem_count)
        alpha_s = alpha[:, :1]
        beta_s = beta[:, :1]

        v_new = (w_vec - alpha_s * v_cur - prev_beta * v_old) / beta_s
        vecs[j + 1] = v_new
        ab_ref[pl.ds(j, 1), :] = alpha
        ab_ref[pl.ds(8 + j, 1), :] = beta

        emit(j + 1)

        @pl.when(j < STEPS - 1)
        def _():
            u_ref[:, z, y, c] = v_new.astype(BF16).reshape(16, 16, 128)
            lo, hi = pl.ds(0, 8), pl.ds(8, 8)
            cps = []
            for d in range(1, 4):
                zrow = lax.rem(z + d, 4) * 16 + y * 4 + x
                yrow = z * 16 + lax.rem(y + d, 4) * 4 + x
                s1_ = u_ref.at[lo, z, y, c]
                s2_ = u_ref.at[hi, z, y, c]
                cps.append(rcopy(s1_, s1_, g1_send.at[0, d - 1], g1_recv.at[0, d - 1], zrow, c))
                cps.append(rcopy(s2_, s2_, g1_send.at[1, d - 1], g1_recv.at[1, d - 1], yrow, c))
            for cp in cps:
                cp.start()
            for cp in cps:
                cp.wait()
            cps = []
            for d in range(1, 4):
                zrow = lax.rem(z + d, 4) * 16 + y * 4 + x
                yrow = z * 16 + lax.rem(y + d, 4) * 4 + x
                s1_ = u_ref.at[lo, :, y, c]
                s2_ = u_ref.at[hi, z, :, c]
                cps.append(rcopy(s1_, s1_, g2_send.at[0, d - 1], g2_recv.at[0, d - 1], yrow, c))
                cps.append(rcopy(s2_, s2_, g2_send.at[1, d - 1], g2_recv.at[1, d - 1], zrow, c))
            for cp in cps:
                cp.start()
            for cp in cps:
                cp.wait()
            s3_ = u_ref.at[:, :, :, c]
            cp3 = rcopy(s3_, s3_, g3_send.at[0], g3_recv.at[0], r, 1 - c)
            cp3.start()
            cp3.wait()
            lax.fori_loop(0, 8, s1, 0)

        return beta_s

    lax.fori_loop(0, STEPS, step, jnp.zeros((1, 1), F32))

    def drain(jv, carry):
        for h in range(2):
            dst_x = 2 * c + h
            dst_c = x // 2

            @pl.when(jnp.logical_not(jnp.logical_and(dst_x == x, dst_c == c)))
            def _():
                rcopy(piece(jv, h), kbuf.at[jv, :, :, 0:128], k_send.at[jv, h], k_recv.at[jv, 0],
                      row_base + dst_x, dst_c).wait_send()

        for m in range(2):
            src_x = 2 * c + m
            src_c = x // 2

            @pl.when(jnp.logical_not(jnp.logical_and(src_x == x, src_c == c)))
            def _():
                rcopy(piece(jv, 0), kbuf.at[jv, :, :, m * 128:(m + 1) * 128], k_send.at[jv, 0], k_recv.at[jv, m],
                      row_base + src_x, src_c).wait_recv()

        return carry

    lax.fori_loop(0, STEPS + 1, drain, 0)
    cp_k = pltpu.make_async_copy(kbuf, kr_ref, ld_sem.at[0])
    cp_k.start()
    cp_k.wait()


def solution(mesh):
    assert mesh.shape['terms'] == 2 and mesh.shape['rows'] == 64

    def body_fn(wavefunc, left_loc, two_loc, right_loc):
        elem_count = float(wavefunc.size)
        vm = pl.BlockSpec(memory_space=pltpu.VMEM)
        hbm = pl.BlockSpec(memory_space=pl.ANY)
        dma = pltpu.SemaphoreType.DMA
        kr, ab = pl.pallas_call(
            lambda *refs: kernel(elem_count, *refs),
            out_shape=(jax.ShapeDtypeStruct((STEPS + 1, 16, 8, 256), F32), jax.ShapeDtypeStruct((16, 128), F32)),
            in_specs=[hbm, hbm, hbm, vm],
            out_specs=(hbm, vm),
            scratch_shapes=[
                pltpu.VMEM((16, 128, 512), F32),
                pltpu.VMEM((16, 128, 512), F32),
                pltpu.VMEM((128, 128), F32),
                pltpu.VMEM((16, 128, 512), BF16),
                pltpu.VMEM((16, 4, 4, 2, 16, 128), BF16),
                pltpu.VMEM((4, 512, 512), BF16),
                pltpu.VMEM((2, 1024, 512), BF16),
                pltpu.VMEM((NT, 128, 512), BF16),
                pltpu.VMEM((NT, 256, 256), BF16),
                pltpu.VMEM((NT, 2, 16, 16, 128), BF16),
                pltpu.VMEM((2, NT, 256, 128), BF16),
                pltpu.VMEM((4, 256, 128), F32),
                pltpu.VMEM((4, 256, 128), F32),
                pltpu.VMEM((4, 256, 128), F32),
                pltpu.VMEM((3, 256, 128), F32),
                pltpu.VMEM((STEPS + 1, 256, 128), F32),
                pltpu.VMEM((STEPS + 1, 16, 8, 256), F32),
                pltpu.VMEM((4, 8, 128), F32),
                pltpu.VMEM((8, 8, 128), F32),
                pltpu.VMEM((16, 8, 128), F32),
                dma((2,)), dma((2, 16)), dma((6,)), dma((6,)), dma((3,)), dma((3,)), dma((1,)), dma((1,)), dma((3,)), dma((3,)),
                dma((7,)), dma((7,)), dma((15,)), dma((15,)),
                dma((2, 3)), dma((2, 3)), dma((2, 3)), dma((2, 3)), dma((1,)), dma((1,)),
                dma((STEPS + 1, 2)), dma((STEPS + 1, 2)),
            ],
            compiler_params=pltpu.CompilerParams(has_side_effects=True, vmem_limit_bytes=60 * 1024 * 1024),
        )(wavefunc, left_loc, right_loc.reshape(512, 512), two_loc.reshape(1024, 16))
        krylov = jnp.transpose(kr.reshape(STEPS + 1, 4, 4, 8, 256), (0, 4, 1, 2, 3))
        return krylov, ab[:STEPS, 0], ab[8:8 + STEPS, 0]

    return jax.shard_map(body_fn, mesh=mesh, in_specs=(P(), P('terms'), P('terms'), P('terms', 'rows')),
                         out_specs=(P(None, 'terms', None, None, 'rows'), P(), P()), check_vma=False)
```

```python
import jax
import jax.numpy as jnp
from jax import lax
from jax.experimental import pallas as pl
from jax.experimental.pallas import tpu as pltpu
from jax.sharding import PartitionSpec as P

STEPS = 6
F32 = jnp.float32
BF16 = jnp.bfloat16
MESH = pl.DeviceIdType.MESH
NT = 64


def total(x):
    return jnp.sum(jnp.sum(x, axis=1, keepdims=True), axis=0, keepdims=True)


def col_sum(x):
    return jnp.sum(x, axis=0, keepdims=True)


def sq_block(blk):
    out = jnp.zeros((8, 128), F32)
    sq = (blk * blk).reshape(16, 8, 512).sum(axis=0)
    for i in range(4):
        out = out + sq[:, i * 128:(i + 1) * 128]
    return out


def kernel(elem_count, wave_ref, left_ref, right_ref, two_ref, kr_ref, ab_ref,
           slab, nslab, tmp, ut, u_ref, rin, rb, lb, wt, y_ref, z_ref, acc_o, acc_m, recv_s, recv_x, vecs, kbuf,
           red_n, red_a, red_b,
           ld_sem, sl_sem, r_send, r_recv, n_send, n_recv, s_send, s_recv, x_send, x_recv, a_send, a_recv,
           b_send, b_recv, g1_send, g1_recv, g2_send, g2_recv, g3_send, g3_recv, k_send, k_recv):
    r = lax.axis_index('rows')
    c = lax.axis_index('terms')
    x = lax.rem(r, 4)
    y = lax.rem(r // 4, 4)
    z = r // 16
    g = r // 4
    row_base = r - x
    z_peers = [lax.rem(z + d, 4) * 16 + y * 4 + x for d in (1, 2, 3)]
    y_peers = [z * 16 + lax.rem(y + d, 4) * 4 + x for d in (1, 2, 3)]
    x_peers = [row_base + lax.rem(x + d, 4) for d in (1, 2, 3)]

    def pair(i, h):
        return pl.ds(8 * h + 2 * i, 2)

    def rcopy(src, dst, ssem, rsem, row, core):
        return pltpu.make_async_remote_copy(src_ref=src, dst_ref=dst, send_sem=ssem, recv_sem=rsem,
                                            device_id=(row, core), device_id_type=MESH)

    cp_r = pltpu.make_async_copy(right_ref, rin.at[x], ld_sem.at[0])
    cp_r.start()
    n_loads, s_loads = [], []
    for p in range(16):
        rows_n = pl.ds(pl.multiple_of(z * 128, 128), 128)
        n_loads.append(pltpu.make_async_copy(wave_ref.at[rows_n, p // 4, p % 4, :], nslab.at[p], sl_sem.at[0, p]))
    for p in range(16):
        rows_s = pl.ds(pl.multiple_of(x * 128, 128), 128)
        s_loads.append(pltpu.make_async_copy(wave_ref.at[rows_s, p // 4, p % 4, :], slab.at[p], sl_sem.at[1, p]))
    cp_l = pltpu.make_async_copy(left_ref.at[:, pl.ds(pl.multiple_of(x * 128, 128), 128), :], lb, ld_sem.at[1])
    for cp in n_loads + s_loads:
        cp.start()
    cp_l.start()
    cp_r.wait()

    right = row_base + lax.rem(x + 1, 4)
    left = row_base + lax.rem(x + 3, 4)
    xl = lax.rem(x + 3, 4)
    xr = lax.rem(x + 1, 4)
    halves = [pl.ds(0, 256), pl.ds(256, 256)]

    def r_move(i, block, half, row):
        ref = rin.at[block, halves[half], :]
        return rcopy(ref, ref, r_send.at[i], r_recv.at[i], row, c)

    r0 = r_move(0, x, 0, right)
    r1 = r_move(1, x, 1, left)
    r2 = r_move(2, x, 1, right)
    r3 = r_move(3, x, 0, left)
    r4 = r_move(4, xl, 0, right)
    r5 = r_move(5, xr, 1, left)
    for cp in (r0, r1, r2, r3):
        cp.start()

    for cp in n_loads:
        cp.wait()

    ssq = jnp.zeros((8, 128), F32)
    ssq = lax.fori_loop(0, 16, lambda p, acc: acc + sq_block(nslab[p]), ssq)
    red_n[0] = jnp.zeros((8, 128), F32) + total(ssq)
    n_copies = []
    for d, row in enumerate(z_peers):
        cp = rcopy(red_n.at[0], red_n.at[d + 1], n_send.at[d], n_recv.at[d], row, c)
        cp.start()
        n_copies.append(cp)

    lane16 = lax.broadcasted_iota(jnp.int32, (16, 256), 1)
    row16 = lax.broadcasted_iota(jnp.int32, (16, 256), 0)
    e_col = (lane16 // 16 == row16).astype(BF16)
    row_e = lax.broadcasted_iota(jnp.int32, (256, 16), 0)
    lane_e = lax.broadcasted_iota(jnp.int32, (256, 16), 1)
    e_row = (row_e // 16 == lane_e).astype(BF16)
    row_m = lax.broadcasted_iota(jnp.int32, (256, 256), 0)
    lane_m = lax.broadcasted_iota(jnp.int32, (256, 256), 1)
    diag = lax.rem(row_m, 16) == lax.rem(lane_m, 16)

    def build_w(k, carry):
        wk = two_ref[pl.ds(pl.multiple_of(k * 16, 16), 16), :]
        wide = jnp.dot(wk, e_col, preferred_element_type=F32).astype(BF16)
        full = jnp.dot(e_row, wide, preferred_element_type=F32)
        wt[k] = jnp.where(diag, full, 0.0).astype(BF16)
        return carry

    lax.fori_loop(0, NT, build_w, 0)
    r0.wait_recv()
    r4.start()
    r1.wait_recv()
    r5.start()

    for cp in n_copies:
        cp.wait()
    norm = [red_n[lax.rem(z - s + 4, 4)] for s in range(4)]
    scale = jnp.sqrt(((norm[0] + norm[1]) + (norm[2] + norm[3]))[:1, :1] / elem_count)
    for cp in s_loads:
        cp.wait()
    b_lanes = pl.ds(pl.multiple_of((g // 4) * 128, 128), 128)
    b_rows = pl.ds(pl.multiple_of(lax.rem(g, 4) * 32 + c * 16, 16), 16)

    def first(p, carry):
        ut[p] = (slab[p] / scale).astype(BF16)
        tmp[...] = jnp.transpose(slab[p, :, b_lanes])
        vecs[0, pl.ds(pl.multiple_of(p * 16, 16), 16), :] = tmp[b_rows, :] / scale
        return carry

    lax.fori_loop(0, 16, first, 0)

    out_lanes = pl.ds(pl.multiple_of(lax.rem(x, 2) * 128, 128), 128)

    def piece(jv, h):
        return vecs.at[jv].reshape(16, 16, 128).at[:, h * 8:(h + 1) * 8, :]

    def emit(jv):
        for h in range(2):
            dst_x = 2 * c + h
            dst_c = x // 2
            is_me = jnp.logical_and(dst_x == x, dst_c == c)

            @pl.when(jnp.logical_not(is_me))
            def _():
                rcopy(piece(jv, h), kbuf.at[jv, :, :, out_lanes], k_send.at[jv, h], k_recv.at[jv, lax.rem(x, 2)],
                      row_base + dst_x, dst_c).start()

            @pl.when(is_me)
            def _():
                kbuf[jv, :, :, out_lanes] = vecs[jv].reshape(16, 16, 128)[:, h * 8:(h + 1) * 8, :]

    for cp in (r2, r3, r4, r5):
        cp.wait_recv()
    emit(0)

    def build_r(i, carry):
        rows = pl.ds(pl.multiple_of(i * 64, 64), 64)
        for bhi in range(2):
            lo = rin[2 * bhi, rows, :].astype(F32).reshape(8, 8, 512)
            hi = rin[2 * bhi + 1, rows, :].astype(F32).reshape(8, 8, 512)
            both = jnp.concatenate([lo, hi], axis=1).reshape(128, 512)
            rb[bhi, pl.ds(pl.multiple_of(i * 128, 128), 128), :] = both.astype(BF16)
        return carry

    lax.fori_loop(0, 8, build_r, 0)
    for cp in (r0, r1, r2, r3, r4, r5):
        cp.wait_send()

    def put_y(o, bhi, mc, pp):
        o = o.astype(BF16).reshape(32, 16, 256)
        y_ref[mc * 32:(mc + 1) * 32, bhi, 2 * pp] = o[:, :, :128]
        y_ref[mc * 32:(mc + 1) * 32, bhi, 2 * pp + 1] = o[:, :, 128:]

    def s1_first(pp, carry):
        w = ut[pl.ds(2 * pp, 2)].reshape(256, 512)
        for bhi in range(2):
            for mc in range(2):
                o = lax.dot_general(rb[bhi, mc * 512:(mc + 1) * 512, :], w, (((1,), (1,)), ((), ())),
                                    preferred_element_type=F32)
                put_y(o, bhi, mc, pp)
        return carry

    def s1(pp, carry):
        w = jnp.concatenate([u_ref[2 * pp].reshape(512, 128), u_ref[2 * pp + 1].reshape(512, 128)], axis=1)
        for bhi in range(2):
            for mc in range(2):
                o = jnp.dot(rb[bhi, mc * 512:(mc + 1) * 512, :], w, preferred_element_type=F32)
                put_y(o, bhi, mc, pp)
        return carry

    lax.fori_loop(0, 8, s1_first, 0)
    cp_l.wait()

    row_id = lax.broadcasted_iota(jnp.int32, (8, 128), 0)
    ab_ref[...] = jnp.zeros_like(ab_ref)

    def pack(p, n, am, rr, ss):
        out = jnp.where(row_id == 0, p, 0.0)
        out = jnp.where(row_id == 1, n, out)
        out = jnp.where(row_id == 2, am, out)
        out = jnp.where(row_id == 3, rr, out)
        return jnp.where(row_id == 4, ss, out)

    def safe_div(num, den):
        ok = den > 0.0
        return jnp.where(ok, num / jnp.where(ok, den, 1.0), 0.0)

    def merge(p, n, am, rr, ss):
        n_all = col_sum(n)
        mean = safe_div(col_sum(am * n), n_all)
        gap = mean - am
        r_all = col_sum(rr + gap * (gap * n - 2.0 * ss))
        return col_sum(p), n_all, mean, r_all, col_sum(ss)

    def step(j, prev_beta):
        def s2(kk, carry):
            for i in range(4):
                k = kk * 4 + i
                rhs = jnp.concatenate([y_ref[k, 0].reshape(256, 128), y_ref[k, 1].reshape(256, 128)], axis=1)
                o = jnp.dot(wt[k], rhs, preferred_element_type=F32).astype(BF16)
                z_ref[0, k] = o[:, :128]
                z_ref[1, k] = o[:, 128:]
            return carry

        lax.fori_loop(0, NT // 4, s2, 0)

        def s3(bhi, acc):
            def part(kc):
                lhs = jnp.concatenate([z_ref[bhi, kc * 8 + i] for i in range(8)], axis=1)
                rhs = lb[pl.ds(kc * 8, 8)].reshape(1024, 512)
                return jnp.dot(lhs, rhs, preferred_element_type=F32)

            o = part(0)
            for i in range(4):
                acc[i] = o[:, i * 128:(i + 1) * 128]

            def more(kc, carry):
                o = part(kc)
                for i in range(4):
                    acc[i] += o[:, i * 128:(i + 1) * 128]
                return carry

            lax.fori_loop(1, 8, more, 0)

        s3(1 - c, acc_o)
        cp_s = rcopy(acc_o, recv_s, s_send.at[0], s_recv.at[0], r, 1 - c)
        cp_s.start()
        s3(c, acc_m)
        cp_s.wait()
        for i in range(4):
            acc_m[i] += recv_s[i]
        x_copies = []
        for d, row in enumerate(x_peers):
            cp = rcopy(acc_m.at[row - row_base], recv_x.at[d], x_send.at[d], x_recv.at[d], row, c)
            cp.start()
            x_copies.append(cp)
        for cp in x_copies:
            cp.wait()
        w_vec = (acc_m[x] + recv_x[0]) + (recv_x[1] + recv_x[2])
        v_cur = vecs[j]
        v_old = vecs[lax.max(j - 1, 0)]

        w_res = w_vec - prev_beta * v_old
        n_loc = total(v_cur * v_cur)
        a_loc = safe_div(total(w_res * v_cur), n_loc)
        e_loc = w_res - a_loc * v_cur
        red_a[0] = pack(total(w_vec * v_cur), n_loc, a_loc, total(e_loc * e_loc), total(e_loc * v_cur))

        a_copies = []
        for d in range(1, 8):
            slot = lax.rem(x * 2 + c + d, 8)
            cp = rcopy(red_a.at[0], red_a.at[d], a_send.at[d - 1], a_recv.at[d - 1], row_base + slot // 2, lax.rem(slot, 2))
            cp.start()
            a_copies.append(cp)
        for cp in a_copies:
            cp.wait()
        me = x * 2 + c
        blocks = [red_a[lax.rem(me - s + 8, 8)] for s in range(8)]

        def gather_rows(blks, i):
            return jnp.concatenate([bk[i:i + 1, :] for bk in blks], axis=0)

        red_b[0] = pack(*merge(*[gather_rows(blocks, i) for i in range(5)]))
        b_copies = []
        for d in range(1, 16):
            pg = lax.rem(g + d, 16)
            cp = rcopy(red_b.at[0], red_b.at[d], b_send.at[d - 1], b_recv.at[d - 1], pg * 4 + x, c)
            cp.start()
            b_copies.append(cp)
        for cp in b_copies:
            cp.wait()
        blocks = [red_b[lax.rem(g - s + 16, 16)] for s in range(16)]
        p_all, n_all, a_all, r_all, s_all = [gather_rows(blocks, i) for i in range(5)]
        alpha = col_sum(p_all) / elem_count
        gap = alpha - a_all
        beta = jnp.sqrt(col_sum(r_all + gap * (gap * n_all - 2.0 * s_all)) / elem_count)
        alpha_s = alpha[:, :1]
        beta_s = beta[:, :1]

        v_new = (w_vec - alpha_s * v_cur - prev_beta * v_old) / beta_s
        vecs[j + 1] = v_new
        ab_ref[pl.ds(j, 1), :] = alpha
        ab_ref[pl.ds(8 + j, 1), :] = beta

        emit(j + 1)

        @pl.when(j < STEPS - 1)
        def _():
            u_ref[:, z, y, c] = v_new.astype(BF16).reshape(16, 16, 128)
            moves = [(h, d) for h in range(2) for d in range(3)]
            cuts = range(4)

            def move(sems, h, i, d, ref, across):
                row = z_peers[d] if across else y_peers[d]
                return rcopy(ref, ref, sems[0].at[h, i, d], sems[1].at[h, i, d], row, c)

            def p1(i, h, d):
                ref = u_ref.at[pair(i, h), z, y, c]
                return move((g1_send, g1_recv), h, i, d, ref, h == 0)

            def p2(i, h, d):
                ref = u_ref.at[pair(i, h), z, :, c] if h else u_ref.at[pair(i, h), :, y, c]
                return move((g2_send, g2_recv), h, i, d, ref, h == 1)

            def p3(i, h):
                ref = u_ref.at[pair(i, h), :, :, c]
                return rcopy(ref, ref, g3_send.at[h, i], g3_recv.at[h, i], r, 1 - c)

            def product(i):
                for h in range(2):
                    p3(i, h).wait_recv()
                lax.fori_loop(0, 2, lambda h, carry: s1(4 * h + i, carry), 0)

            for i in cuts:
                for h, d in moves:
                    p1(i, h, d).start()
            for i in cuts:
                for h, d in moves:
                    p1(i, h, d).wait_recv()
                for h, d in moves:
                    p2(i, h, d).start()
            for i in cuts:
                for h, d in moves:
                    p2(i, h, d).wait_recv()
                for h in range(2):
                    p3(i, h).start()
                if i:
                    product(i - 1)
            product(cuts[-1])
            for i in cuts:
                for h, d in moves:
                    p1(i, h, d).wait_send()
                    p2(i, h, d).wait_send()
                for h in range(2):
                    p3(i, h).wait_send()

        return beta_s

    lax.fori_loop(0, STEPS, step, jnp.zeros((1, 1), F32))

    def drain(jv, carry):
        for h in range(2):
            dst_x = 2 * c + h
            dst_c = x // 2

            @pl.when(jnp.logical_not(jnp.logical_and(dst_x == x, dst_c == c)))
            def _():
                rcopy(piece(jv, h), kbuf.at[jv, :, :, 0:128], k_send.at[jv, h], k_recv.at[jv, 0],
                      row_base + dst_x, dst_c).wait_send()

        for m in range(2):
            src_x = 2 * c + m
            src_c = x // 2

            @pl.when(jnp.logical_not(jnp.logical_and(src_x == x, src_c == c)))
            def _():
                rcopy(piece(jv, 0), kbuf.at[jv, :, :, m * 128:(m + 1) * 128], k_send.at[jv, 0], k_recv.at[jv, m],
                      row_base + src_x, src_c).wait_recv()

        return carry

    lax.fori_loop(0, STEPS + 1, drain, 0)
    cp_k = pltpu.make_async_copy(kbuf, kr_ref, ld_sem.at[0])
    cp_k.start()
    cp_k.wait()


def solution(mesh):
    assert mesh.shape['terms'] == 2 and mesh.shape['rows'] == 64

    def body_fn(wavefunc, left_loc, two_loc, right_loc):
        elem_count = float(wavefunc.size)
        vm = pl.BlockSpec(memory_space=pltpu.VMEM)
        hbm = pl.BlockSpec(memory_space=pl.ANY)
        dma = pltpu.SemaphoreType.DMA
        kr, ab = pl.pallas_call(
            lambda *refs: kernel(elem_count, *refs),
            out_shape=(jax.ShapeDtypeStruct((STEPS + 1, 16, 8, 256), F32), jax.ShapeDtypeStruct((16, 128), F32)),
            in_specs=[hbm, hbm, hbm, vm],
            out_specs=(hbm, vm),
            scratch_shapes=[
                pltpu.VMEM((16, 128, 512), F32),
                pltpu.VMEM((16, 128, 512), F32),
                pltpu.VMEM((128, 128), F32),
                pltpu.VMEM((16, 128, 512), BF16),
                pltpu.VMEM((16, 4, 4, 2, 16, 128), BF16),
                pltpu.VMEM((4, 512, 512), BF16),
                pltpu.VMEM((2, 1024, 512), BF16),
                pltpu.VMEM((NT, 128, 512), BF16),
                pltpu.VMEM((NT, 256, 256), BF16),
                pltpu.VMEM((NT, 2, 16, 16, 128), BF16),
                pltpu.VMEM((2, NT, 256, 128), BF16),
                pltpu.VMEM((4, 256, 128), F32),
                pltpu.VMEM((4, 256, 128), F32),
                pltpu.VMEM((4, 256, 128), F32),
                pltpu.VMEM((3, 256, 128), F32),
                pltpu.VMEM((STEPS + 1, 256, 128), F32),
                pltpu.VMEM((STEPS + 1, 16, 8, 256), F32),
                pltpu.VMEM((4, 8, 128), F32),
                pltpu.VMEM((8, 8, 128), F32),
                pltpu.VMEM((16, 8, 128), F32),
                dma((2,)), dma((2, 16)), dma((6,)), dma((6,)), dma((3,)), dma((3,)), dma((1,)), dma((1,)), dma((3,)), dma((3,)),
                dma((7,)), dma((7,)), dma((15,)), dma((15,)),
                dma((2, 4, 3)), dma((2, 4, 3)), dma((2, 4, 3)), dma((2, 4, 3)), dma((2, 4)), dma((2, 4)),
                dma((STEPS + 1, 2)), dma((STEPS + 1, 2)),
            ],
            compiler_params=pltpu.CompilerParams(has_side_effects=True, vmem_limit_bytes=60 * 1024 * 1024),
        )(wavefunc, left_loc, right_loc.reshape(512, 512), two_loc.reshape(1024, 16))
        krylov = jnp.transpose(kr.reshape(STEPS + 1, 4, 4, 8, 256), (0, 4, 1, 2, 3))
        return krylov, ab[:STEPS, 0], ab[8:8 + STEPS, 0]

    return jax.shard_map(body_fn, mesh=mesh, in_specs=(P(), P('terms'), P('terms'), P('terms', 'rows')),
                         out_specs=(P(None, 'terms', None, None, 'rows'), P(), P()), check_vma=False)
```

```python
import jax
import jax.numpy as jnp
from jax import lax
from jax.experimental import pallas as pl
from jax.experimental.pallas import tpu as pltpu
from jax.sharding import PartitionSpec as P

STEPS = 6
F32 = jnp.float32
BF16 = jnp.bfloat16
MESH = pl.DeviceIdType.MESH
NT = 64


def total(x):
    return jnp.sum(jnp.sum(x, axis=1, keepdims=True), axis=0, keepdims=True)


def blk(i, size):
    return pl.ds(pl.multiple_of(i * size, size), size)


def col_sum(x):
    return jnp.sum(x, axis=0, keepdims=True)


def sq_block(blk):
    out = jnp.zeros((8, 128), F32)
    sq = (blk * blk).reshape(16, 8, 512).sum(axis=0)
    for i in range(4):
        out = out + sq[:, i * 128:(i + 1) * 128]
    return out


def kernel(elem_count, wave_ref, left_ref, right_ref, two_ref, kr_ref, ab_ref,
           slab, nslab, tmp, wide, ut, u_ref, rin, rb, lb, wt, y_ref, z_ref, acc, recv_s, recv_x, vecs, kbuf,
           red_n, red_a, red_b,
           ld_sem, sl_sem, r_send, r_recv, n_send, n_recv, s_send, s_recv, x_send, x_recv, a_send, a_recv,
           b_send, b_recv, g1_send, g1_recv, g2_send, g2_recv, g3_send, g3_recv, k_send, k_recv):
    r = lax.axis_index('rows')
    c = lax.axis_index('terms')
    x = lax.rem(r, 4)
    y = lax.rem(r // 4, 4)
    z = r // 16
    g = r // 4
    row_base = r - x
    z_peers = [lax.rem(z + d, 4) * 16 + y * 4 + x for d in (1, 2, 3)]
    y_peers = [z * 16 + lax.rem(y + d, 4) * 4 + x for d in (1, 2, 3)]
    x_peers = [row_base + lax.rem(x + d, 4) for d in (1, 2, 3)]

    def pair(i, h):
        return pl.ds(8 * h + 2 * i, 2)

    def rcopy(src, dst, ssem, rsem, row, core):
        return pltpu.make_async_remote_copy(src_ref=src, dst_ref=dst, send_sem=ssem, recv_sem=rsem,
                                            device_id=(row, core), device_id_type=MESH)

    me = x * 2 + c
    group = [(row_base + lax.rem(me + d, 8) // 2, lax.rem(me + d, 2)) for d in range(1, 8)]
    plane = [(lax.rem(g + d, 16) * 4 + x, c) for d in range(1, 16)]
    barrier = pltpu.get_barrier_semaphore()
    for peer in group + plane:
        pl.semaphore_signal(barrier, inc=1, device_id=peer, device_id_type=MESH)

    cp_r = pltpu.make_async_copy(right_ref, rin.at[x], ld_sem.at[0])
    cp_r.start()
    n_loads, s_loads = [], []
    for p in range(16):
        rows_n = blk(z, 128)
        n_loads.append(pltpu.make_async_copy(wave_ref.at[rows_n, p // 4, p % 4, :], nslab.at[p], sl_sem.at[0, p]))
    for p in range(16):
        rows_s = blk(x, 128)
        s_loads.append(pltpu.make_async_copy(wave_ref.at[rows_s, p // 4, p % 4, :], slab.at[p], sl_sem.at[1, p]))
    cp_l = pltpu.make_async_copy(left_ref.at[:, blk(x, 128), :], lb, ld_sem.at[1])
    for cp in n_loads + s_loads:
        cp.start()
    cp_l.start()
    cp_r.wait()
    pl.semaphore_wait(barrier, len(group) + len(plane))

    right = row_base + lax.rem(x + 1, 4)
    left = row_base + lax.rem(x + 3, 4)
    xl = lax.rem(x + 3, 4)
    xr = lax.rem(x + 1, 4)
    halves = [pl.ds(0, 256), pl.ds(256, 256)]

    def r_move(i, block, half, row):
        ref = rin.at[block, halves[half], :]
        return rcopy(ref, ref, r_send.at[i], r_recv.at[i], row, c)

    r0 = r_move(0, x, 0, right)
    r1 = r_move(1, x, 1, left)
    r2 = r_move(2, x, 1, right)
    r3 = r_move(3, x, 0, left)
    r4 = r_move(4, xl, 0, right)
    r5 = r_move(5, xr, 1, left)
    for cp in (r0, r1, r2, r3):
        cp.start()

    for cp in n_loads:
        cp.wait()

    ssq = jnp.zeros((8, 128), F32)
    ssq = lax.fori_loop(0, 16, lambda p, acc: acc + sq_block(nslab[p]), ssq)
    red_n[0] = jnp.zeros((8, 128), F32) + total(ssq)
    n_copies = []
    for d, row in enumerate(z_peers):
        cp = rcopy(red_n.at[0], red_n.at[d + 1], n_send.at[d], n_recv.at[d], row, c)
        cp.start()
        n_copies.append(cp)

    lane16 = lax.broadcasted_iota(jnp.int32, (16, 256), 1)
    row16 = lax.broadcasted_iota(jnp.int32, (16, 256), 0)
    e_col = (lane16 // 16 == row16).astype(BF16)
    row_e = lax.broadcasted_iota(jnp.int32, (256, 16), 0)
    lane_e = lax.broadcasted_iota(jnp.int32, (256, 16), 1)
    e_row = (row_e // 16 == lane_e).astype(BF16)
    row_m = lax.broadcasted_iota(jnp.int32, (256, 256), 0)
    lane_m = lax.broadcasted_iota(jnp.int32, (256, 256), 1)
    diag = lax.rem(row_m, 16) == lax.rem(lane_m, 16)

    wide[...] = jnp.dot(two_ref[...], e_col, preferred_element_type=F32).astype(BF16)

    def build_w(kk, carry):
        for i in range(8):
            k = kk * 8 + i
            rows = wide[blk(k, 16), :]
            full = jnp.dot(e_row, rows, preferred_element_type=F32)
            wt[k] = jnp.where(diag, full, 0.0).astype(BF16)
        return carry

    lax.fori_loop(0, NT // 8, build_w, 0)
    r0.wait_recv()
    r4.start()
    r1.wait_recv()
    r5.start()

    for cp in n_copies:
        cp.wait()
    norm = [red_n[lax.rem(z - s + 4, 4)] for s in range(4)]
    scale = jnp.sqrt(((norm[0] + norm[1]) + (norm[2] + norm[3]))[:1, :1] / elem_count)
    for cp in s_loads:
        cp.wait()
    b_lanes = blk(g // 4, 128)
    b_rows = blk(lax.rem(g, 4) * 2 + c, 16)

    def first(p, carry):
        ut[p] = (slab[p] / scale).astype(BF16)
        tmp[...] = jnp.transpose(slab[p, :, b_lanes])
        vecs[0, blk(p, 16), :] = tmp[b_rows, :] / scale
        return carry

    lax.fori_loop(0, 16, first, 0)

    out_lanes = blk(lax.rem(x, 2), 128)

    def piece(jv, h):
        return vecs.at[jv].reshape(16, 16, 128).at[:, h * 8:(h + 1) * 8, :]

    def emit(jv):
        for h in range(2):
            dst_x = 2 * c + h
            dst_c = x // 2
            is_me = jnp.logical_and(dst_x == x, dst_c == c)

            @pl.when(jnp.logical_not(is_me))
            def _():
                rcopy(piece(jv, h), kbuf.at[jv, :, :, out_lanes], k_send.at[jv, h], k_recv.at[jv, lax.rem(x, 2)],
                      row_base + dst_x, dst_c).start()

            @pl.when(is_me)
            def _():
                kbuf[jv, :, :, out_lanes] = vecs[jv].reshape(16, 16, 128)[:, h * 8:(h + 1) * 8, :]

    def build_r(bhi):
        def body(i, carry):
            rows = blk(i, 64)
            lo = rin[2 * bhi, rows, :].astype(F32).reshape(8, 8, 512)
            hi = rin[2 * bhi + 1, rows, :].astype(F32).reshape(8, 8, 512)
            both = jnp.concatenate([lo, hi], axis=1).reshape(128, 512)
            rb[bhi, blk(i, 128), :] = both.astype(BF16)
            return carry

        lax.fori_loop(0, 8, body, 0)

    def put_y(o, bhi, mc, pp):
        o = o.astype(BF16).reshape(32, 16, 256)
        rows = pl.ds(mc * 32, 32)
        y_ref[rows, bhi, 2 * pp] = o[:, :, :128]
        y_ref[rows, bhi, 2 * pp + 1] = o[:, :, 128:]

    def s1_first(bhi):
        def body(i, carry):
            for pp in (i, i + 4):
                w = ut[pl.ds(2 * pp, 2)].reshape(256, 512)
                for mc in range(2):
                    rows = rb[bhi, pl.ds(mc * 512, 512), :]
                    o = lax.dot_general(rows, w, (((1,), (1,)), ((), ())), preferred_element_type=F32)
                    put_y(o, bhi, mc, pp)
            return carry

        lax.fori_loop(0, 4, body, 0)

    def s1(pp):
        w = jnp.concatenate([u_ref[2 * pp + i].reshape(512, 128) for i in range(2)], axis=1)
        for bhi in range(2):
            for mc in range(2):
                put_y(jnp.dot(rb[bhi, pl.ds(mc * 512, 512), :], w, preferred_element_type=F32), bhi, mc, pp)

    for cp in (r2, r3):
        cp.wait_recv()
    emit(0)
    own = x // 2
    build_r(own)
    s1_first(own)
    for cp in (r4, r5):
        cp.wait_recv()
    build_r(1 - own)
    s1_first(1 - own)
    for cp in (r0, r1, r2, r3, r4, r5):
        cp.wait_send()
    cp_l.wait()

    row_id = lax.broadcasted_iota(jnp.int32, (8, 128), 0)
    ab_ref[...] = jnp.zeros_like(ab_ref)

    def pack(p, n, am, rr, ss):
        out = jnp.where(row_id == 0, p, 0.0)
        out = jnp.where(row_id == 1, n, out)
        out = jnp.where(row_id == 2, am, out)
        out = jnp.where(row_id == 3, rr, out)
        return jnp.where(row_id == 4, ss, out)

    def safe_div(num, den):
        ok = den > 0.0
        return jnp.where(ok, num / jnp.where(ok, den, 1.0), 0.0)

    def merge(p, n, am, rr, ss):
        n_all = col_sum(n)
        mean = safe_div(col_sum(am * n), n_all)
        gap = mean - am
        r_all = col_sum(rr + gap * (gap * n - 2.0 * ss))
        return col_sum(p), n_all, mean, r_all, col_sum(ss)

    def step(j, prev_beta):
        def s2(kk, carry):
            for i in range(16):
                k = kk * 16 + i
                rhs = jnp.concatenate([y_ref[k, 0].reshape(256, 128), y_ref[k, 1].reshape(256, 128)], axis=1)
                o = jnp.dot(wt[k], rhs, preferred_element_type=F32).astype(BF16)
                z_ref[0, k] = o[:, :128]
                z_ref[1, k] = o[:, 128:]
            return carry

        lax.fori_loop(0, NT // 16, s2, 0)


        order = [lax.rem(x + d, 4) for d in (2, 1, 3, 0)]

        def s3(lo, first_k, count):
            slices = [blk(pos, 128) for pos in order[lo:lo + 2]]
            outs = [None, None]
            for k0 in range(first_k, first_k + count, 8):
                rhs = jnp.concatenate([lb[pl.ds(k0, 8), :, sl].reshape(1024, 128) for sl in slices], axis=1)
                for bhi in range(2):
                    lhs = jnp.concatenate([z_ref[bhi, k0 + k] for k in range(8)], axis=1)
                    o = jnp.dot(lhs, rhs, preferred_element_type=F32)
                    outs[bhi] = o if outs[bhi] is None else outs[bhi] + o
            for n in range(2):
                for bhi in range(2):
                    part = outs[bhi][:, n * 128:(n + 1) * 128]
                    acc[bhi, lo + n] = acc[bhi, lo + n] + part if first_k else part

        acc_o = acc.at[1 - c]
        acc_m = acc.at[c]
        s_copies = []
        for n in range(2):
            two = pl.ds(2 * n, 2)
            s_copies.append(rcopy(acc_o.at[two], recv_s.at[two], s_send.at[n], s_recv.at[n], r, 1 - c))
        x_copies = []
        for n in range(3):
            x_copies.append(rcopy(acc_m.at[n], recv_x.at[n], x_send.at[n], x_recv.at[n], row_base + order[n], c))
        s3(0, 0, NT)
        s_copies[0].start()
        s3(2, 0, NT // 2)
        s_copies[0].wait_recv()
        for n in range(2):
            acc_m[n] += recv_s[n]
            x_copies[n].start()
        s3(2, NT // 2, NT // 2)
        s_copies[1].start()
        s_copies[1].wait_recv()
        acc_m[2] += recv_s[2]
        x_copies[2].start()
        w_own = acc_m[3] + recv_s[3]
        for cp in s_copies:
            cp.wait_send()
        for cp in x_copies:
            cp.wait()
        w_vec = (w_own + recv_x[0]) + (recv_x[1] + recv_x[2])
        v_cur = vecs[j]
        v_old = vecs[lax.max(j - 1, 0)]

        w_res = w_vec - prev_beta * v_old
        n_loc = total(v_cur * v_cur)
        a_loc = safe_div(total(w_res * v_cur), n_loc)
        e_loc = w_res - a_loc * v_cur
        red_a[0] = pack(total(w_vec * v_cur), n_loc, a_loc, total(e_loc * e_loc), total(e_loc * v_cur))

        a_copies = [rcopy(red_a.at[0], red_a.at[d + 1], a_send.at[d], a_recv.at[d], *peer) for d, peer in enumerate(group)]
        for cp in a_copies:
            cp.start()
        for cp in a_copies:
            cp.wait()
        blocks = [red_a[lax.rem(me - s + 8, 8)] for s in range(8)]

        def gather_rows(blks, i):
            return jnp.concatenate([bk[i:i + 1, :] for bk in blks], axis=0)

        red_b[0] = pack(*merge(*[gather_rows(blocks, i) for i in range(5)]))
        b_copies = [rcopy(red_b.at[0], red_b.at[d + 1], b_send.at[d], b_recv.at[d], *peer) for d, peer in enumerate(plane)]
        for cp in b_copies:
            cp.start()
        for cp in b_copies:
            cp.wait()
        blocks = [red_b[lax.rem(g - s + 16, 16)] for s in range(16)]
        p_all, n_all, a_all, r_all, s_all = [gather_rows(blocks, i) for i in range(5)]
        alpha = col_sum(p_all) / elem_count
        gap = alpha - a_all
        beta = jnp.sqrt(col_sum(r_all + gap * (gap * n_all - 2.0 * s_all)) / elem_count)
        alpha_s = alpha[:, :1]
        beta_s = beta[:, :1]

        v_new = (w_vec - alpha_s * v_cur - prev_beta * v_old) / beta_s
        vecs[j + 1] = v_new
        ab_ref[pl.ds(j, 1), :] = alpha
        ab_ref[pl.ds(8 + j, 1), :] = beta

        emit(j + 1)

        @pl.when(j < STEPS - 1)
        def _():
            u_ref[:, z, y, c] = v_new.astype(BF16).reshape(16, 16, 128)
            moves = [(h, d) for h in range(2) for d in range(3)]
            cuts = range(4)

            def move(sems, h, i, d, ref, across):
                row = z_peers[d] if across else y_peers[d]
                return rcopy(ref, ref, sems[0].at[h, i, d], sems[1].at[h, i, d], row, c)

            def p1(i, h, d):
                ref = u_ref.at[pair(i, h), z, y, c]
                return move((g1_send, g1_recv), h, i, d, ref, h == 0)

            def p2(i, h, d):
                ref = u_ref.at[pair(i, h), z, :, c] if h else u_ref.at[pair(i, h), :, y, c]
                return move((g2_send, g2_recv), h, i, d, ref, h == 1)

            def p3(i, h):
                ref = u_ref.at[pair(i, h), :, :, c]
                return rcopy(ref, ref, g3_send.at[h, i], g3_recv.at[h, i], r, 1 - c)

            def product(i):
                for h in range(2):
                    p3(i, h).wait_recv()
                s1(i)
                s1(4 + i)

            for i in cuts:
                for h, d in moves:
                    p1(i, h, d).start()
            for i in cuts:
                for h, d in moves:
                    p1(i, h, d).wait_recv()
                for h, d in moves:
                    p2(i, h, d).start()
            for i in cuts:
                for h, d in moves:
                    p2(i, h, d).wait_recv()
                for h in range(2):
                    p3(i, h).start()
                if i:
                    product(i - 1)
            product(cuts[-1])
            for i in cuts:
                for h, d in moves:
                    p1(i, h, d).wait_send()
                    p2(i, h, d).wait_send()
                for h in range(2):
                    p3(i, h).wait_send()

        return beta_s

    lax.fori_loop(0, STEPS, step, jnp.zeros((1, 1), F32))

    def drain(jv, carry):
        for h in range(2):
            dst_x = 2 * c + h
            dst_c = x // 2

            @pl.when(jnp.logical_not(jnp.logical_and(dst_x == x, dst_c == c)))
            def _():
                rcopy(piece(jv, h), kbuf.at[jv, :, :, 0:128], k_send.at[jv, h], k_recv.at[jv, 0],
                      row_base + dst_x, dst_c).wait_send()

        for m in range(2):
            src_x = 2 * c + m
            src_c = x // 2

            @pl.when(jnp.logical_not(jnp.logical_and(src_x == x, src_c == c)))
            def _():
                rcopy(piece(jv, 0), kbuf.at[jv, :, :, m * 128:(m + 1) * 128], k_send.at[jv, 0], k_recv.at[jv, m],
                      row_base + src_x, src_c).wait_recv()

        return carry

    lax.fori_loop(0, STEPS + 1, drain, 0)
    cp_k = pltpu.make_async_copy(kbuf, kr_ref, ld_sem.at[0])
    cp_k.start()
    cp_k.wait()


def solution(mesh):
    assert mesh.shape['terms'] == 2 and mesh.shape['rows'] == 64

    def body_fn(wavefunc, left_loc, two_loc, right_loc):
        elem_count = float(wavefunc.size)
        vm = pl.BlockSpec(memory_space=pltpu.VMEM)
        hbm = pl.BlockSpec(memory_space=pl.ANY)
        dma = pltpu.SemaphoreType.DMA
        kr, ab = pl.pallas_call(
            lambda *refs: kernel(elem_count, *refs),
            out_shape=(jax.ShapeDtypeStruct((STEPS + 1, 16, 8, 256), F32), jax.ShapeDtypeStruct((16, 128), F32)),
            in_specs=[hbm, hbm, hbm, vm],
            out_specs=(hbm, vm),
            scratch_shapes=[
                pltpu.VMEM((16, 128, 512), F32),
                pltpu.VMEM((16, 128, 512), F32),
                pltpu.VMEM((128, 128), F32),
                pltpu.VMEM((1024, 256), BF16),
                pltpu.VMEM((16, 128, 512), BF16),
                pltpu.VMEM((16, 4, 4, 2, 16, 128), BF16),
                pltpu.VMEM((4, 512, 512), BF16),
                pltpu.VMEM((2, 1024, 512), BF16),
                pltpu.VMEM((NT, 128, 512), BF16),
                pltpu.VMEM((NT, 256, 256), BF16),
                pltpu.VMEM((NT, 2, 16, 16, 128), BF16),
                pltpu.VMEM((2, NT, 256, 128), BF16),
                pltpu.VMEM((2, 4, 256, 128), F32),
                pltpu.VMEM((4, 256, 128), F32),
                pltpu.VMEM((3, 256, 128), F32),
                pltpu.VMEM((STEPS + 1, 256, 128), F32),
                pltpu.VMEM((STEPS + 1, 16, 8, 256), F32),
                pltpu.VMEM((4, 8, 128), F32),
                pltpu.VMEM((8, 8, 128), F32),
                pltpu.VMEM((16, 8, 128), F32),
                dma((2,)), dma((2, 16)), dma((6,)), dma((6,)), dma((3,)), dma((3,)), dma((2,)), dma((2,)), dma((3,)), dma((3,)),
                dma((7,)), dma((7,)), dma((15,)), dma((15,)),
                dma((2, 4, 3)), dma((2, 4, 3)), dma((2, 4, 3)), dma((2, 4, 3)), dma((2, 4)), dma((2, 4)),
                dma((STEPS + 1, 2)), dma((STEPS + 1, 2)),
            ],
            compiler_params=pltpu.CompilerParams(has_side_effects=True, collective_id=0, vmem_limit_bytes=60 * 1024 * 1024),
        )(wavefunc, left_loc, right_loc.reshape(512, 512), two_loc.reshape(1024, 16))
        krylov = jnp.transpose(kr.reshape(STEPS + 1, 4, 4, 8, 256), (0, 4, 1, 2, 3))
        return krylov, ab[:STEPS, 0], ab[8:8 + STEPS, 0]

    return jax.shard_map(body_fn, mesh=mesh, in_specs=(P(), P('terms'), P('terms'), P('terms', 'rows')),
                         out_specs=(P(None, 'terms', None, None, 'rows'), P(), P()), check_vma=False)
```

```python
import jax
import jax.numpy as jnp
from jax import lax
from jax.experimental import pallas as pl
from jax.experimental.pallas import tpu as pltpu
from jax.sharding import PartitionSpec as P

STEPS = 6
F32 = jnp.float32
BF16 = jnp.bfloat16
MESH = pl.DeviceIdType.MESH
NT = 64
BOND = 512
SLICE = 128
BLK = 16
QB = 256


def total(x):
    return jnp.sum(jnp.sum(x, axis=1, keepdims=True), axis=0, keepdims=True)


def blk(i, size):
    return pl.ds(pl.multiple_of(i * size, size), size)


def col_sum(x):
    return jnp.sum(x, axis=0, keepdims=True)


def sq_block(blk):
    out = jnp.zeros((8, SLICE), F32)
    sq = (blk * blk).reshape(BLK, 8, BOND).sum(axis=0)
    for i in range(4):
        out = out + sq[:, i * SLICE:(i + 1) * SLICE]
    return out


def kernel(elem_count, wave_ref, left_ref, right_ref, two_ref, kr_ref, ab_ref,
           slab, nslab, tmp, wide, ut, u_ref, rin, rb, lb, wt, y_ref, z_ref, acc, recv_s, recv_x, vecs, kbuf, wg, vg,
           red_n, red_a, red_b,
           ld_sem, sl_sem, r_send, r_recv, n_send, n_recv, s_send, s_recv, x_send, x_recv, a_send, a_recv,
           b_send, b_recv, g1_send, g1_recv, g2_send, g2_recv, g3_send, g3_recv, k_send, k_recv):
    r = lax.axis_index('rows')
    c = lax.axis_index('terms')
    x = lax.rem(r, 4)
    y = lax.rem(r // 4, 4)
    z = r // BLK
    g = r // 4
    row_base = r - x
    z_peers = [lax.rem(z + d, 4) * BLK + y * 4 + x for d in (1, 2, 3)]
    y_peers = [z * BLK + lax.rem(y + d, 4) * 4 + x for d in (1, 2, 3)]
    x_peers = [row_base + lax.rem(x + d, 4) for d in (1, 2, 3)]

    def pair(i, h):
        return pl.ds(8 * h + 2 * i, 2)

    def rcopy(src, dst, ssem, rsem, row, core):
        return pltpu.make_async_remote_copy(src_ref=src, dst_ref=dst, send_sem=ssem, recv_sem=rsem,
                                            device_id=(row, core), device_id_type=MESH)

    me = x * 2 + c
    group = [(row_base + lax.rem(me + d, 8) // 2, lax.rem(me + d, 2)) for d in range(1, 8)]
    plane = [(lax.rem(g + d, BLK) * 4 + x, c) for d in range(1, BLK)]
    barrier = pltpu.get_barrier_semaphore()
    for peer in group + plane:
        pl.semaphore_signal(barrier, inc=1, device_id=peer, device_id_type=MESH)

    cp_r = pltpu.make_async_copy(right_ref, rin.at[x], ld_sem.at[0])
    cp_r.start()
    n_loads, s_loads = [], []
    for p in range(BLK):
        rows_n = blk(z, SLICE)
        n_loads.append(pltpu.make_async_copy(wave_ref.at[rows_n, p // 4, p % 4, :], nslab.at[p], sl_sem.at[0, p]))
    for p in range(BLK):
        rows_s = blk(x, SLICE)
        s_loads.append(pltpu.make_async_copy(wave_ref.at[rows_s, p // 4, p % 4, :], slab.at[p], sl_sem.at[1, p]))
    cp_l = pltpu.make_async_copy(left_ref.at[:, blk(x, SLICE), :], lb, ld_sem.at[1])
    for cp in n_loads + s_loads:
        cp.start()
    cp_l.start()
    cp_r.wait()
    pl.semaphore_wait(barrier, len(group) + len(plane))

    right = row_base + lax.rem(x + 1, 4)
    left = row_base + lax.rem(x + 3, 4)
    xl = lax.rem(x + 3, 4)
    xr = lax.rem(x + 1, 4)
    halves = [pl.ds(0, QB), pl.ds(QB, QB)]

    def r_move(i, block, half, row):
        ref = rin.at[block, halves[half], :]
        return rcopy(ref, ref, r_send.at[i], r_recv.at[i], row, c)

    r0 = r_move(0, x, 0, right)
    r1 = r_move(1, x, 1, left)
    r2 = r_move(2, x, 1, right)
    r3 = r_move(3, x, 0, left)
    r4 = r_move(4, xl, 0, right)
    r5 = r_move(5, xr, 1, left)
    for cp in (r0, r1, r2, r3):
        cp.start()

    for cp in n_loads:
        cp.wait()

    ssq = jnp.zeros((8, SLICE), F32)
    ssq = lax.fori_loop(0, BLK, lambda p, acc: acc + sq_block(nslab[p]), ssq)
    red_n[0] = jnp.zeros((8, SLICE), F32) + total(ssq)
    n_copies = []
    for d, row in enumerate(z_peers):
        cp = rcopy(red_n.at[0], red_n.at[d + 1], n_send.at[d], n_recv.at[d], row, c)
        cp.start()
        n_copies.append(cp)

    lane16 = lax.broadcasted_iota(jnp.int32, (BLK, QB), 1)
    row16 = lax.broadcasted_iota(jnp.int32, (BLK, QB), 0)
    e_col = (lane16 // BLK == row16).astype(BF16)
    row_e = lax.broadcasted_iota(jnp.int32, (QB, BLK), 0)
    lane_e = lax.broadcasted_iota(jnp.int32, (QB, BLK), 1)
    e_row = (row_e // BLK == lane_e).astype(BF16)
    row_m = lax.broadcasted_iota(jnp.int32, (QB, QB), 0)
    lane_m = lax.broadcasted_iota(jnp.int32, (QB, QB), 1)
    diag = lax.rem(row_m, BLK) == lax.rem(lane_m, BLK)

    wide[...] = jnp.dot(two_ref[...], e_col, preferred_element_type=F32).astype(BF16)

    def build_w(kk, carry):
        for i in range(8):
            k = kk * 8 + i
            rows = wide[blk(k, BLK), :]
            full = jnp.dot(e_row, rows, preferred_element_type=F32)
            wt[k] = jnp.where(diag, full, 0.0).astype(BF16)
        return carry

    lax.fori_loop(0, NT // 8, build_w, 0)
    r0.wait_recv()
    r4.start()
    r1.wait_recv()
    r5.start()

    for cp in n_copies:
        cp.wait()
    norm = [red_n[lax.rem(z - s + 4, 4)] for s in range(4)]
    scale = jnp.sqrt(((norm[0] + norm[1]) + (norm[2] + norm[3]))[:1, :1] / elem_count)
    for cp in s_loads:
        cp.wait()
    vg[1] = jnp.zeros_like(vg[1])

    def first(p, carry):
        ut[p] = (slab[p] / scale).astype(BF16)
        ut[p + 8] = (slab[p + 8] / scale).astype(BF16)
        for n in range(4):
            tmp[n] = jnp.transpose(slab[p, :, n * SLICE:(n + 1) * SLICE])
        tmp[4] = jnp.transpose(slab[p + 8, :, blk(z, SLICE)])
        for n in range(4):
            vg[0, 0, n, blk(p, BLK), :] = tmp[n, blk(y * 2 + c, BLK), :] / scale
            vg[0, 1, n, blk(p, BLK), :] = tmp[4, blk(n * 2 + c, BLK), :] / scale
        return carry

    lax.fori_loop(0, 8, first, 0)
    vecs[0, :SLICE] = vg[0, 0, z]
    vecs[0, SLICE:] = vg[0, 1, y]

    out_lanes = blk(lax.rem(x, 2), SLICE)

    def piece(jv, h):
        return vecs.at[jv].reshape(BLK, BLK, SLICE).at[:, h * 8:(h + 1) * 8, :]

    def emit(jv):
        for h in range(2):
            dst_x = 2 * c + h
            dst_c = x // 2
            is_me = jnp.logical_and(dst_x == x, dst_c == c)

            @pl.when(jnp.logical_not(is_me))
            def _():
                rcopy(piece(jv, h), kbuf.at[jv, :, :, out_lanes], k_send.at[jv, h], k_recv.at[jv, lax.rem(x, 2)],
                      row_base + dst_x, dst_c).start()

            @pl.when(is_me)
            def _():
                kbuf[jv, :, :, out_lanes] = vecs[jv].reshape(BLK, BLK, SLICE)[:, h * 8:(h + 1) * 8, :]

    def build_r(bhi):
        def body(i, carry):
            rows = blk(i, 64)
            lo = rin[2 * bhi, rows, :].astype(F32).reshape(8, 8, BOND)
            hi = rin[2 * bhi + 1, rows, :].astype(F32).reshape(8, 8, BOND)
            both = jnp.concatenate([lo, hi], axis=1).reshape(SLICE, BOND)
            rb[bhi, blk(i, SLICE), :] = both.astype(BF16)
            return carry

        lax.fori_loop(0, 8, body, 0)

    def put_y(o, bhi, mc, pp):
        o = o.astype(BF16).reshape(32, BLK, QB)
        rows = pl.ds(mc * 32, 32)
        y_ref[rows, bhi, 2 * pp] = o[:, :, :SLICE]
        y_ref[rows, bhi, 2 * pp + 1] = o[:, :, SLICE:]

    def s1_first(bhi):
        def body(i, carry):
            for pp in (i, i + 4):
                w = ut[pl.ds(2 * pp, 2)].reshape(QB, BOND)
                for mc in range(2):
                    rows = rb[bhi, pl.ds(mc * BOND, BOND), :]
                    o = lax.dot_general(rows, w, (((1,), (1,)), ((), ())), preferred_element_type=F32)
                    put_y(o, bhi, mc, pp)
            return carry

        lax.fori_loop(0, 4, body, 0)

    def s1(pp):
        w = jnp.concatenate([u_ref[2 * pp + i].reshape(BOND, SLICE) for i in range(2)], axis=1)
        for bhi in range(2):
            for mc in range(2):
                put_y(jnp.dot(rb[bhi, pl.ds(mc * BOND, BOND), :], w, preferred_element_type=F32), bhi, mc, pp)

    for cp in (r2, r3):
        cp.wait_recv()
    emit(0)
    own = x // 2
    build_r(own)
    s1_first(own)
    for cp in (r4, r5):
        cp.wait_recv()
    build_r(1 - own)
    s1_first(1 - own)
    for cp in (r0, r1, r2, r3, r4, r5):
        cp.wait_send()
    cp_l.wait()

    row_id = lax.broadcasted_iota(jnp.int32, (8, SLICE), 0)
    ab_ref[...] = jnp.zeros_like(ab_ref)

    def pack(p, n, am, rr, ss):
        out = jnp.where(row_id == 0, p, 0.0)
        out = jnp.where(row_id == 1, n, out)
        out = jnp.where(row_id == 2, am, out)
        out = jnp.where(row_id == 3, rr, out)
        return jnp.where(row_id == 4, ss, out)

    def safe_div(num, den):
        ok = den > 0.0
        return jnp.where(ok, num / jnp.where(ok, den, 1.0), 0.0)

    def merge(p, n, am, rr, ss):
        n_all = col_sum(n)
        mean = safe_div(col_sum(am * n), n_all)
        gap = mean - am
        r_all = col_sum(rr + gap * (gap * n - 2.0 * ss))
        return col_sum(p), n_all, mean, r_all, col_sum(ss)

    def step(j, prev_beta):
        def s2(kk, carry):
            for i in range(BLK):
                k = kk * BLK + i
                rhs = jnp.concatenate([y_ref[k, 0].reshape(QB, SLICE), y_ref[k, 1].reshape(QB, SLICE)], axis=1)
                o = jnp.dot(wt[k], rhs, preferred_element_type=F32).astype(BF16)
                z_ref[0, k] = o[:, :SLICE]
                z_ref[1, k] = o[:, SLICE:]
            return carry

        lax.fori_loop(0, NT // BLK, s2, 0)


        order = [lax.rem(x + d, 4) for d in (2, 1, 3, 0)]

        def s3(bhi, out, lo):
            slices = [blk(pos, SLICE) for pos in order[lo:lo + 2]]
            outs = [None, None]
            for k0 in range(0, NT // 2, 8):
                for kh in range(2):
                    ks = k0 + kh * NT // 2
                    rhs = jnp.concatenate([lb[pl.ds(ks, 8), :, sl].reshape(1024, SLICE) for sl in slices], axis=1)
                    lhs = jnp.concatenate([z_ref[bhi, ks + k] for k in range(8)], axis=1)
                    o = jnp.dot(lhs, rhs, preferred_element_type=F32)
                    outs[kh] = o if outs[kh] is None else outs[kh] + o
            for n in range(2):
                cols = slice(n * SLICE, (n + 1) * SLICE)
                out[lo + n] = outs[0][:, cols] - (0.0 - outs[1][:, cols])

        acc_o = acc.at[1 - c]
        acc_m = acc.at[c]
        s_copies = []
        for n in range(2):
            two = pl.ds(2 * n, 2)
            s_copies.append(rcopy(acc_o.at[two], recv_s.at[two], s_send.at[n], s_recv.at[n], r, 1 - c))
        x_copies = []
        for n in range(3):
            x_copies.append(rcopy(acc_m.at[n], recv_x.at[n], x_send.at[n], x_recv.at[n], row_base + order[n], c))
        s3(1 - c, acc_o, 0)
        s_copies[0].start()
        s3(c, acc_m, 0)
        s_copies[0].wait_recv()
        for n in range(2):
            acc_m[n] += recv_s[n]
            x_copies[n].start()
        s3(1 - c, acc_o, 2)
        s_copies[1].start()
        s3(c, acc_m, 2)
        s_copies[1].wait_recv()
        acc_m[2] += recv_s[2]
        x_copies[2].start()
        w_own = acc_m[3] + recv_s[3]
        for cp in s_copies:
            cp.wait_send()
        for cp in x_copies:
            cp.wait()
        w_vec = (w_own + recv_x[0]) + (recv_x[1] + recv_x[2])
        v_cur = vecs[j]
        v_old = vecs[lax.max(j - 1, 0)]

        w_res = w_vec - prev_beta * v_old
        n_loc = total(v_cur * v_cur)
        a_loc = safe_div(total(w_res * v_cur), n_loc)
        e_loc = w_res - a_loc * v_cur
        red_a[0] = pack(total(w_vec * v_cur), n_loc, a_loc, total(e_loc * e_loc), total(e_loc * v_cur))

        a_copies = [rcopy(red_a.at[0], red_a.at[d + 1], a_send.at[d], a_recv.at[d], *peer) for d, peer in enumerate(group)]
        for cp in a_copies:
            cp.start()

        wg[0, z] = w_vec[:SLICE]
        wg[1, y] = w_vec[SLICE:]
        near = []
        for d in range(3):
            near.append(rcopy(wg.at[0, z], wg.at[0, z], g1_send.at[0, d], g1_recv.at[0, d], z_peers[d], c))
            near.append(rcopy(wg.at[1, y], wg.at[1, y], g1_send.at[1, d], g1_recv.at[1, d], y_peers[d], c))

        @pl.when(j < STEPS - 1)
        def _():
            for cp in near:
                cp.start()

        for cp in a_copies:
            cp.wait()
        blocks = [red_a[lax.rem(me - s + 8, 8)] for s in range(8)]

        def gather_rows(blks, i):
            return jnp.concatenate([bk[i:i + 1, :] for bk in blks], axis=0)

        par = lax.rem(j, 2)
        red_b[par, 0] = pack(*merge(*[gather_rows(blocks, i) for i in range(5)]))
        b_copies = []
        for d, peer in enumerate(plane):
            b_copies.append(rcopy(red_b.at[par, 0], red_b.at[par, d + 1], b_send.at[par, d], b_recv.at[par, d], *peer))
        for cp in b_copies:
            cp.start()
        for cp in b_copies:
            cp.wait()
        blocks = [red_b[par, lax.rem(g - s + BLK, BLK)] for s in range(BLK)]
        p_all, n_all, a_all, r_all, s_all = [gather_rows(blocks, i) for i in range(5)]
        alpha = col_sum(p_all) / elem_count
        gap = alpha - a_all
        beta = jnp.sqrt(col_sum(r_all + gap * (gap * n_all - 2.0 * s_all)) / elem_count)
        alpha_s = alpha[:, :1]
        beta_s = beta[:, :1]

        v_new = (w_vec - alpha_s * v_cur - prev_beta * v_old) / beta_s
        vecs[j + 1] = v_new
        ab_ref[pl.ds(j, 1), :] = alpha
        ab_ref[pl.ds(8 + j, 1), :] = beta

        emit(j + 1)

        @pl.when(j < STEPS - 1)
        def _():
            for cp in near:
                cp.wait()
            new = lax.rem(j + 1, 2)
            for h in range(2):
                for n in range(4):
                    v = (wg[h, n] - alpha_s * vg[1 - new, h, n] - prev_beta * vg[new, h, n]) / beta_s
                    vg[new, h, n] = v
                    at = (z, n) if h else (n, y)
                    u_ref[pl.ds(8 * h, 8), at[0], at[1], c] = v.astype(BF16).reshape(8, BLK, SLICE)
            moves = [(h, d) for h in range(2) for d in range(3)]
            cuts = range(4)

            def move(sems, h, i, d, ref, across):
                row = z_peers[d] if across else y_peers[d]
                return rcopy(ref, ref, sems[0].at[h, i, d], sems[1].at[h, i, d], row, c)

            def p2(i, h, d):
                ref = u_ref.at[pair(i, h), z, :, c] if h else u_ref.at[pair(i, h), :, y, c]
                return move((g2_send, g2_recv), h, i, d, ref, h == 1)

            def p3(i, h):
                ref = u_ref.at[pair(i, h), :, :, c]
                return rcopy(ref, ref, g3_send.at[h, i], g3_recv.at[h, i], r, 1 - c)

            def product(i):
                for h in range(2):
                    p3(i, h).wait_recv()
                s1(i)
                s1(4 + i)

            for i in cuts:
                for h, d in moves:
                    p2(i, h, d).start()
            for i in cuts:
                for h, d in moves:
                    p2(i, h, d).wait_recv()
                for h in range(2):
                    p3(i, h).start()
                if i:
                    product(i - 1)
            product(cuts[-1])
            for i in cuts:
                for h, d in moves:
                    p2(i, h, d).wait_send()
                for h in range(2):
                    p3(i, h).wait_send()

        return beta_s

    lax.fori_loop(0, STEPS, step, jnp.zeros((1, 1), F32))

    def drain(jv, carry):
        for h in range(2):
            dst_x = 2 * c + h
            dst_c = x // 2

            @pl.when(jnp.logical_not(jnp.logical_and(dst_x == x, dst_c == c)))
            def _():
                rcopy(piece(jv, h), kbuf.at[jv, :, :, 0:SLICE], k_send.at[jv, h], k_recv.at[jv, 0],
                      row_base + dst_x, dst_c).wait_send()

        for m in range(2):
            src_x = 2 * c + m
            src_c = x // 2

            @pl.when(jnp.logical_not(jnp.logical_and(src_x == x, src_c == c)))
            def _():
                rcopy(piece(jv, 0), kbuf.at[jv, :, :, m * SLICE:(m + 1) * SLICE], k_send.at[jv, 0], k_recv.at[jv, m],
                      row_base + src_x, src_c).wait_recv()

        return carry

    lax.fori_loop(0, STEPS + 1, drain, 0)
    cp_k = pltpu.make_async_copy(kbuf, kr_ref, ld_sem.at[0])
    cp_k.start()
    cp_k.wait()


def solution(mesh):
    assert mesh.shape['terms'] == 2 and mesh.shape['rows'] == 64

    def body_fn(wavefunc, left_loc, two_loc, right_loc):
        elem_count = float(wavefunc.size)
        vm = pl.BlockSpec(memory_space=pltpu.VMEM)
        hbm = pl.BlockSpec(memory_space=pl.ANY)
        dma = pltpu.SemaphoreType.DMA
        kr, ab = pl.pallas_call(
            lambda *refs: kernel(elem_count, *refs),
            out_shape=(jax.ShapeDtypeStruct((STEPS + 1, BLK, 8, QB), F32), jax.ShapeDtypeStruct((BLK, SLICE), F32)),
            in_specs=[hbm, hbm, hbm, vm],
            out_specs=(hbm, vm),
            scratch_shapes=[
                pltpu.VMEM((BLK, SLICE, BOND), F32),
                pltpu.VMEM((BLK, SLICE, BOND), F32),
                pltpu.VMEM((5, SLICE, SLICE), F32),
                pltpu.VMEM((1024, QB), BF16),
                pltpu.VMEM((BLK, SLICE, BOND), BF16),
                pltpu.VMEM((BLK, 4, 4, 2, BLK, SLICE), BF16),
                pltpu.VMEM((4, BOND, BOND), BF16),
                pltpu.VMEM((2, 1024, BOND), BF16),
                pltpu.VMEM((NT, SLICE, BOND), BF16),
                pltpu.VMEM((NT, QB, QB), BF16),
                pltpu.VMEM((NT, 2, BLK, BLK, SLICE), BF16),
                pltpu.VMEM((2, NT, QB, SLICE), BF16),
                pltpu.VMEM((2, 4, QB, SLICE), F32),
                pltpu.VMEM((4, QB, SLICE), F32),
                pltpu.VMEM((3, QB, SLICE), F32),
                pltpu.VMEM((STEPS + 1, QB, SLICE), F32),
                pltpu.VMEM((STEPS + 1, BLK, 8, QB), F32),
                pltpu.VMEM((2, 4, SLICE, SLICE), F32),
                pltpu.VMEM((2, 2, 4, SLICE, SLICE), F32),
                pltpu.VMEM((4, 8, SLICE), F32),
                pltpu.VMEM((8, 8, SLICE), F32),
                pltpu.VMEM((2, BLK, 8, SLICE), F32),
                dma((2,)), dma((2, BLK)), dma((6,)), dma((6,)), dma((3,)), dma((3,)), dma((2,)), dma((2,)), dma((3,)), dma((3,)),
                dma((7,)), dma((7,)), dma((2, 15)), dma((2, 15)),
                dma((2, 3)), dma((2, 3)), dma((2, 4, 3)), dma((2, 4, 3)), dma((2, 4)), dma((2, 4)),
                dma((STEPS + 1, 2)), dma((STEPS + 1, 2)),
            ],
            compiler_params=pltpu.CompilerParams(has_side_effects=True, collective_id=0, vmem_limit_bytes=60 * 1024 * 1024),
        )(wavefunc, left_loc, right_loc.reshape(BOND, BOND), two_loc.reshape(1024, BLK))
        krylov = jnp.transpose(kr.reshape(STEPS + 1, 4, 4, 8, QB), (0, 4, 1, 2, 3))
        return krylov, ab[:STEPS, 0], ab[8:8 + STEPS, 0]

    return jax.shard_map(body_fn, mesh=mesh, in_specs=(P(), P('terms'), P('terms'), P('terms', 'rows')),
                         out_specs=(P(None, 'terms', None, None, 'rows'), P(), P()), check_vma=False)
```

```python
import jax
import jax.numpy as jnp
from jax import lax
from jax.experimental import pallas as pl
from jax.experimental.pallas import tpu as pltpu
from jax.sharding import PartitionSpec as P

STEPS = 6
F32 = jnp.float32
BF16 = jnp.bfloat16
MESH = pl.DeviceIdType.MESH
NT = 64
BOND = 512
SLICE = 128
BLK = 16
QB = 256


def total(x):
    return jnp.sum(jnp.sum(x, axis=1, keepdims=True), axis=0, keepdims=True)


def blk(i, size):
    return pl.ds(pl.multiple_of(i * size, size), size)


def col_sum(x):
    return jnp.sum(x, axis=0, keepdims=True)


def sq_block(blk):
    out = jnp.zeros((8, SLICE), F32)
    sq = (blk * blk).reshape(BLK, 8, BOND).sum(axis=0)
    for i in range(4):
        out = out + sq[:, i * SLICE:(i + 1) * SLICE]
    return out


def kernel(elem_count, wave_ref, left_ref, right_ref, two_ref, kr_ref, ab_ref,
           slab, nslab, tmp, wide, ut, u_ref, rin, rb, lb, wt, y_ref, z_ref, acc, recv_s, recv_x, vecs, kbuf, wg, vg, wq, vq,
           red_n, red_a, red_b,
           ld_sem, sl_sem, r_send, r_recv, n_send, n_recv, s_send, s_recv, x_send, x_recv, a_send, a_recv,
           b_send, b_recv, g1_send, g1_recv, f_send, f_recv, g2_send, g2_recv, g3_send, g3_recv, k_send, k_recv):
    r = lax.axis_index('rows')
    c = lax.axis_index('terms')
    x = lax.rem(r, 4)
    y = lax.rem(r // 4, 4)
    z = r // BLK
    g = r // 4
    row_base = r - x
    z_peers = [lax.rem(z + d, 4) * BLK + y * 4 + x for d in (1, 2, 3)]
    y_peers = [z * BLK + lax.rem(y + d, 4) * 4 + x for d in (1, 2, 3)]
    x_peers = [row_base + lax.rem(x + d, 4) for d in (1, 2, 3)]

    def pair(i, h):
        return pl.ds(8 * h + 2 * i, 2)

    def rcopy(src, dst, ssem, rsem, row, core):
        return pltpu.make_async_remote_copy(src_ref=src, dst_ref=dst, send_sem=ssem, recv_sem=rsem,
                                            device_id=(row, core), device_id_type=MESH)

    me = x * 2 + c
    group = [(row_base + lax.rem(me + d, 8) // 2, lax.rem(me + d, 2)) for d in range(1, 8)]
    plane = [(lax.rem(g + d, BLK) * 4 + x, c) for d in range(1, BLK)]
    barrier = pltpu.get_barrier_semaphore()
    for peer in group + plane:
        pl.semaphore_signal(barrier, inc=1, device_id=peer, device_id_type=MESH)

    cp_r = pltpu.make_async_copy(right_ref, rin.at[x], ld_sem.at[0])
    cp_r.start()
    n_loads, s_loads = [], []
    for p in range(BLK):
        rows_n = blk(z, SLICE)
        n_loads.append(pltpu.make_async_copy(wave_ref.at[rows_n, p // 4, p % 4, :], nslab.at[p], sl_sem.at[0, p]))
    for p in range(BLK):
        rows_s = blk(x, SLICE)
        s_loads.append(pltpu.make_async_copy(wave_ref.at[rows_s, p // 4, p % 4, :], slab.at[p], sl_sem.at[1, p]))
    cp_l = pltpu.make_async_copy(left_ref.at[:, blk(x, SLICE), :], lb, ld_sem.at[1])
    for cp in n_loads + s_loads:
        cp.start()
    cp_l.start()
    cp_r.wait()
    pl.semaphore_wait(barrier, len(group) + len(plane))

    right = row_base + lax.rem(x + 1, 4)
    left = row_base + lax.rem(x + 3, 4)
    xl = lax.rem(x + 3, 4)
    xr = lax.rem(x + 1, 4)
    halves = [pl.ds(0, QB), pl.ds(QB, QB)]

    def r_move(i, block, half, row):
        ref = rin.at[block, halves[half], :]
        return rcopy(ref, ref, r_send.at[i], r_recv.at[i], row, c)

    r0 = r_move(0, x, 0, right)
    r1 = r_move(1, x, 1, left)
    r2 = r_move(2, x, 1, right)
    r3 = r_move(3, x, 0, left)
    r4 = r_move(4, xl, 0, right)
    r5 = r_move(5, xr, 1, left)
    for cp in (r0, r1, r2, r3):
        cp.start()

    for cp in n_loads:
        cp.wait()

    ssq = jnp.zeros((8, SLICE), F32)
    ssq = lax.fori_loop(0, BLK, lambda p, acc: acc + sq_block(nslab[p]), ssq)
    red_n[0] = jnp.zeros((8, SLICE), F32) + total(ssq)
    n_copies = []
    for d, row in enumerate(z_peers):
        cp = rcopy(red_n.at[0], red_n.at[d + 1], n_send.at[d], n_recv.at[d], row, c)
        cp.start()
        n_copies.append(cp)

    lane16 = lax.broadcasted_iota(jnp.int32, (BLK, QB), 1)
    row16 = lax.broadcasted_iota(jnp.int32, (BLK, QB), 0)
    e_col = (lane16 // BLK == row16).astype(BF16)
    row_e = lax.broadcasted_iota(jnp.int32, (QB, BLK), 0)
    lane_e = lax.broadcasted_iota(jnp.int32, (QB, BLK), 1)
    e_row = (row_e // BLK == lane_e).astype(BF16)
    row_m = lax.broadcasted_iota(jnp.int32, (QB, QB), 0)
    lane_m = lax.broadcasted_iota(jnp.int32, (QB, QB), 1)
    diag = lax.rem(row_m, BLK) == lax.rem(lane_m, BLK)

    wide[...] = jnp.dot(two_ref[...], e_col, preferred_element_type=F32).astype(BF16)

    def build_w(kk, carry):
        for i in range(8):
            k = kk * 8 + i
            rows = wide[blk(k, BLK), :]
            full = jnp.dot(e_row, rows, preferred_element_type=F32)
            wt[k] = jnp.where(diag, full, 0.0).astype(BF16)
        return carry

    lax.fori_loop(0, NT // 8, build_w, 0)
    r0.wait_recv()
    r4.start()
    r1.wait_recv()
    r5.start()

    for cp in n_copies:
        cp.wait()
    norm = [red_n[lax.rem(z - s + 4, 4)] for s in range(4)]
    scale = jnp.sqrt(((norm[0] + norm[1]) + (norm[2] + norm[3]))[:1, :1] / elem_count)
    for cp in s_loads:
        cp.wait()
    vg[1] = jnp.zeros_like(vg[1])

    def first(p, carry):
        ut[p] = (slab[p] / scale).astype(BF16)
        ut[p + 8] = (slab[p + 8] / scale).astype(BF16)
        for n in range(4):
            tmp[n] = jnp.transpose(slab[p, :, n * SLICE:(n + 1) * SLICE])
        tmp[4] = jnp.transpose(slab[p + 8, :, blk(z, SLICE)])
        for n in range(4):
            vg[0, 0, n, blk(p, BLK), :] = tmp[n, blk(y * 2 + c, BLK), :] / scale
            vg[0, 1, n, blk(p, BLK), :] = tmp[4, blk(n * 2 + c, BLK), :] / scale
        return carry

    lax.fori_loop(0, 8, first, 0)
    vq[1] = jnp.zeros_like(vq[1])

    def first_pairs(p, carry):
        for h in range(2):
            for n in range(4):
                tmp[n] = jnp.transpose(slab[8 * h + p, :, n * SLICE:(n + 1) * SLICE])
            for n in range(4):
                for m in range(4):
                    at = (n, m) if h else (m, n)
                    vq[0, h, at[0], at[1], blk(p, BLK), :] = tmp[n, blk(m * 2 + c, BLK), :] / scale
        return carry

    lax.fori_loop(0, 2, first_pairs, 0)
    vecs[0, :SLICE] = vg[0, 0, z]
    vecs[0, SLICE:] = vg[0, 1, y]

    out_lanes = blk(lax.rem(x, 2), SLICE)

    def piece(jv, h):
        return vecs.at[jv].reshape(BLK, BLK, SLICE).at[:, h * 8:(h + 1) * 8, :]

    def emit(jv):
        for h in range(2):
            dst_x = 2 * c + h
            dst_c = x // 2
            is_me = jnp.logical_and(dst_x == x, dst_c == c)

            @pl.when(jnp.logical_not(is_me))
            def _():
                rcopy(piece(jv, h), kbuf.at[jv, :, :, out_lanes], k_send.at[jv, h], k_recv.at[jv, lax.rem(x, 2)],
                      row_base + dst_x, dst_c).start()

            @pl.when(is_me)
            def _():
                kbuf[jv, :, :, out_lanes] = vecs[jv].reshape(BLK, BLK, SLICE)[:, h * 8:(h + 1) * 8, :]

    def build_r(bhi):
        def body(i, carry):
            rows = blk(i, 64)
            lo = rin[2 * bhi, rows, :].astype(F32).reshape(8, 8, BOND)
            hi = rin[2 * bhi + 1, rows, :].astype(F32).reshape(8, 8, BOND)
            both = jnp.concatenate([lo, hi], axis=1).reshape(SLICE, BOND)
            rb[bhi, blk(i, SLICE), :] = both.astype(BF16)
            return carry

        lax.fori_loop(0, 8, body, 0)

    def put_y(o, bhi, mc, pp):
        o = o.astype(BF16).reshape(32, BLK, QB)
        rows = pl.ds(mc * 32, 32)
        y_ref[rows, bhi, 2 * pp] = o[:, :, :SLICE]
        y_ref[rows, bhi, 2 * pp + 1] = o[:, :, SLICE:]

    def s1_first(bhi):
        def body(i, carry):
            for pp in (i, i + 4):
                w = ut[pl.ds(2 * pp, 2)].reshape(QB, BOND)
                for mc in range(2):
                    rows = rb[bhi, pl.ds(mc * BOND, BOND), :]
                    o = lax.dot_general(rows, w, (((1,), (1,)), ((), ())), preferred_element_type=F32)
                    put_y(o, bhi, mc, pp)
            return carry

        lax.fori_loop(0, 4, body, 0)

    def s1(pp):
        w = jnp.concatenate([u_ref[2 * pp + i].reshape(BOND, SLICE) for i in range(2)], axis=1)
        for bhi in range(2):
            for mc in range(2):
                put_y(jnp.dot(rb[bhi, pl.ds(mc * BOND, BOND), :], w, preferred_element_type=F32), bhi, mc, pp)

    for cp in (r2, r3):
        cp.wait_recv()
    emit(0)
    own = x // 2
    build_r(own)
    s1_first(own)
    for cp in (r4, r5):
        cp.wait_recv()
    build_r(1 - own)
    s1_first(1 - own)
    for cp in (r0, r1, r2, r3, r4, r5):
        cp.wait_send()
    cp_l.wait()

    row_id = lax.broadcasted_iota(jnp.int32, (8, SLICE), 0)
    ab_ref[...] = jnp.zeros_like(ab_ref)

    def pack(p, n, am, rr, ss):
        out = jnp.where(row_id == 0, p, 0.0)
        out = jnp.where(row_id == 1, n, out)
        out = jnp.where(row_id == 2, am, out)
        out = jnp.where(row_id == 3, rr, out)
        return jnp.where(row_id == 4, ss, out)

    def safe_div(num, den):
        ok = den > 0.0
        return jnp.where(ok, num / jnp.where(ok, den, 1.0), 0.0)

    def merge(p, n, am, rr, ss):
        n_all = col_sum(n)
        mean = safe_div(col_sum(am * n), n_all)
        gap = mean - am
        r_all = col_sum(rr + gap * (gap * n - 2.0 * ss))
        return col_sum(p), n_all, mean, r_all, col_sum(ss)

    def step(j, prev_beta):
        for k in range(NT):
            rhs = jnp.concatenate([y_ref[k, bhi].reshape(QB, SLICE) for bhi in range(2)], axis=1)
            o = jnp.dot(wt[k], rhs, preferred_element_type=F32).astype(BF16)
            z_ref[0, k] = o[:, :SLICE]
            z_ref[1, k] = o[:, SLICE:]


        order = [lax.rem(x + d, 4) for d in (2, 1, 3, 0)]

        def s3(bhi, out, lo):
            slices = [blk(pos, SLICE) for pos in order[lo:lo + 2]]
            outs = [None, None]
            for k0 in range(0, NT // 2, 8):
                for kh in range(2):
                    ks = k0 + kh * NT // 2
                    rhs = jnp.concatenate([lb[pl.ds(ks, 8), :, sl].reshape(1024, SLICE) for sl in slices], axis=1)
                    lhs = jnp.concatenate([z_ref[bhi, ks + k] for k in range(8)], axis=1)
                    o = jnp.dot(lhs, rhs, preferred_element_type=F32)
                    outs[kh] = o if outs[kh] is None else outs[kh] + o
            for n in range(2):
                cols = slice(n * SLICE, (n + 1) * SLICE)
                out[lo + n] = outs[0][:, cols] - (0.0 - outs[1][:, cols])

        acc_o = acc.at[1 - c]
        acc_m = acc.at[c]
        s_copies = []
        for n in range(2):
            two = pl.ds(2 * n, 2)
            s_copies.append(rcopy(acc_o.at[two], recv_s.at[two], s_send.at[n], s_recv.at[n], r, 1 - c))
        x_copies = []
        for n in range(3):
            x_copies.append(rcopy(acc_m.at[n], recv_x.at[n], x_send.at[n], x_recv.at[n], row_base + order[n], c))
        s3(1 - c, acc_o, 0)
        s_copies[0].start()
        s3(c, acc_m, 0)
        s_copies[0].wait_recv()
        for n in range(2):
            acc_m[n] += recv_s[n]
            x_copies[n].start()
        s3(1 - c, acc_o, 2)
        s_copies[1].start()
        s3(c, acc_m, 2)
        s_copies[1].wait_recv()
        acc_m[2] += recv_s[2]
        x_copies[2].start()
        w_own = acc_m[3] + recv_s[3]
        for cp in s_copies:
            cp.wait_send()
        for cp in x_copies:
            cp.wait()
        w_vec = (w_own + recv_x[0]) + (recv_x[1] + recv_x[2])
        v_cur = vecs[j]
        v_old = vecs[lax.max(j - 1, 0)]

        w_res = w_vec - prev_beta * v_old
        n_loc = total(v_cur * v_cur)
        a_loc = safe_div(total(w_res * v_cur), n_loc)
        e_loc = w_res - a_loc * v_cur
        red_a[0] = pack(total(w_vec * v_cur), n_loc, a_loc, total(e_loc * e_loc), total(e_loc * v_cur))

        a_copies = [rcopy(red_a.at[0], red_a.at[d + 1], a_send.at[d], a_recv.at[d], *peer) for d, peer in enumerate(group)]
        for cp in a_copies:
            cp.start()

        wg[0, z] = w_vec[:SLICE]
        wg[1, y] = w_vec[SLICE:]
        near = []
        for d in range(3):
            near.append(rcopy(wg.at[0, z], wg.at[0, z], g1_send.at[0, d], g1_recv.at[0, d], z_peers[d], c))
            near.append(rcopy(wg.at[1, y], wg.at[1, y], g1_send.at[1, d], g1_recv.at[1, d], y_peers[d], c))

        @pl.when(j < STEPS - 1)
        def _():
            for cp in near:
                cp.start()

        for cp in a_copies:
            cp.wait()
        blocks = [red_a[lax.rem(me - s + 8, 8)] for s in range(8)]

        def gather_rows(blks, i):
            return jnp.concatenate([bk[i:i + 1, :] for bk in blks], axis=0)

        par = lax.rem(j, 2)
        red_b[par, 0] = pack(*merge(*[gather_rows(blocks, i) for i in range(5)]))
        b_copies = []
        for d, peer in enumerate(plane):
            b_copies.append(rcopy(red_b.at[par, 0], red_b.at[par, d + 1], b_send.at[par, d], b_recv.at[par, d], *peer))
        for cp in b_copies:
            cp.start()

        far = []
        for d in range(3):
            far.append(rcopy(wq.at[0, y], wq.at[0, y], f_send.at[0, d], f_recv.at[0, d], y_peers[d], c))
            far.append(rcopy(wq.at[1, z], wq.at[1, z], f_send.at[1, d], f_recv.at[1, d], z_peers[d], c))

        @pl.when(j < STEPS - 1)
        def _():
            for cp in near:
                cp.wait()
            wq[0, y] = wg[0, :, :32]
            wq[1, z] = wg[1, :, :32]
            for cp in far:
                cp.start()

        for cp in b_copies:
            cp.wait()
        blocks = [red_b[par, lax.rem(g - s + BLK, BLK)] for s in range(BLK)]
        p_all, n_all, a_all, r_all, s_all = [gather_rows(blocks, i) for i in range(5)]
        alpha = col_sum(p_all) / elem_count
        gap = alpha - a_all
        beta = jnp.sqrt(col_sum(r_all + gap * (gap * n_all - 2.0 * s_all)) / elem_count)
        alpha_s = alpha[:, :1]
        beta_s = beta[:, :1]

        v_new = (w_vec - alpha_s * v_cur - prev_beta * v_old) / beta_s
        vecs[j + 1] = v_new
        ab_ref[pl.ds(j, 1), :] = alpha
        ab_ref[pl.ds(8 + j, 1), :] = beta

        emit(j + 1)

        @pl.when(j < STEPS - 1)
        def _():
            new = lax.rem(j + 1, 2)
            for h in range(2):
                for n in range(4):
                    v = (wg[h, n] - alpha_s * vg[1 - new, h, n] - prev_beta * vg[new, h, n]) / beta_s
                    vg[new, h, n] = v
                    at = (z, n) if h else (n, y)
                    u_ref[pl.ds(8 * h, 8), at[0], at[1], c] = v.astype(BF16).reshape(8, BLK, SLICE)
            moves = [(h, d) for h in range(2) for d in range(3)]
            cuts = range(4)

            def move(sems, h, i, d, ref, across):
                row = z_peers[d] if across else y_peers[d]
                return rcopy(ref, ref, sems[0].at[h, i, d], sems[1].at[h, i, d], row, c)

            def p2(i, h, d):
                ref = u_ref.at[pair(i, h), z, :, c] if h else u_ref.at[pair(i, h), :, y, c]
                return move((g2_send, g2_recv), h, i, d, ref, h == 1)

            def p3(i, h):
                ref = u_ref.at[pair(i, h), :, :, c]
                return rcopy(ref, ref, g3_send.at[h, i], g3_recv.at[h, i], r, 1 - c)

            def product(i):
                for h in range(2):
                    p3(i, h).wait_recv()
                s1(i)
                s1(4 + i)

            for i in cuts[1:]:
                for h, d in moves:
                    p2(i, h, d).start()
            for cp in far:
                cp.wait()
            for h in range(2):
                for m in range(4):
                    v = (wq[h, m] - alpha_s * vq[1 - new, h, m] - prev_beta * vq[new, h, m]) / beta_s
                    vq[new, h, m] = v
                    for n in range(4):
                        at = (m, n) if h else (n, m)
                        u_ref[pair(0, h), at[0], at[1], c] = v[n].astype(BF16).reshape(2, BLK, SLICE)
            for i in cuts:
                if i:
                    for h, d in moves:
                        p2(i, h, d).wait_recv()
                for h in range(2):
                    p3(i, h).start()
                if i:
                    product(i - 1)
            product(cuts[-1])
            for i in cuts:
                if i:
                    for h, d in moves:
                        p2(i, h, d).wait_send()
                for h in range(2):
                    p3(i, h).wait_send()

        return beta_s

    lax.fori_loop(0, STEPS, step, jnp.zeros((1, 1), F32))

    def drain(jv, carry):
        for h in range(2):
            dst_x = 2 * c + h
            dst_c = x // 2

            @pl.when(jnp.logical_not(jnp.logical_and(dst_x == x, dst_c == c)))
            def _():
                rcopy(piece(jv, h), kbuf.at[jv, :, :, 0:SLICE], k_send.at[jv, h], k_recv.at[jv, 0],
                      row_base + dst_x, dst_c).wait_send()

        for m in range(2):
            src_x = 2 * c + m
            src_c = x // 2

            @pl.when(jnp.logical_not(jnp.logical_and(src_x == x, src_c == c)))
            def _():
                rcopy(piece(jv, 0), kbuf.at[jv, :, :, m * SLICE:(m + 1) * SLICE], k_send.at[jv, 0], k_recv.at[jv, m],
                      row_base + src_x, src_c).wait_recv()

        return carry

    lax.fori_loop(0, STEPS + 1, drain, 0)
    cp_k = pltpu.make_async_copy(kbuf, kr_ref, ld_sem.at[0])
    cp_k.start()
    cp_k.wait()


def solution(mesh):
    assert mesh.shape['terms'] == 2 and mesh.shape['rows'] == 64

    def body_fn(wavefunc, left_loc, two_loc, right_loc):
        elem_count = float(wavefunc.size)
        vm = pl.BlockSpec(memory_space=pltpu.VMEM)
        hbm = pl.BlockSpec(memory_space=pl.ANY)
        dma = pltpu.SemaphoreType.DMA
        kr, ab = pl.pallas_call(
            lambda *refs: kernel(elem_count, *refs),
            out_shape=(jax.ShapeDtypeStruct((STEPS + 1, BLK, 8, QB), F32), jax.ShapeDtypeStruct((BLK, SLICE), F32)),
            in_specs=[hbm, hbm, hbm, vm],
            out_specs=(hbm, vm),
            scratch_shapes=[
                pltpu.VMEM((BLK, SLICE, BOND), F32),
                pltpu.VMEM((BLK, SLICE, BOND), F32),
                pltpu.VMEM((5, SLICE, SLICE), F32),
                pltpu.VMEM((1024, QB), BF16),
                pltpu.VMEM((BLK, SLICE, BOND), BF16),
                pltpu.VMEM((BLK, 4, 4, 2, BLK, SLICE), BF16),
                pltpu.VMEM((4, BOND, BOND), BF16),
                pltpu.VMEM((2, 1024, BOND), BF16),
                pltpu.VMEM((NT, SLICE, BOND), BF16),
                pltpu.VMEM((NT, QB, QB), BF16),
                pltpu.VMEM((NT, 2, BLK, BLK, SLICE), BF16),
                pltpu.VMEM((2, NT, QB, SLICE), BF16),
                pltpu.VMEM((2, 4, QB, SLICE), F32),
                pltpu.VMEM((4, QB, SLICE), F32),
                pltpu.VMEM((3, QB, SLICE), F32),
                pltpu.VMEM((STEPS + 1, QB, SLICE), F32),
                pltpu.VMEM((STEPS + 1, BLK, 8, QB), F32),
                pltpu.VMEM((2, 4, SLICE, SLICE), F32),
                pltpu.VMEM((2, 2, 4, SLICE, SLICE), F32),
                pltpu.VMEM((2, 4, 4, 32, SLICE), F32),
                pltpu.VMEM((2, 2, 4, 4, 32, SLICE), F32),
                pltpu.VMEM((4, 8, SLICE), F32),
                pltpu.VMEM((8, 8, SLICE), F32),
                pltpu.VMEM((2, BLK, 8, SLICE), F32),
                dma((2,)), dma((2, BLK)), dma((6,)), dma((6,)), dma((3,)), dma((3,)), dma((2,)), dma((2,)), dma((3,)), dma((3,)),
                dma((7,)), dma((7,)), dma((2, 15)), dma((2, 15)),
                dma((2, 3)), dma((2, 3)), dma((2, 3)), dma((2, 3)), dma((2, 4, 3)), dma((2, 4, 3)), dma((2, 4)), dma((2, 4)),
                dma((STEPS + 1, 2)), dma((STEPS + 1, 2)),
            ],
            compiler_params=pltpu.CompilerParams(has_side_effects=True, collective_id=0, vmem_limit_bytes=60 * 1024 * 1024),
        )(wavefunc, left_loc, right_loc.reshape(BOND, BOND), two_loc.reshape(1024, BLK))
        krylov = jnp.transpose(kr.reshape(STEPS + 1, 4, 4, 8, QB), (0, 4, 1, 2, 3))
        return krylov, ab[:STEPS, 0], ab[8:8 + STEPS, 0]

    return jax.shard_map(body_fn, mesh=mesh, in_specs=(P(), P('terms'), P('terms'), P('terms', 'rows')),
                         out_specs=(P(None, 'terms', None, None, 'rows'), P(), P()), check_vma=False)
```

```python
import jax
import jax.numpy as jnp
from jax import lax
from jax.experimental import pallas as pl
from jax.experimental.pallas import tpu as pltpu
from jax.sharding import PartitionSpec as P

STEPS = 6
F32 = jnp.float32
BF16 = jnp.bfloat16
MESH = pl.DeviceIdType.MESH
NT = 64
BOND = 512
SLICE = 128
BLK = 16
QB = 256


def total(x):
    return jnp.sum(jnp.sum(x, axis=1, keepdims=True), axis=0, keepdims=True)


def blk(i, size):
    return pl.ds(pl.multiple_of(i * size, size), size)


def col_sum(x):
    return jnp.sum(x, axis=0, keepdims=True)


def sq_block(blk):
    out = jnp.zeros((8, SLICE), F32)
    sq = (blk * blk).reshape(BLK, 8, BOND).sum(axis=0)
    for i in range(4):
        out = out + sq[:, i * SLICE:(i + 1) * SLICE]
    return out


def kernel(elem_count, wave_ref, left_ref, right_ref, two_ref, kr_ref, ab_ref,
           slab, nslab, tmp, wide, ut, u_ref, rin, rb, lb, wt, y_ref, z_ref, acc, recv_s, recv_x, vecs, kbuf, wg, vg, wq, vq,
           red_n, red_a, red_b,
           ld_sem, sl_sem, r_send, r_recv, n_send, n_recv, s_send, s_recv, x_send, x_recv, a_send, a_recv,
           b_send, b_recv, g1_send, g1_recv, f_send, f_recv, g2_send, g2_recv, g3_send, g3_recv, k_send, k_recv):
    r = lax.axis_index('rows')
    c = lax.axis_index('terms')
    x = lax.rem(r, 4)
    y = lax.rem(r // 4, 4)
    z = r // BLK
    g = r // 4
    row_base = r - x
    z_peers = [lax.rem(z + d, 4) * BLK + y * 4 + x for d in (1, 2, 3)]
    y_peers = [z * BLK + lax.rem(y + d, 4) * 4 + x for d in (1, 2, 3)]
    x_peers = [row_base + lax.rem(x + d, 4) for d in (1, 2, 3)]

    def pair(i, h):
        return pl.ds(8 * h + 2 * i, 2)

    def rcopy(src, dst, ssem, rsem, row, core):
        return pltpu.make_async_remote_copy(src_ref=src, dst_ref=dst, send_sem=ssem, recv_sem=rsem,
                                            device_id=(row, core), device_id_type=MESH)

    me = x * 2 + c
    group = [(row_base + lax.rem(me + d, 8) // 2, lax.rem(me + d, 2)) for d in range(1, 8)]
    plane = [(lax.rem(g + d, BLK) * 4 + x, c) for d in range(1, BLK)]
    barrier = pltpu.get_barrier_semaphore()
    for peer in group + plane:
        pl.semaphore_signal(barrier, inc=1, device_id=peer, device_id_type=MESH)

    cp_r = pltpu.make_async_copy(right_ref, rin.at[x], ld_sem.at[0])
    cp_r.start()
    n_loads, s_loads = [], []
    for p in range(BLK):
        rows_n = blk(z, SLICE)
        n_loads.append(pltpu.make_async_copy(wave_ref.at[rows_n, p // 4, p % 4, :], nslab.at[p], sl_sem.at[0, p]))
    for p in range(BLK):
        rows_s = blk(x, SLICE)
        s_loads.append(pltpu.make_async_copy(wave_ref.at[rows_s, p // 4, p % 4, :], slab.at[p], sl_sem.at[1, p]))
    cp_l = pltpu.make_async_copy(left_ref.at[:, blk(x, SLICE), :], lb, ld_sem.at[1])
    for cp in n_loads + s_loads:
        cp.start()
    cp_l.start()
    cp_r.wait()
    pl.semaphore_wait(barrier, len(group) + len(plane))

    right = row_base + lax.rem(x + 1, 4)
    left = row_base + lax.rem(x + 3, 4)
    xl = lax.rem(x + 3, 4)
    xr = lax.rem(x + 1, 4)
    halves = [pl.ds(0, QB), pl.ds(QB, QB)]

    quarters = [pl.ds(i * SLICE, SLICE) for i in range(4)]

    def r_move(i, block, rows, row):
        ref = rin.at[block, rows, :]
        return rcopy(ref, ref, r_send.at[i], r_recv.at[i], row, c)

    r0 = r_move(0, x, halves[0], right)
    r1 = r_move(1, x, halves[1], left)
    r2 = r_move(2, x, halves[1], right)
    r3 = r_move(3, x, halves[0], left)
    r4 = [r_move(4 + i, xl, quarters[i], right) for i in range(2)]
    r5 = [r_move(6 + i, xr, quarters[2 + i], left) for i in range(2)]
    for cp in (r0, r1, r2, r3):
        cp.start()

    for cp in n_loads:
        cp.wait()

    ssq = jnp.zeros((8, SLICE), F32)
    ssq = lax.fori_loop(0, BLK, lambda p, acc: acc + sq_block(nslab[p]), ssq)
    red_n[0] = jnp.zeros((8, SLICE), F32) + total(ssq)
    n_copies = []
    for d, row in enumerate(z_peers):
        cp = rcopy(red_n.at[0], red_n.at[d + 1], n_send.at[d], n_recv.at[d], row, c)
        cp.start()
        n_copies.append(cp)

    lane16 = lax.broadcasted_iota(jnp.int32, (BLK, QB), 1)
    row16 = lax.broadcasted_iota(jnp.int32, (BLK, QB), 0)
    e_col = (lane16 // BLK == row16).astype(BF16)
    row_e = lax.broadcasted_iota(jnp.int32, (QB, BLK), 0)
    lane_e = lax.broadcasted_iota(jnp.int32, (QB, BLK), 1)
    e_row = (row_e // BLK == lane_e).astype(BF16)
    row_m = lax.broadcasted_iota(jnp.int32, (QB, QB), 0)
    lane_m = lax.broadcasted_iota(jnp.int32, (QB, QB), 1)
    diag = lax.rem(row_m, BLK) == lax.rem(lane_m, BLK)

    wide[...] = jnp.dot(two_ref[...], e_col, preferred_element_type=F32).astype(BF16)

    def build_w(kk, carry):
        for i in range(8):
            k = kk * 8 + i
            rows = wide[blk(k, BLK), :]
            full = jnp.dot(e_row, rows, preferred_element_type=F32)
            wt[k] = jnp.where(diag, full, 0.0).astype(BF16)
        return carry

    lax.fori_loop(0, NT // 8, build_w, 0)
    r0.wait_recv()
    for cp in r4:
        cp.start()
    r1.wait_recv()
    for cp in r5:
        cp.start()

    for cp in n_copies:
        cp.wait()
    norm = [red_n[lax.rem(z - s + 4, 4)] for s in range(4)]
    scale = jnp.sqrt(((norm[0] + norm[1]) + (norm[2] + norm[3]))[:1, :1] / elem_count)
    for cp in s_loads:
        cp.wait()
    vg[1] = jnp.zeros_like(vg[1])

    def first(p, carry):
        ut[p] = (slab[p] / scale).astype(BF16)
        ut[p + 8] = (slab[p + 8] / scale).astype(BF16)
        for n in range(4):
            tmp[n] = jnp.transpose(slab[p, :, n * SLICE:(n + 1) * SLICE])
        tmp[4] = jnp.transpose(slab[p + 8, :, blk(z, SLICE)])
        for n in range(4):
            vg[0, 0, n, blk(p, BLK), :] = tmp[n, blk(y * 2 + c, BLK), :] / scale
            vg[0, 1, n, blk(p, BLK), :] = tmp[4, blk(n * 2 + c, BLK), :] / scale
        return carry

    lax.fori_loop(0, 8, first, 0)
    vq[1] = jnp.zeros_like(vq[1])

    def first_pairs(p, carry):
        for h in range(2):
            for n in range(4):
                tmp[n] = jnp.transpose(slab[8 * h + p, :, n * SLICE:(n + 1) * SLICE])
            for n in range(4):
                for m in range(4):
                    at = (n, m) if h else (m, n)
                    vq[0, h, at[0], at[1], blk(p, BLK), :] = tmp[n, blk(m * 2 + c, BLK), :] / scale
        return carry

    lax.fori_loop(0, 2, first_pairs, 0)
    vecs[0, :SLICE] = vg[0, 0, z]
    vecs[0, SLICE:] = vg[0, 1, y]

    out_lanes = blk(lax.rem(x, 2), SLICE)

    def piece(jv, h):
        return vecs.at[jv].reshape(BLK, BLK, SLICE).at[:, h * 8:(h + 1) * 8, :]

    def emit(jv):
        for h in range(2):
            dst_x = 2 * c + h
            dst_c = x // 2
            is_me = jnp.logical_and(dst_x == x, dst_c == c)

            @pl.when(jnp.logical_not(is_me))
            def _():
                rcopy(piece(jv, h), kbuf.at[jv, :, :, out_lanes], k_send.at[jv, h], k_recv.at[jv, lax.rem(x, 2)],
                      row_base + dst_x, dst_c).start()

            @pl.when(is_me)
            def _():
                kbuf[jv, :, :, out_lanes] = vecs[jv].reshape(BLK, BLK, SLICE)[:, h * 8:(h + 1) * 8, :]

    def build_r(bhi, parts):
        for i in parts:
            rows = quarters[i]
            lo = rin[2 * bhi, rows, :].astype(F32).reshape(BLK, 8, BOND)
            hi = rin[2 * bhi + 1, rows, :].astype(F32).reshape(BLK, 8, BOND)
            both = jnp.concatenate([lo, hi], axis=1).reshape(QB, BOND)
            rb[bhi, pl.ds(i * QB, QB), :] = both.astype(BF16)

    def put_y(o, bhi, first_k, pp):
        o = o.astype(BF16).reshape(-1, BLK, QB)
        rows = pl.ds(first_k, o.shape[0])
        y_ref[rows, bhi, 2 * pp] = o[:, :, :SLICE]
        y_ref[rows, bhi, 2 * pp + 1] = o[:, :, SLICE:]

    def s1_first(bhi, parts):
        build_r(bhi, parts)

        def body(i, carry):
            for pp in (i, i + 4):
                w = ut[pl.ds(2 * pp, 2)].reshape(QB, BOND)
                for m in parts:
                    rows = rb[bhi, pl.ds(m * QB, QB), :]
                    o = lax.dot_general(rows, w, (((1,), (1,)), ((), ())), preferred_element_type=F32)
                    put_y(o, bhi, m * BLK, pp)
            return carry

        lax.fori_loop(0, 4, body, 0)

    def s1(pp):
        w = jnp.concatenate([u_ref[2 * pp + i].reshape(BOND, SLICE) for i in range(2)], axis=1)
        for bhi in range(2):
            for mc in range(2):
                put_y(jnp.dot(rb[bhi, pl.ds(mc * BOND, BOND), :], w, preferred_element_type=F32), bhi, mc * 32, pp)

    for cp in (r2, r3):
        cp.wait_recv()
    emit(0)
    own = x // 2
    s1_first(own, range(4))
    for i in range(2):
        r4[i].wait_recv()
        r5[i].wait_recv()
        s1_first(1 - own, (i, 2 + i))
    for cp in [r0, r1, r2, r3] + r4 + r5:
        cp.wait_send()
    cp_l.wait()

    row_id = lax.broadcasted_iota(jnp.int32, (8, SLICE), 0)
    ab_ref[...] = jnp.zeros_like(ab_ref)

    def pack(p, n, am, rr, ss):
        out = jnp.where(row_id == 0, p, 0.0)
        out = jnp.where(row_id == 1, n, out)
        out = jnp.where(row_id == 2, am, out)
        out = jnp.where(row_id == 3, rr, out)
        return jnp.where(row_id == 4, ss, out)

    def safe_div(num, den):
        ok = den > 0.0
        return jnp.where(ok, num / jnp.where(ok, den, 1.0), 0.0)

    def merge(p, n, am, rr, ss):
        n_all = col_sum(n)
        mean = safe_div(col_sum(am * n), n_all)
        gap = mean - am
        r_all = col_sum(rr + gap * (gap * n - 2.0 * ss))
        return col_sum(p), n_all, mean, r_all, col_sum(ss)

    def step(j, prev_beta):
        for k in range(NT):
            rhs = jnp.concatenate([y_ref[k, bhi].reshape(QB, SLICE) for bhi in range(2)], axis=1)
            o = jnp.dot(wt[k], rhs, preferred_element_type=F32).astype(BF16)
            z_ref[0, k] = o[:, :SLICE]
            z_ref[1, k] = o[:, SLICE:]


        order = [lax.rem(x + d, 4) for d in (2, 1, 3, 0)]

        def s3(bhi, out, lo):
            slices = [blk(pos, SLICE) for pos in order[lo:lo + 2]]
            outs = [None, None]
            for k0 in range(0, NT // 2, 8):
                for kh in range(2):
                    ks = k0 + kh * NT // 2
                    rhs = jnp.concatenate([lb[pl.ds(ks, 8), :, sl].reshape(1024, SLICE) for sl in slices], axis=1)
                    lhs = jnp.concatenate([z_ref[bhi, ks + k] for k in range(8)], axis=1)
                    o = jnp.dot(lhs, rhs, preferred_element_type=F32)
                    outs[kh] = o if outs[kh] is None else outs[kh] + o
            for n in range(2):
                cols = slice(n * SLICE, (n + 1) * SLICE)
                out[lo + n] = outs[0][:, cols] - (0.0 - outs[1][:, cols])

        acc_o = acc.at[1 - c]
        acc_m = acc.at[c]
        s_copies = []
        for n in range(2):
            two = pl.ds(2 * n, 2)
            s_copies.append(rcopy(acc_o.at[two], recv_s.at[two], s_send.at[n], s_recv.at[n], r, 1 - c))
        x_copies = []
        for n in range(3):
            x_copies.append(rcopy(acc_m.at[n], recv_x.at[n], x_send.at[n], x_recv.at[n], row_base + order[n], c))
        s3(1 - c, acc_o, 0)
        s_copies[0].start()
        s3(c, acc_m, 0)
        s_copies[0].wait_recv()
        for n in range(2):
            acc_m[n] += recv_s[n]
            x_copies[n].start()
        s3(1 - c, acc_o, 2)
        s_copies[1].start()
        s3(c, acc_m, 2)
        s_copies[1].wait_recv()
        acc_m[2] += recv_s[2]
        x_copies[2].start()
        w_own = acc_m[3] + recv_s[3]
        for cp in s_copies:
            cp.wait_send()
        for cp in x_copies:
            cp.wait()
        w_vec = (w_own + recv_x[0]) + (recv_x[1] + recv_x[2])
        v_cur = vecs[j]
        v_old = vecs[lax.max(j - 1, 0)]

        w_res = w_vec - prev_beta * v_old
        n_loc = total(v_cur * v_cur)
        a_loc = safe_div(total(w_res * v_cur), n_loc)
        e_loc = w_res - a_loc * v_cur
        red_a[0] = pack(total(w_vec * v_cur), n_loc, a_loc, total(e_loc * e_loc), total(e_loc * v_cur))

        a_copies = [rcopy(red_a.at[0], red_a.at[d + 1], a_send.at[d], a_recv.at[d], *peer) for d, peer in enumerate(group)]
        for cp in a_copies:
            cp.start()

        wg[0, z] = w_vec[:SLICE]
        wg[1, y] = w_vec[SLICE:]
        near = []
        for d in range(3):
            near.append(rcopy(wg.at[0, z], wg.at[0, z], g1_send.at[0, d], g1_recv.at[0, d], z_peers[d], c))
            near.append(rcopy(wg.at[1, y], wg.at[1, y], g1_send.at[1, d], g1_recv.at[1, d], y_peers[d], c))

        @pl.when(j < STEPS - 1)
        def _():
            for cp in near:
                cp.start()

        for cp in a_copies:
            cp.wait()
        blocks = [red_a[lax.rem(me - s + 8, 8)] for s in range(8)]

        def gather_rows(blks, i):
            return jnp.concatenate([bk[i:i + 1, :] for bk in blks], axis=0)

        par = lax.rem(j, 2)
        red_b[par, 0] = pack(*merge(*[gather_rows(blocks, i) for i in range(5)]))
        b_copies = []
        for d, peer in enumerate(plane):
            b_copies.append(rcopy(red_b.at[par, 0], red_b.at[par, d + 1], b_send.at[par, d], b_recv.at[par, d], *peer))
        for cp in b_copies:
            cp.start()

        far = []
        for d in range(3):
            far.append(rcopy(wq.at[0, y], wq.at[0, y], f_send.at[0, d], f_recv.at[0, d], y_peers[d], c))
            far.append(rcopy(wq.at[1, z], wq.at[1, z], f_send.at[1, d], f_recv.at[1, d], z_peers[d], c))

        @pl.when(j < STEPS - 1)
        def _():
            for cp in near:
                cp.wait()
            wq[0, y] = wg[0, :, :32]
            wq[1, z] = wg[1, :, :32]
            for cp in far:
                cp.start()

        for cp in b_copies:
            cp.wait()
        blocks = [red_b[par, lax.rem(g - s + BLK, BLK)] for s in range(BLK)]
        p_all, n_all, a_all, r_all, s_all = [gather_rows(blocks, i) for i in range(5)]
        alpha = col_sum(p_all) / elem_count
        gap = alpha - a_all
        beta = jnp.sqrt(col_sum(r_all + gap * (gap * n_all - 2.0 * s_all)) / elem_count)
        alpha_s = alpha[:, :1]
        beta_s = beta[:, :1]

        def advance(w, cur, old):
            return (w - alpha_s * cur - prev_beta * old) / beta_s

        new = lax.rem(j + 1, 2)
        moves = [(h, d) for h in range(2) for d in range(3)]
        cuts = range(4)

        def p2(i, h, d):
            ref = u_ref.at[pair(i, h), z, :, c] if h else u_ref.at[pair(i, h), :, y, c]
            row = z_peers[d] if h else y_peers[d]
            return rcopy(ref, ref, g2_send.at[h, i, d], g2_recv.at[h, i, d], row, c)

        def p3(i, h):
            ref = u_ref.at[pair(i, h), :, :, c]
            return rcopy(ref, ref, g3_send.at[h, i], g3_recv.at[h, i], r, 1 - c)

        def product(i):
            for h in range(2):
                p3(i, h).wait_recv()
            s1(i)
            s1(4 + i)

        @pl.when(j < STEPS - 1)
        def _():
            for i in cuts[1:]:
                rows = pl.ds(32 * i, 32)
                for h in range(2):
                    for n in range(4):
                        v = advance(wg[h, n, rows], vg[1 - new, h, n, rows], vg[new, h, n, rows])
                        vg[new, h, n, rows] = v
                        at = (z, n) if h else (n, y)
                        u_ref[pair(i, h), at[0], at[1], c] = v.astype(BF16).reshape(2, BLK, SLICE)
                for h, d in moves:
                    p2(i, h, d).start()

        v_new = advance(w_vec, v_cur, v_old)
        vecs[j + 1] = v_new
        ab_ref[pl.ds(j, 1), :] = alpha
        ab_ref[pl.ds(8 + j, 1), :] = beta

        @pl.when(j < STEPS - 1)
        def _():
            for cp in far:
                cp.wait()
            for h in range(2):
                for m in range(4):
                    v = advance(wq[h, m], vq[1 - new, h, m], vq[new, h, m])
                    vq[new, h, m] = v
                    for n in range(4):
                        at = (m, n) if h else (n, m)
                        u_ref[pair(0, h), at[0], at[1], c] = v[n].astype(BF16).reshape(2, BLK, SLICE)
            for i in cuts:
                if i:
                    for h, d in moves:
                        p2(i, h, d).wait_recv()
                for h in range(2):
                    p3(i, h).start()
                if i:
                    product(i - 1)
            product(cuts[-1])
            for i in cuts:
                if i:
                    for h, d in moves:
                        p2(i, h, d).wait_send()
                for h in range(2):
                    p3(i, h).wait_send()

        emit(j + 1)
        return beta_s

    lax.fori_loop(0, STEPS, step, jnp.zeros((1, 1), F32))

    def drain(jv, carry):
        for h in range(2):
            dst_x = 2 * c + h
            dst_c = x // 2

            @pl.when(jnp.logical_not(jnp.logical_and(dst_x == x, dst_c == c)))
            def _():
                rcopy(piece(jv, h), kbuf.at[jv, :, :, 0:SLICE], k_send.at[jv, h], k_recv.at[jv, 0],
                      row_base + dst_x, dst_c).wait_send()

        for m in range(2):
            src_x = 2 * c + m
            src_c = x // 2

            @pl.when(jnp.logical_not(jnp.logical_and(src_x == x, src_c == c)))
            def _():
                rcopy(piece(jv, 0), kbuf.at[jv, :, :, m * SLICE:(m + 1) * SLICE], k_send.at[jv, 0], k_recv.at[jv, m],
                      row_base + src_x, src_c).wait_recv()

        return carry

    lax.fori_loop(0, STEPS + 1, drain, 0)
    cp_k = pltpu.make_async_copy(kbuf, kr_ref, ld_sem.at[0])
    cp_k.start()
    cp_k.wait()


def solution(mesh):
    assert mesh.shape['terms'] == 2 and mesh.shape['rows'] == 64

    def body_fn(wavefunc, left_loc, two_loc, right_loc):
        elem_count = float(wavefunc.size)
        vm = pl.BlockSpec(memory_space=pltpu.VMEM)
        hbm = pl.BlockSpec(memory_space=pl.ANY)
        dma = pltpu.SemaphoreType.DMA
        kr, ab = pl.pallas_call(
            lambda *refs: kernel(elem_count, *refs),
            out_shape=(jax.ShapeDtypeStruct((STEPS + 1, BLK, 8, QB), F32), jax.ShapeDtypeStruct((BLK, SLICE), F32)),
            in_specs=[hbm, hbm, hbm, vm],
            out_specs=(hbm, vm),
            scratch_shapes=[
                pltpu.VMEM((BLK, SLICE, BOND), F32),
                pltpu.VMEM((BLK, SLICE, BOND), F32),
                pltpu.VMEM((5, SLICE, SLICE), F32),
                pltpu.VMEM((1024, QB), BF16),
                pltpu.VMEM((BLK, SLICE, BOND), BF16),
                pltpu.VMEM((BLK, 4, 4, 2, BLK, SLICE), BF16),
                pltpu.VMEM((4, BOND, BOND), BF16),
                pltpu.VMEM((2, 1024, BOND), BF16),
                pltpu.VMEM((NT, SLICE, BOND), BF16),
                pltpu.VMEM((NT, QB, QB), BF16),
                pltpu.VMEM((NT, 2, BLK, BLK, SLICE), BF16),
                pltpu.VMEM((2, NT, QB, SLICE), BF16),
                pltpu.VMEM((2, 4, QB, SLICE), F32),
                pltpu.VMEM((4, QB, SLICE), F32),
                pltpu.VMEM((3, QB, SLICE), F32),
                pltpu.VMEM((STEPS + 1, QB, SLICE), F32),
                pltpu.VMEM((STEPS + 1, BLK, 8, QB), F32),
                pltpu.VMEM((2, 4, SLICE, SLICE), F32),
                pltpu.VMEM((2, 2, 4, SLICE, SLICE), F32),
                pltpu.VMEM((2, 4, 4, 32, SLICE), F32),
                pltpu.VMEM((2, 2, 4, 4, 32, SLICE), F32),
                pltpu.VMEM((4, 8, SLICE), F32),
                pltpu.VMEM((8, 8, SLICE), F32),
                pltpu.VMEM((2, BLK, 8, SLICE), F32),
                dma((2,)), dma((2, BLK)), dma((8,)), dma((8,)), dma((3,)), dma((3,)), dma((2,)), dma((2,)), dma((3,)), dma((3,)),
                dma((7,)), dma((7,)), dma((2, 15)), dma((2, 15)),
                dma((2, 3)), dma((2, 3)), dma((2, 3)), dma((2, 3)), dma((2, 4, 3)), dma((2, 4, 3)), dma((2, 4)), dma((2, 4)),
                dma((STEPS + 1, 2)), dma((STEPS + 1, 2)),
            ],
            compiler_params=pltpu.CompilerParams(has_side_effects=True, collective_id=0, vmem_limit_bytes=60 * 1024 * 1024),
        )(wavefunc, left_loc, right_loc.reshape(BOND, BOND), two_loc.reshape(1024, BLK))
        krylov = jnp.transpose(kr.reshape(STEPS + 1, 4, 4, 8, QB), (0, 4, 1, 2, 3))
        return krylov, ab[:STEPS, 0], ab[8:8 + STEPS, 0]

    return jax.shard_map(body_fn, mesh=mesh, in_specs=(P(), P('terms'), P('terms'), P('terms', 'rows')),
                         out_specs=(P(None, 'terms', None, None, 'rows'), P(), P()), check_vma=False)
```

```python
import jax
import jax.numpy as jnp
from jax import lax
from jax.experimental import pallas as pl
from jax.experimental.pallas import tpu as pltpu
from jax.sharding import PartitionSpec as P

STEPS = 6
F32 = jnp.float32
BF16 = jnp.bfloat16
MESH = pl.DeviceIdType.MESH
NT = 64
BOND = 512
SLICE = 128
BLK = 16
QB = 256


def total(x):
    return jnp.sum(jnp.sum(x, axis=1, keepdims=True), axis=0, keepdims=True)


def blk(i, size):
    return pl.ds(pl.multiple_of(i * size, size), size)


def col_sum(x):
    return jnp.sum(x, axis=0, keepdims=True)


def sq_block(blk):
    out = jnp.zeros((8, SLICE), F32)
    sq = (blk * blk).reshape(BLK, 8, BOND).sum(axis=0)
    for i in range(4):
        out = out + sq[:, i * SLICE:(i + 1) * SLICE]
    return out


def kernel(elem_count, wave_ref, left_ref, right_ref, two_ref, kr_ref, ab_ref,
           slab, nslab, tmp, wide, ut, u_ref, rin, rb, lb, wt, y_ref, z_ref, acc, recv_s, recv_x, vecs, kbuf, wg, vg, wq, vq,
           red_n, red_a, red_b,
           ld_sem, sl_sem, r_send, r_recv, n_send, n_recv, s_send, s_recv, x_send, x_recv, a_send, a_recv,
           b_send, b_recv, g1_send, g1_recv, f_send, f_recv, g2_send, g2_recv, g3_send, g3_recv, k_send, k_recv):
    r = lax.axis_index('rows')
    c = lax.axis_index('terms')
    x = lax.rem(r, 4)
    y = lax.rem(r // 4, 4)
    z = r // BLK
    g = r // 4
    row_base = r - x
    z_peers = [lax.rem(z + d, 4) * BLK + y * 4 + x for d in (1, 2, 3)]
    y_peers = [z * BLK + lax.rem(y + d, 4) * 4 + x for d in (1, 2, 3)]
    x_peers = [row_base + lax.rem(x + d, 4) for d in (1, 2, 3)]

    def pair(i, h):
        return pl.ds(8 * h + 2 * i, 2)

    def rcopy(src, dst, ssem, rsem, row, core):
        return pltpu.make_async_remote_copy(src_ref=src, dst_ref=dst, send_sem=ssem, recv_sem=rsem,
                                            device_id=(row, core), device_id_type=MESH)

    me = x * 2 + c
    group = [(row_base + lax.rem(me + d, 8) // 2, lax.rem(me + d, 2)) for d in range(1, 8)]
    plane = [(lax.rem(g + d, BLK) * 4 + x, c) for d in range(1, BLK)]
    barrier = pltpu.get_barrier_semaphore()
    for peer in group + plane:
        pl.semaphore_signal(barrier, inc=1, device_id=peer, device_id_type=MESH)

    cp_r = pltpu.make_async_copy(right_ref, rin.at[x], ld_sem.at[0])
    cp_r.start()
    n_loads, s_loads = [], []
    for p in range(BLK):
        rows_n = blk(z, SLICE)
        n_loads.append(pltpu.make_async_copy(wave_ref.at[rows_n, p // 4, p % 4, :], nslab.at[p], sl_sem.at[0, p]))
    for p in range(BLK):
        rows_s = blk(x, SLICE)
        s_loads.append(pltpu.make_async_copy(wave_ref.at[rows_s, p // 4, p % 4, :], slab.at[p], sl_sem.at[1, p]))
    cp_l = pltpu.make_async_copy(left_ref.at[:, blk(x, SLICE), :], lb, ld_sem.at[1])
    for cp in n_loads + s_loads:
        cp.start()
    cp_l.start()
    cp_r.wait()
    pl.semaphore_wait(barrier, len(group) + len(plane))

    right = row_base + lax.rem(x + 1, 4)
    left = row_base + lax.rem(x + 3, 4)
    xl = lax.rem(x + 3, 4)
    xr = lax.rem(x + 1, 4)
    halves = [pl.ds(0, QB), pl.ds(QB, QB)]

    quarters = [pl.ds(i * SLICE, SLICE) for i in range(4)]

    def r_move(i, block, rows, row):
        ref = rin.at[block, rows, :]
        return rcopy(ref, ref, r_send.at[i], r_recv.at[i], row, c)

    r0 = r_move(0, x, halves[0], right)
    r1 = r_move(1, x, halves[1], left)
    r2 = r_move(2, x, halves[1], right)
    r3 = r_move(3, x, halves[0], left)
    r4 = [r_move(4 + i, xl, quarters[i], right) for i in range(2)]
    r5 = [r_move(6 + i, xr, quarters[2 + i], left) for i in range(2)]
    for cp in (r0, r1, r2, r3):
        cp.start()

    for cp in n_loads:
        cp.wait()

    ssq = jnp.zeros((8, SLICE), F32)
    ssq = lax.fori_loop(0, BLK, lambda p, acc: acc + sq_block(nslab[p]), ssq)
    red_n[0] = jnp.zeros((8, SLICE), F32) + total(ssq)
    n_copies = []
    for d, row in enumerate(z_peers):
        cp = rcopy(red_n.at[0], red_n.at[d + 1], n_send.at[d], n_recv.at[d], row, c)
        cp.start()
        n_copies.append(cp)

    row_e = lax.broadcasted_iota(jnp.int32, (QB, BLK), 0)
    lane_e = lax.broadcasted_iota(jnp.int32, (QB, BLK), 1)
    e_row = (row_e // BLK == lane_e).astype(BF16)
    row_m = lax.broadcasted_iota(jnp.int32, (QB, QB), 0)
    lane_m = lax.broadcasted_iota(jnp.int32, (QB, QB), 1)
    diag = lax.rem(row_m, BLK) == lax.rem(lane_m, BLK)

    by_term = jnp.transpose(two_ref[...].astype(F32)).astype(BF16)
    for q in range(BLK):
        pick = (row_m == q * BLK + lane_m // BLK).astype(BF16)
        wide[q] = jnp.dot(by_term, pick, preferred_element_type=F32)

    def build_w(kk, carry):
        for i in range(8):
            k = kk * 8 + i
            rows = wide[:, k, :].astype(BF16)
            full = jnp.dot(e_row, rows, preferred_element_type=F32)
            wt[k] = jnp.where(diag, full, 0.0).astype(BF16)
        return carry

    lax.fori_loop(0, NT // 8, build_w, 0)
    r0.wait_recv()
    for cp in r4:
        cp.start()
    r1.wait_recv()
    for cp in r5:
        cp.start()

    for cp in n_copies:
        cp.wait()
    norm = [red_n[lax.rem(z - s + 4, 4)] for s in range(4)]
    scale = jnp.sqrt(((norm[0] + norm[1]) + (norm[2] + norm[3]))[:1, :1] / elem_count)
    for cp in s_loads:
        cp.wait()
    vg[1] = jnp.zeros_like(vg[1])

    def first(p, carry):
        ut[p] = (slab[p] / scale).astype(BF16)
        ut[p + 8] = (slab[p + 8] / scale).astype(BF16)
        for n in range(4):
            tmp[n] = jnp.transpose(slab[p, :, n * SLICE:(n + 1) * SLICE])
        tmp[4] = jnp.transpose(slab[p + 8, :, blk(z, SLICE)])
        for n in range(4):
            vg[0, 0, n, blk(p, BLK), :] = tmp[n, blk(y * 2 + c, BLK), :] / scale
            vg[0, 1, n, blk(p, BLK), :] = tmp[4, blk(n * 2 + c, BLK), :] / scale
        return carry

    lax.fori_loop(0, 8, first, 0)
    vq[1] = jnp.zeros_like(vq[1])

    def first_pairs(p, carry):
        for h in range(2):
            for n in range(4):
                tmp[n] = jnp.transpose(slab[8 * h + p, :, n * SLICE:(n + 1) * SLICE])
            for n in range(4):
                for m in range(4):
                    at = (n, m) if h else (m, n)
                    vq[0, h, at[0], at[1], blk(p, BLK), :] = tmp[n, blk(m * 2 + c, BLK), :] / scale
        return carry

    lax.fori_loop(0, 2, first_pairs, 0)
    vecs[0, :SLICE] = vg[0, 0, z]
    vecs[0, SLICE:] = vg[0, 1, y]

    out_lanes = blk(lax.rem(x, 2), SLICE)

    def piece(jv, h):
        return vecs.at[jv].reshape(BLK, BLK, SLICE).at[:, h * 8:(h + 1) * 8, :]

    def emit(jv):
        for h in range(2):
            dst_x = 2 * c + h
            dst_c = x // 2
            is_me = jnp.logical_and(dst_x == x, dst_c == c)

            @pl.when(jnp.logical_not(is_me))
            def _():
                rcopy(piece(jv, h), kbuf.at[jv, :, :, out_lanes], k_send.at[jv, h], k_recv.at[jv, lax.rem(x, 2)],
                      row_base + dst_x, dst_c).start()

            @pl.when(is_me)
            def _():
                kbuf[jv, :, :, out_lanes] = vecs[jv].reshape(BLK, BLK, SLICE)[:, h * 8:(h + 1) * 8, :]

    def build_r(bhi, parts):
        for i in parts:
            rows = quarters[i]
            lo = rin[2 * bhi, rows, :].astype(F32).reshape(BLK, 8, BOND)
            hi = rin[2 * bhi + 1, rows, :].astype(F32).reshape(BLK, 8, BOND)
            both = jnp.concatenate([lo, hi], axis=1).reshape(QB, BOND)
            rb[bhi, pl.ds(i * QB, QB), :] = both.astype(BF16)

    def put_y(o, bhi, first_k, pp):
        o = o.astype(BF16).reshape(-1, BLK, QB)
        rows = pl.ds(first_k, o.shape[0])
        y_ref[rows, bhi, 2 * pp] = o[:, :, :SLICE]
        y_ref[rows, bhi, 2 * pp + 1] = o[:, :, SLICE:]

    def s1_first(bhi, parts):
        build_r(bhi, parts)

        def body(i, carry):
            for pp in (i, i + 4):
                w = ut[pl.ds(2 * pp, 2)].reshape(QB, BOND)
                for m in parts:
                    rows = rb[bhi, pl.ds(m * QB, QB), :]
                    o = lax.dot_general(rows, w, (((1,), (1,)), ((), ())), preferred_element_type=F32)
                    put_y(o, bhi, m * BLK, pp)
            return carry

        lax.fori_loop(0, 4, body, 0)

    def s1(pp):
        w = jnp.concatenate([u_ref[2 * pp + i].reshape(BOND, SLICE) for i in range(2)], axis=1)
        for bhi in range(2):
            for mc in range(2):
                put_y(jnp.dot(rb[bhi, pl.ds(mc * BOND, BOND), :], w, preferred_element_type=F32), bhi, mc * 32, pp)

    for cp in (r2, r3):
        cp.wait_recv()
    emit(0)
    own = x // 2
    s1_first(own, range(4))
    for i in range(2):
        r4[i].wait_recv()
        r5[i].wait_recv()
        s1_first(1 - own, (i, 2 + i))
    for cp in [r0, r1, r2, r3] + r4 + r5:
        cp.wait_send()
    cp_l.wait()

    row_id = lax.broadcasted_iota(jnp.int32, (8, SLICE), 0)
    ab_ref[...] = jnp.zeros_like(ab_ref)

    def pack(p, n, am, rr, ss):
        out = jnp.where(row_id == 0, p, 0.0)
        out = jnp.where(row_id == 1, n, out)
        out = jnp.where(row_id == 2, am, out)
        out = jnp.where(row_id == 3, rr, out)
        return jnp.where(row_id == 4, ss, out)

    def safe_div(num, den):
        ok = den > 0.0
        return jnp.where(ok, num / jnp.where(ok, den, 1.0), 0.0)

    def merge(p, n, am, rr, ss):
        n_all = col_sum(n)
        mean = safe_div(col_sum(am * n), n_all)
        gap = mean - am
        r_all = col_sum(rr + gap * (gap * n - 2.0 * ss))
        return col_sum(p), n_all, mean, r_all, col_sum(ss)

    def step(j, prev_beta):
        for k in range(NT):
            rhs = jnp.concatenate([y_ref[k, bhi].reshape(QB, SLICE) for bhi in range(2)], axis=1)
            o = jnp.dot(wt[k], rhs, preferred_element_type=F32).astype(BF16)
            z_ref[0, k] = o[:, :SLICE]
            z_ref[1, k] = o[:, SLICE:]


        order = [lax.rem(x + d, 4) for d in (2, 1, 3, 0)]

        def s3(bhi, out, lo):
            slices = [blk(pos, SLICE) for pos in order[lo:lo + 2]]
            outs = [None, None]
            for k0 in range(0, NT // 2, 8):
                for kh in range(2):
                    ks = k0 + kh * NT // 2
                    rhs = jnp.concatenate([lb[pl.ds(ks, 8), :, sl].reshape(1024, SLICE) for sl in slices], axis=1)
                    lhs = jnp.concatenate([z_ref[bhi, ks + k] for k in range(8)], axis=1)
                    o = jnp.dot(lhs, rhs, preferred_element_type=F32)
                    outs[kh] = o if outs[kh] is None else outs[kh] + o
            for n in range(2):
                cols = slice(n * SLICE, (n + 1) * SLICE)
                out[lo + n] = outs[0][:, cols] - (0.0 - outs[1][:, cols])

        acc_o = acc.at[1 - c]
        acc_m = acc.at[c]
        s_copies = []
        for n in range(2):
            two = pl.ds(2 * n, 2)
            s_copies.append(rcopy(acc_o.at[two], recv_s.at[two], s_send.at[n], s_recv.at[n], r, 1 - c))
        x_copies = []
        for n in range(3):
            x_copies.append(rcopy(acc_m.at[n], recv_x.at[n], x_send.at[n], x_recv.at[n], row_base + order[n], c))
        s3(1 - c, acc_o, 0)
        s_copies[0].start()
        s3(c, acc_m, 0)
        s_copies[0].wait_recv()
        for n in range(2):
            acc_m[n] += recv_s[n]
            x_copies[n].start()
        s3(1 - c, acc_o, 2)
        s_copies[1].start()
        s3(c, acc_m, 2)
        s_copies[1].wait_recv()
        acc_m[2] += recv_s[2]
        x_copies[2].start()
        w_own = acc_m[3] + recv_s[3]
        for cp in s_copies:
            cp.wait_send()
        for cp in x_copies:
            cp.wait()
        w_vec = (w_own + recv_x[0]) + (recv_x[1] + recv_x[2])
        v_cur = vecs[j]
        v_old = vecs[lax.max(j - 1, 0)]

        w_res = w_vec - prev_beta * v_old
        n_loc = total(v_cur * v_cur)
        a_loc = safe_div(total(w_res * v_cur), n_loc)
        e_loc = w_res - a_loc * v_cur
        red_a[0] = pack(total(w_vec * v_cur), n_loc, a_loc, total(e_loc * e_loc), total(e_loc * v_cur))

        a_copies = [rcopy(red_a.at[0], red_a.at[d + 1], a_send.at[d], a_recv.at[d], *peer) for d, peer in enumerate(group)]
        for cp in a_copies:
            cp.start()

        wg[0, z] = w_vec[:SLICE]
        wg[1, y] = w_vec[SLICE:]
        near = []
        for d in range(3):
            near.append(rcopy(wg.at[0, z], wg.at[0, z], g1_send.at[0, d], g1_recv.at[0, d], z_peers[d], c))
            near.append(rcopy(wg.at[1, y], wg.at[1, y], g1_send.at[1, d], g1_recv.at[1, d], y_peers[d], c))

        @pl.when(j < STEPS - 1)
        def _():
            for cp in near:
                cp.start()

        for cp in a_copies:
            cp.wait()
        blocks = [red_a[lax.rem(me - s + 8, 8)] for s in range(8)]

        def gather_rows(blks, i):
            return jnp.concatenate([bk[i:i + 1, :] for bk in blks], axis=0)

        par = lax.rem(j, 2)
        red_b[par, 0] = pack(*merge(*[gather_rows(blocks, i) for i in range(5)]))
        b_copies = []
        for d, peer in enumerate(plane):
            b_copies.append(rcopy(red_b.at[par, 0], red_b.at[par, d + 1], b_send.at[par, d], b_recv.at[par, d], *peer))
        for cp in b_copies:
            cp.start()

        far = []
        for d in range(3):
            far.append(rcopy(wq.at[0, y], wq.at[0, y], f_send.at[0, d], f_recv.at[0, d], y_peers[d], c))
            far.append(rcopy(wq.at[1, z], wq.at[1, z], f_send.at[1, d], f_recv.at[1, d], z_peers[d], c))

        @pl.when(j < STEPS - 1)
        def _():
            for cp in near:
                cp.wait()
            wq[0, y] = wg[0, :, :32]
            wq[1, z] = wg[1, :, :32]
            for cp in far:
                cp.start()

        for cp in b_copies:
            cp.wait()
        blocks = [red_b[par, lax.rem(g - s + BLK, BLK)] for s in range(BLK)]
        p_all, n_all, a_all, r_all, s_all = [gather_rows(blocks, i) for i in range(5)]
        alpha = col_sum(p_all) / elem_count
        gap = alpha - a_all
        beta = jnp.sqrt(col_sum(r_all + gap * (gap * n_all - 2.0 * s_all)) / elem_count)
        alpha_s = alpha[:, :1]
        beta_s = beta[:, :1]

        def advance(w, cur, old):
            return (w - alpha_s * cur - prev_beta * old) / beta_s

        new = lax.rem(j + 1, 2)
        moves = [(h, d) for h in range(2) for d in range(3)]
        cuts = range(4)

        def p2(i, h, d):
            ref = u_ref.at[pair(i, h), z, :, c] if h else u_ref.at[pair(i, h), :, y, c]
            row = z_peers[d] if h else y_peers[d]
            return rcopy(ref, ref, g2_send.at[h, i, d], g2_recv.at[h, i, d], row, c)

        def p3(i, h):
            ref = u_ref.at[pair(i, h), :, :, c]
            return rcopy(ref, ref, g3_send.at[h, i], g3_recv.at[h, i], r, 1 - c)

        def product(i):
            for h in range(2):
                p3(i, h).wait_recv()
            s1(i)
            s1(4 + i)

        @pl.when(j < STEPS - 1)
        def _():
            for i in cuts[1:]:
                rows = pl.ds(32 * i, 32)
                for h in range(2):
                    for n in range(4):
                        v = advance(wg[h, n, rows], vg[1 - new, h, n, rows], vg[new, h, n, rows])
                        vg[new, h, n, rows] = v
                        at = (z, n) if h else (n, y)
                        u_ref[pair(i, h), at[0], at[1], c] = v.astype(BF16).reshape(2, BLK, SLICE)
                for h, d in moves:
                    p2(i, h, d).start()

        v_new = advance(w_vec, v_cur, v_old)
        vecs[j + 1] = v_new
        ab_ref[pl.ds(j, 1), :] = alpha
        ab_ref[pl.ds(8 + j, 1), :] = beta

        @pl.when(j < STEPS - 1)
        def _():
            for cp in far:
                cp.wait()
            for h in range(2):
                for m in range(4):
                    v = advance(wq[h, m], vq[1 - new, h, m], vq[new, h, m])
                    vq[new, h, m] = v
                    for n in range(4):
                        at = (m, n) if h else (n, m)
                        u_ref[pair(0, h), at[0], at[1], c] = v[n].astype(BF16).reshape(2, BLK, SLICE)
            for i in cuts:
                if i:
                    for h, d in moves:
                        p2(i, h, d).wait_recv()
                for h in range(2):
                    p3(i, h).start()
                if i:
                    product(i - 1)
            product(cuts[-1])
            for i in cuts:
                if i:
                    for h, d in moves:
                        p2(i, h, d).wait_send()
                for h in range(2):
                    p3(i, h).wait_send()

        emit(j + 1)
        return beta_s

    lax.fori_loop(0, STEPS, step, jnp.zeros((1, 1), F32))

    def drain(jv, carry):
        for h in range(2):
            dst_x = 2 * c + h
            dst_c = x // 2

            @pl.when(jnp.logical_not(jnp.logical_and(dst_x == x, dst_c == c)))
            def _():
                rcopy(piece(jv, h), kbuf.at[jv, :, :, 0:SLICE], k_send.at[jv, h], k_recv.at[jv, 0],
                      row_base + dst_x, dst_c).wait_send()

        for m in range(2):
            src_x = 2 * c + m
            src_c = x // 2

            @pl.when(jnp.logical_not(jnp.logical_and(src_x == x, src_c == c)))
            def _():
                rcopy(piece(jv, 0), kbuf.at[jv, :, :, m * SLICE:(m + 1) * SLICE], k_send.at[jv, 0], k_recv.at[jv, m],
                      row_base + src_x, src_c).wait_recv()

        return carry

    lax.fori_loop(0, STEPS + 1, drain, 0)
    cp_k = pltpu.make_async_copy(kbuf, kr_ref, ld_sem.at[0])
    cp_k.start()
    cp_k.wait()


def solution(mesh):
    assert mesh.shape['terms'] == 2 and mesh.shape['rows'] == 64

    def body_fn(wavefunc, left_loc, two_loc, right_loc):
        elem_count = float(wavefunc.size)
        vm = pl.BlockSpec(memory_space=pltpu.VMEM)
        hbm = pl.BlockSpec(memory_space=pl.ANY)
        dma = pltpu.SemaphoreType.DMA
        kr, ab = pl.pallas_call(
            lambda *refs: kernel(elem_count, *refs),
            out_shape=(jax.ShapeDtypeStruct((STEPS + 1, BLK, 8, QB), F32), jax.ShapeDtypeStruct((BLK, SLICE), F32)),
            in_specs=[hbm, hbm, hbm, vm],
            out_specs=(hbm, vm),
            scratch_shapes=[
                pltpu.VMEM((BLK, SLICE, BOND), F32),
                pltpu.VMEM((BLK, SLICE, BOND), F32),
                pltpu.VMEM((5, SLICE, SLICE), F32),
                pltpu.VMEM((BLK, NT, QB), F32),
                pltpu.VMEM((BLK, SLICE, BOND), BF16),
                pltpu.VMEM((BLK, 4, 4, 2, BLK, SLICE), BF16),
                pltpu.VMEM((4, BOND, BOND), BF16),
                pltpu.VMEM((2, 1024, BOND), BF16),
                pltpu.VMEM((NT, SLICE, BOND), BF16),
                pltpu.VMEM((NT, QB, QB), BF16),
                pltpu.VMEM((NT, 2, BLK, BLK, SLICE), BF16),
                pltpu.VMEM((2, NT, QB, SLICE), BF16),
                pltpu.VMEM((2, 4, QB, SLICE), F32),
                pltpu.VMEM((4, QB, SLICE), F32),
                pltpu.VMEM((3, QB, SLICE), F32),
                pltpu.VMEM((STEPS + 1, QB, SLICE), F32),
                pltpu.VMEM((STEPS + 1, BLK, 8, QB), F32),
                pltpu.VMEM((2, 4, SLICE, SLICE), F32),
                pltpu.VMEM((2, 2, 4, SLICE, SLICE), F32),
                pltpu.VMEM((2, 4, 4, 32, SLICE), F32),
                pltpu.VMEM((2, 2, 4, 4, 32, SLICE), F32),
                pltpu.VMEM((4, 8, SLICE), F32),
                pltpu.VMEM((8, 8, SLICE), F32),
                pltpu.VMEM((2, BLK, 8, SLICE), F32),
                dma((2,)), dma((2, BLK)), dma((8,)), dma((8,)), dma((3,)), dma((3,)), dma((2,)), dma((2,)), dma((3,)), dma((3,)),
                dma((7,)), dma((7,)), dma((2, 15)), dma((2, 15)),
                dma((2, 3)), dma((2, 3)), dma((2, 3)), dma((2, 3)), dma((2, 4, 3)), dma((2, 4, 3)), dma((2, 4)), dma((2, 4)),
                dma((STEPS + 1, 2)), dma((STEPS + 1, 2)),
            ],
            compiler_params=pltpu.CompilerParams(has_side_effects=True, collective_id=0, vmem_limit_bytes=60 * 1024 * 1024),
        )(wavefunc, left_loc, right_loc.reshape(BOND, BOND), jnp.transpose(two_loc, (1, 2, 0)).reshape(QB, NT))
        krylov = jnp.transpose(kr.reshape(STEPS + 1, 4, 4, 8, QB), (0, 4, 1, 2, 3))
        return krylov, ab[:STEPS, 0], ab[8:8 + STEPS, 0]

    return jax.shard_map(body_fn, mesh=mesh, in_specs=(P(), P('terms'), P('terms'), P('terms', 'rows')),
                         out_specs=(P(None, 'terms', None, None, 'rows'), P(), P()), check_vma=False)
```

```python
import jax
import jax.numpy as jnp
from jax import lax
from jax.experimental import pallas as pl
from jax.experimental.pallas import tpu as pltpu
from jax.sharding import PartitionSpec as P

STEPS = 6
F32 = jnp.float32
BF16 = jnp.bfloat16
MESH = pl.DeviceIdType.MESH
NT = 64
BOND = 512
SLICE = 128
BLK = 16
QB = 256


def total(x):
    return jnp.sum(jnp.sum(x, axis=1, keepdims=True), axis=0, keepdims=True)


def blk(i, size):
    return pl.ds(pl.multiple_of(i * size, size), size)


def col_sum(x):
    return jnp.sum(x, axis=0, keepdims=True)


def sq_block(blk):
    out = jnp.zeros((8, SLICE), F32)
    sq = (blk * blk).reshape(BLK, 8, BOND).sum(axis=0)
    for i in range(4):
        out = out + sq[:, i * SLICE:(i + 1) * SLICE]
    return out


def kernel(elem_count, wave_ref, left_ref, right_ref, two_ref, kr_ref, ab_ref,
           slab, nslab, tmp, wide, ut, u_ref, rin, rb, lb, wt, y_ref, z_ref, acc, recv_s, recv_x, vecs, kbuf, wg, vg, wq, vq,
           red_n, red_a, red_b,
           ld_sem, sl_sem, r_send, r_recv, n_send, n_recv, s_send, s_recv, x_send, x_recv, a_send, a_recv,
           b_send, b_recv, g1_send, g1_recv, f_send, f_recv, g2_send, g2_recv, g3_send, g3_recv, k_send, k_recv):
    r = lax.axis_index('rows')
    c = lax.axis_index('terms')
    x = lax.rem(r, 4)
    y = lax.rem(r // 4, 4)
    z = r // BLK
    g = r // 4
    row_base = r - x
    z_peers = [lax.rem(z + d, 4) * BLK + y * 4 + x for d in (1, 2, 3)]
    y_peers = [z * BLK + lax.rem(y + d, 4) * 4 + x for d in (1, 2, 3)]
    x_peers = [row_base + lax.rem(x + d, 4) for d in (1, 2, 3)]

    def pair(i, h):
        return pl.ds(8 * h + 2 * i, 2)

    def rcopy(src, dst, ssem, rsem, row, core):
        return pltpu.make_async_remote_copy(src_ref=src, dst_ref=dst, send_sem=ssem, recv_sem=rsem,
                                            device_id=(row, core), device_id_type=MESH)

    me = x * 2 + c
    group = [(row_base + lax.rem(me + d, 8) // 2, lax.rem(me + d, 2)) for d in range(1, 8)]
    plane = [(lax.rem(g + d, BLK) * 4 + x, c) for d in range(1, BLK)]
    barrier = pltpu.get_barrier_semaphore()
    for peer in group + plane:
        pl.semaphore_signal(barrier, inc=1, device_id=peer, device_id_type=MESH)

    cp_r = pltpu.make_async_copy(right_ref, rin.at[x], ld_sem.at[0])
    cp_r.start()
    n_loads, s_loads = [], []
    for p in range(BLK):
        rows_n = blk(z, SLICE)
        n_loads.append(pltpu.make_async_copy(wave_ref.at[rows_n, p // 4, p % 4, :], nslab.at[p], sl_sem.at[0, p]))
    for p in range(BLK):
        rows_s = blk(x, SLICE)
        s_loads.append(pltpu.make_async_copy(wave_ref.at[rows_s, p // 4, p % 4, :], slab.at[p], sl_sem.at[1, p]))
    cp_l = pltpu.make_async_copy(left_ref.at[:, blk(x, SLICE), :], lb, ld_sem.at[1])
    for cp in n_loads + s_loads:
        cp.start()
    cp_l.start()
    cp_r.wait()
    pl.semaphore_wait(barrier, len(group) + len(plane))

    right = row_base + lax.rem(x + 1, 4)
    left = row_base + lax.rem(x + 3, 4)
    xl = lax.rem(x + 3, 4)
    xr = lax.rem(x + 1, 4)
    halves = [pl.ds(0, QB), pl.ds(QB, QB)]

    quarters = [pl.ds(i * SLICE, SLICE) for i in range(4)]

    def r_move(i, block, rows, row):
        ref = rin.at[block, rows, :]
        return rcopy(ref, ref, r_send.at[i], r_recv.at[i], row, c)

    r0 = r_move(0, x, halves[0], right)
    r1 = r_move(1, x, halves[1], left)
    r2 = r_move(2, x, halves[1], right)
    r3 = r_move(3, x, halves[0], left)
    r4 = [r_move(4 + i, xl, quarters[i], right) for i in range(2)]
    r5 = [r_move(6 + i, xr, quarters[2 + i], left) for i in range(2)]
    for cp in (r0, r1, r2, r3):
        cp.start()

    for cp in n_loads:
        cp.wait()

    ssq = jnp.zeros((8, SLICE), F32)
    ssq = lax.fori_loop(0, BLK, lambda p, acc: acc + sq_block(nslab[p]), ssq)
    red_n[0] = jnp.zeros((8, SLICE), F32) + total(ssq)
    n_copies = []
    for d, row in enumerate(z_peers):
        cp = rcopy(red_n.at[0], red_n.at[d + 1], n_send.at[d], n_recv.at[d], row, c)
        cp.start()
        n_copies.append(cp)

    row_e = lax.broadcasted_iota(jnp.int32, (QB, BLK), 0)
    lane_e = lax.broadcasted_iota(jnp.int32, (QB, BLK), 1)
    e_row = (row_e // BLK == lane_e).astype(BF16)
    row_m = lax.broadcasted_iota(jnp.int32, (QB, QB), 0)
    lane_m = lax.broadcasted_iota(jnp.int32, (QB, QB), 1)
    diag = lax.rem(row_m, BLK) == lax.rem(lane_m, BLK)

    by_term = jnp.transpose(two_ref[...].astype(F32)).astype(BF16)
    for q in range(BLK):
        pick = (row_m == q * BLK + lane_m // BLK).astype(BF16)
        wide[q] = jnp.dot(by_term, pick, preferred_element_type=F32)

    def build_w(kk, carry):
        for i in range(8):
            k = kk * 8 + i
            rows = wide[:, k, :].astype(BF16)
            full = jnp.dot(e_row, rows, preferred_element_type=F32)
            wt[k] = jnp.where(diag, full, 0.0).astype(BF16)
        return carry

    lax.fori_loop(0, NT // 8, build_w, 0)
    r0.wait_recv()
    for cp in r4:
        cp.start()
    r1.wait_recv()
    for cp in r5:
        cp.start()

    for cp in n_copies:
        cp.wait()
    norm = [red_n[lax.rem(z - s + 4, 4)] for s in range(4)]
    scale = jnp.sqrt(((norm[0] + norm[1]) + (norm[2] + norm[3]))[:1, :1] / elem_count)
    for cp in s_loads:
        cp.wait()
    vg[1] = jnp.zeros_like(vg[1])

    def first(p, carry):
        ut[p] = (slab[p] / scale).astype(BF16)
        ut[p + 8] = (slab[p + 8] / scale).astype(BF16)
        for n in range(4):
            tmp[n] = jnp.transpose(slab[p, :, n * SLICE:(n + 1) * SLICE])
        tmp[4] = jnp.transpose(slab[p + 8, :, blk(z, SLICE)])
        for n in range(4):
            vg[0, 0, n, blk(p, BLK), :] = tmp[n, blk(y * 2 + c, BLK), :] / scale
            vg[0, 1, n, blk(p, BLK), :] = tmp[4, blk(n * 2 + c, BLK), :] / scale
        return carry

    lax.fori_loop(0, 8, first, 0)
    vq[1] = jnp.zeros_like(vq[1])

    def first_pairs(p, carry):
        for h in range(2):
            for n in range(4):
                tmp[n] = jnp.transpose(slab[8 * h + p, :, n * SLICE:(n + 1) * SLICE])
            for n in range(4):
                for m in range(4):
                    at = (n, m) if h else (m, n)
                    vq[0, h, at[0], at[1], blk(p, BLK), :] = tmp[n, blk(m * 2 + c, BLK), :] / scale
        return carry

    lax.fori_loop(0, 2, first_pairs, 0)
    vecs[0, :SLICE] = vg[0, 0, z]
    vecs[0, SLICE:] = vg[0, 1, y]

    out_lanes = blk(lax.rem(x, 2), SLICE)

    def piece(jv, h):
        return vecs.at[jv].reshape(BLK, BLK, SLICE).at[:, h * 8:(h + 1) * 8, :]

    def emit(jv):
        for h in range(2):
            dst_x = 2 * c + h
            dst_c = x // 2
            is_me = jnp.logical_and(dst_x == x, dst_c == c)

            @pl.when(jnp.logical_not(is_me))
            def _():
                rcopy(piece(jv, h), kbuf.at[jv, :, :, out_lanes], k_send.at[jv, h], k_recv.at[jv, lax.rem(x, 2)],
                      row_base + dst_x, dst_c).start()

            @pl.when(is_me)
            def _():
                kbuf[jv, :, :, out_lanes] = vecs[jv].reshape(BLK, BLK, SLICE)[:, h * 8:(h + 1) * 8, :]

    def build_r(bhi, parts):
        for i in parts:
            rows = quarters[i]
            lo = rin[2 * bhi, rows, :].astype(F32).reshape(BLK, 8, BOND)
            hi = rin[2 * bhi + 1, rows, :].astype(F32).reshape(BLK, 8, BOND)
            both = jnp.concatenate([lo, hi], axis=1).reshape(QB, BOND)
            rb[bhi, pl.ds(i * QB, QB), :] = both.astype(BF16)

    def put_y(o, bhi, first_k, pp):
        o = o.astype(BF16).reshape(-1, BLK, QB)
        rows = pl.ds(first_k, o.shape[0])
        y_ref[rows, bhi, 2 * pp] = o[:, :, :SLICE]
        y_ref[rows, bhi, 2 * pp + 1] = o[:, :, SLICE:]

    def s1_first(bhi, parts):
        build_r(bhi, parts)

        def body(i, carry):
            for pp in (i, i + 4):
                w = ut[pl.ds(2 * pp, 2)].reshape(QB, BOND)
                for m in parts:
                    rows = rb[bhi, pl.ds(m * QB, QB), :]
                    o = lax.dot_general(rows, w, (((1,), (1,)), ((), ())), preferred_element_type=F32)
                    put_y(o, bhi, m * BLK, pp)
            return carry

        lax.fori_loop(0, 4, body, 0)

    def s1(pp):
        w = jnp.concatenate([u_ref[2 * pp + i].reshape(BOND, SLICE) for i in range(2)], axis=1)
        for bhi in range(2):
            for mc in range(2):
                put_y(jnp.dot(rb[bhi, pl.ds(mc * BOND, BOND), :], w, preferred_element_type=F32), bhi, mc * 32, pp)

    for cp in (r2, r3):
        cp.wait_recv()
    own = x // 2
    s1_first(own, range(4))
    for i in range(2):
        r4[i].wait_recv()
        r5[i].wait_recv()
        s1_first(1 - own, (i, 2 + i))
    for cp in [r0, r1, r2, r3] + r4 + r5:
        cp.wait_send()
    cp_l.wait()
    emit(0)

    row_id = lax.broadcasted_iota(jnp.int32, (8, SLICE), 0)
    ab_ref[...] = jnp.zeros_like(ab_ref)

    def pack(p, n, am, rr, ss):
        out = jnp.where(row_id == 0, p, 0.0)
        out = jnp.where(row_id == 1, n, out)
        out = jnp.where(row_id == 2, am, out)
        out = jnp.where(row_id == 3, rr, out)
        return jnp.where(row_id == 4, ss, out)

    def safe_div(num, den):
        ok = den > 0.0
        return jnp.where(ok, num / jnp.where(ok, den, 1.0), 0.0)

    def merge(p, n, am, rr, ss):
        n_all = col_sum(n)
        mean = safe_div(col_sum(am * n), n_all)
        gap = mean - am
        r_all = col_sum(rr + gap * (gap * n - 2.0 * ss))
        return col_sum(p), n_all, mean, r_all, col_sum(ss)

    def step(j, prev_beta):
        for k in range(NT):
            rhs = jnp.concatenate([y_ref[k, bhi].reshape(QB, SLICE) for bhi in range(2)], axis=1)
            o = jnp.dot(wt[k], rhs, preferred_element_type=F32).astype(BF16)
            z_ref[0, k] = o[:, :SLICE]
            z_ref[1, k] = o[:, SLICE:]


        order = [lax.rem(x + d, 4) for d in (2, 1, 3, 0)]

        def s3(bhi, out, lo):
            slices = [blk(pos, SLICE) for pos in order[lo:lo + 2]]
            outs = [None, None]
            for k0 in range(0, NT // 2, 8):
                for kh in range(2):
                    ks = k0 + kh * NT // 2
                    rhs = jnp.concatenate([lb[pl.ds(ks, 8), :, sl].reshape(1024, SLICE) for sl in slices], axis=1)
                    lhs = jnp.concatenate([z_ref[bhi, ks + k] for k in range(8)], axis=1)
                    o = jnp.dot(lhs, rhs, preferred_element_type=F32)
                    outs[kh] = o if outs[kh] is None else outs[kh] + o
            for n in range(2):
                cols = slice(n * SLICE, (n + 1) * SLICE)
                out[lo + n] = outs[0][:, cols] - (0.0 - outs[1][:, cols])

        acc_o = acc.at[1 - c]
        acc_m = acc.at[c]
        s_copies = []
        for n in range(2):
            two = pl.ds(2 * n, 2)
            s_copies.append(rcopy(acc_o.at[two], recv_s.at[two], s_send.at[n], s_recv.at[n], r, 1 - c))
        x_copies = []
        for n in range(3):
            x_copies.append(rcopy(acc_m.at[n], recv_x.at[n], x_send.at[n], x_recv.at[n], row_base + order[n], c))
        s3(1 - c, acc_o, 0)
        s_copies[0].start()
        s3(c, acc_m, 0)
        s_copies[0].wait_recv()
        for n in range(2):
            acc_m[n] += recv_s[n]
            x_copies[n].start()
        s3(1 - c, acc_o, 2)
        s_copies[1].start()
        s3(c, acc_m, 2)
        s_copies[1].wait_recv()
        acc_m[2] += recv_s[2]
        x_copies[2].start()
        w_own = acc_m[3] + recv_s[3]
        for cp in s_copies:
            cp.wait_send()
        for cp in x_copies:
            cp.wait()
        w_vec = (w_own + recv_x[0]) + (recv_x[1] + recv_x[2])
        v_cur = vecs[j]
        v_old = vecs[lax.max(j - 1, 0)]

        w_res = w_vec - prev_beta * v_old
        n_loc = total(v_cur * v_cur)
        a_loc = safe_div(total(w_res * v_cur), n_loc)
        e_loc = w_res - a_loc * v_cur
        red_a[0] = pack(total(w_vec * v_cur), n_loc, a_loc, total(e_loc * e_loc), total(e_loc * v_cur))

        a_copies = [rcopy(red_a.at[0], red_a.at[d + 1], a_send.at[d], a_recv.at[d], *peer) for d, peer in enumerate(group)]
        for cp in a_copies:
            cp.start()

        wg[0, z] = w_vec[:SLICE]
        wg[1, y] = w_vec[SLICE:]
        near = []
        for d in range(3):
            near.append(rcopy(wg.at[0, z], wg.at[0, z], g1_send.at[0, d], g1_recv.at[0, d], z_peers[d], c))
            near.append(rcopy(wg.at[1, y], wg.at[1, y], g1_send.at[1, d], g1_recv.at[1, d], y_peers[d], c))

        @pl.when(j < STEPS - 1)
        def _():
            for cp in near:
                cp.start()

        for cp in a_copies:
            cp.wait()
        blocks = [red_a[lax.rem(me - s + 8, 8)] for s in range(8)]

        def gather_rows(blks, i):
            return jnp.concatenate([bk[i:i + 1, :] for bk in blks], axis=0)

        par = lax.rem(j, 2)
        red_b[par, 0] = pack(*merge(*[gather_rows(blocks, i) for i in range(5)]))
        b_copies = []
        for d, peer in enumerate(plane):
            b_copies.append(rcopy(red_b.at[par, 0], red_b.at[par, d + 1], b_send.at[par, d], b_recv.at[par, d], *peer))
        for cp in b_copies:
            cp.start()

        far = []
        for d in range(3):
            far.append(rcopy(wq.at[0, y], wq.at[0, y], f_send.at[0, d], f_recv.at[0, d], y_peers[d], c))
            far.append(rcopy(wq.at[1, z], wq.at[1, z], f_send.at[1, d], f_recv.at[1, d], z_peers[d], c))

        @pl.when(j < STEPS - 1)
        def _():
            for cp in near:
                cp.wait()
            wq[0, y] = wg[0, :, :32]
            wq[1, z] = wg[1, :, :32]
            for cp in far:
                cp.start()

        for cp in b_copies:
            cp.wait()
        blocks = [red_b[par, lax.rem(g - s + BLK, BLK)] for s in range(BLK)]
        p_all, n_all, a_all, r_all, s_all = [gather_rows(blocks, i) for i in range(5)]
        alpha = col_sum(p_all) / elem_count
        gap = alpha - a_all
        beta = jnp.sqrt(col_sum(r_all + gap * (gap * n_all - 2.0 * s_all)) / elem_count)
        alpha_s = alpha[:, :1]
        beta_s = beta[:, :1]

        def advance(w, cur, old):
            return (w - alpha_s * cur - prev_beta * old) / beta_s

        new = lax.rem(j + 1, 2)
        moves = [(h, d) for h in range(2) for d in range(3)]
        cuts = range(4)

        def p2(i, h, d):
            ref = u_ref.at[pair(i, h), z, :, c] if h else u_ref.at[pair(i, h), :, y, c]
            row = z_peers[d] if h else y_peers[d]
            return rcopy(ref, ref, g2_send.at[h, i, d], g2_recv.at[h, i, d], row, c)

        def p3(i, h):
            ref = u_ref.at[pair(i, h), :, :, c]
            return rcopy(ref, ref, g3_send.at[h, i], g3_recv.at[h, i], r, 1 - c)

        def product(i):
            for h in range(2):
                p3(i, h).wait_recv()
            s1(i)
            s1(4 + i)

        @pl.when(j < STEPS - 1)
        def _():
            for i in cuts[1:]:
                rows = pl.ds(32 * i, 32)
                for h in range(2):
                    for n in range(4):
                        v = advance(wg[h, n, rows], vg[1 - new, h, n, rows], vg[new, h, n, rows])
                        vg[new, h, n, rows] = v
                        at = (z, n) if h else (n, y)
                        u_ref[pair(i, h), at[0], at[1], c] = v.astype(BF16).reshape(2, BLK, SLICE)
                for h, d in moves:
                    p2(i, h, d).start()

        v_new = advance(w_vec, v_cur, v_old)
        vecs[j + 1] = v_new
        ab_ref[pl.ds(j, 1), :] = alpha
        ab_ref[pl.ds(8 + j, 1), :] = beta

        @pl.when(j < STEPS - 1)
        def _():
            for cp in far:
                cp.wait()
            for h in range(2):
                for m in range(4):
                    v = advance(wq[h, m], vq[1 - new, h, m], vq[new, h, m])
                    vq[new, h, m] = v
                    for n in range(4):
                        at = (m, n) if h else (n, m)
                        u_ref[pair(0, h), at[0], at[1], c] = v[n].astype(BF16).reshape(2, BLK, SLICE)
            for i in cuts:
                if i:
                    for h, d in moves:
                        p2(i, h, d).wait_recv()
                for h in range(2):
                    p3(i, h).start()
                if i:
                    product(i - 1)
            product(cuts[-1])
            for i in cuts:
                if i:
                    for h, d in moves:
                        p2(i, h, d).wait_send()
                for h in range(2):
                    p3(i, h).wait_send()

        emit(j + 1)
        return beta_s

    lax.fori_loop(0, STEPS, step, jnp.zeros((1, 1), F32))

    def drain(jv, carry):
        for h in range(2):
            dst_x = 2 * c + h
            dst_c = x // 2

            @pl.when(jnp.logical_not(jnp.logical_and(dst_x == x, dst_c == c)))
            def _():
                rcopy(piece(jv, h), kbuf.at[jv, :, :, 0:SLICE], k_send.at[jv, h], k_recv.at[jv, 0],
                      row_base + dst_x, dst_c).wait_send()

        for m in range(2):
            src_x = 2 * c + m
            src_c = x // 2

            @pl.when(jnp.logical_not(jnp.logical_and(src_x == x, src_c == c)))
            def _():
                rcopy(piece(jv, 0), kbuf.at[jv, :, :, m * SLICE:(m + 1) * SLICE], k_send.at[jv, 0], k_recv.at[jv, m],
                      row_base + src_x, src_c).wait_recv()

        return carry

    lax.fori_loop(0, STEPS + 1, drain, 0)
    cp_k = pltpu.make_async_copy(kbuf, kr_ref, ld_sem.at[0])
    cp_k.start()
    cp_k.wait()


def solution(mesh):
    assert mesh.shape['terms'] == 2 and mesh.shape['rows'] == 64

    def body_fn(wavefunc, left_loc, two_loc, right_loc):
        elem_count = float(wavefunc.size)
        vm = pl.BlockSpec(memory_space=pltpu.VMEM)
        hbm = pl.BlockSpec(memory_space=pl.ANY)
        dma = pltpu.SemaphoreType.DMA
        kr, ab = pl.pallas_call(
            lambda *refs: kernel(elem_count, *refs),
            out_shape=(jax.ShapeDtypeStruct((STEPS + 1, BLK, 8, QB), F32), jax.ShapeDtypeStruct((BLK, SLICE), F32)),
            in_specs=[hbm, hbm, hbm, vm],
            out_specs=(hbm, vm),
            scratch_shapes=[
                pltpu.VMEM((BLK, SLICE, BOND), F32),
                pltpu.VMEM((BLK, SLICE, BOND), F32),
                pltpu.VMEM((5, SLICE, SLICE), F32),
                pltpu.VMEM((BLK, NT, QB), F32),
                pltpu.VMEM((BLK, SLICE, BOND), BF16),
                pltpu.VMEM((BLK, 4, 4, 2, BLK, SLICE), BF16),
                pltpu.VMEM((4, BOND, BOND), BF16),
                pltpu.VMEM((2, 1024, BOND), BF16),
                pltpu.VMEM((NT, SLICE, BOND), BF16),
                pltpu.VMEM((NT, QB, QB), BF16),
                pltpu.VMEM((NT, 2, BLK, BLK, SLICE), BF16),
                pltpu.VMEM((2, NT, QB, SLICE), BF16),
                pltpu.VMEM((2, 4, QB, SLICE), F32),
                pltpu.VMEM((4, QB, SLICE), F32),
                pltpu.VMEM((3, QB, SLICE), F32),
                pltpu.VMEM((STEPS + 1, QB, SLICE), F32),
                pltpu.VMEM((STEPS + 1, BLK, 8, QB), F32),
                pltpu.VMEM((2, 4, SLICE, SLICE), F32),
                pltpu.VMEM((2, 2, 4, SLICE, SLICE), F32),
                pltpu.VMEM((2, 4, 4, 32, SLICE), F32),
                pltpu.VMEM((2, 2, 4, 4, 32, SLICE), F32),
                pltpu.VMEM((4, 8, SLICE), F32),
                pltpu.VMEM((8, 8, SLICE), F32),
                pltpu.VMEM((2, BLK, 8, SLICE), F32),
                dma((2,)), dma((2, BLK)), dma((8,)), dma((8,)), dma((3,)), dma((3,)), dma((2,)), dma((2,)), dma((3,)), dma((3,)),
                dma((7,)), dma((7,)), dma((2, 15)), dma((2, 15)),
                dma((2, 3)), dma((2, 3)), dma((2, 3)), dma((2, 3)), dma((2, 4, 3)), dma((2, 4, 3)), dma((2, 4)), dma((2, 4)),
                dma((STEPS + 1, 2)), dma((STEPS + 1, 2)),
            ],
            compiler_params=pltpu.CompilerParams(has_side_effects=True, collective_id=0, vmem_limit_bytes=60 * 1024 * 1024),
        )(wavefunc, left_loc, right_loc.reshape(BOND, BOND), jnp.transpose(two_loc, (1, 2, 0)).reshape(QB, NT))
        krylov = jnp.transpose(kr.reshape(STEPS + 1, 4, 4, 8, QB), (0, 4, 1, 2, 3))
        return krylov, ab[:STEPS, 0], ab[8:8 + STEPS, 0]

    return jax.shard_map(body_fn, mesh=mesh, in_specs=(P(), P('terms'), P('terms'), P('terms', 'rows')),
                         out_specs=(P(None, 'terms', None, None, 'rows'), P(), P()), check_vma=False)
```
